32 devices in a mesh: frame: 4 (over y, x), row: 8 (over z, core).
Axes of the slice: x: 2, y: 2, z: 4, core: 2. Of those that a mesh axis runs over, the one named last changes fastest.
Arguments:
- tokens: bfloat16 [1, 32, 16, 16, 1024], P(None, 'frame', 'row'), may hold values from -6 to 6
- timesteps: int32 [1, 32], P(None, 'frame'), may hold values from 0 to 999, as said below
- noise_table: bfloat16 [1000, 1024], replicated, may hold values from -5 to 5
- mod_weight: bfloat16 [1024, 6144], P(None, 'row'), may hold values from -0.1875 to 0.1875
- mod_bias: bfloat16 [6144], P('row'), may hold values from -3 to 3
- attn_in: bfloat16 [1024, 4096], P('row'), may hold values from -0.1875 to 0.1875
- out_weight: bfloat16 [1024, 1024], P('row'), may hold values from -4 to 4
- up_weight: bfloat16 [1024, 4096], P('row'), may hold values from -0.1875 to 0.1875
- down_weight: bfloat16 [1024, 4096], P('row'), may hold values from -0.09375 to 0.09375
- cotangent: bfloat16 [1, 32, 16, 16, 1024], P(None, 'frame', 'row'), may hold values from -6 to 6
Outputs:
- mixed: bfloat16 [1, 32, 16, 16, 1024], P(None, 'frame', 'row')
- tokens_grad: bfloat16 [1, 32, 16, 16, 1024], P(None, 'frame', 'row')
- noise_table_grad: float32 [1000, 1024], replicated
- mod_weight_grad: float32 [1024, 6144], P(None, 'row')
- mod_bias_grad: float32 [6144], P('row')
- attn_in_grad: float32 [1024, 4096], P('row')
- out_weight_grad: float32 [1024, 1024], P('row')
- up_weight_grad: float32 [1024, 4096], P('row')
- down_weight_grad: float32 [1024, 4096], P('row')
The draws below stay inside these ranges and needn't reach their ends.
Inputs may be any that keep to these rules, and one draw needn't show every extreme that they name: `timesteps`: Noise-level index of each frame; both 0 and 999 occur in every draw.
All inputs are finite; a program needn't handle non-finite values.
Results may differ from the reference program's by a relative error of at most 0.019.
The reference program's roundings to bfloat16 on the way count: a program that leaves them out, or rounds other values in their place, can miss the bound.
Values may be sent and summed in bfloat16 or wider, within the bound.
A program may use at most 576 MiB of HBM per device.

```python
import jax
import jax.numpy as jnp
import numpy as np
from jax import lax

D = 1024
HEADS = 16
HEAD_DIM = 64
FF = 4096
GRID = 16
CLIP_LEN = 32
STEPS = 1000
CLIPS = 1


def draw_timesteps(key, part):
    key_left, key_right, key_order = jax.random.split(key, 3)
    total_frames = CLIPS * CLIP_LEN
    draws_left = jax.random.randint(key_left, (total_frames,), 0, STEPS)
    draws_right = jax.random.randint(key_right, (total_frames,), 0, STEPS)
    levels = STEPS - 1 - draws_left * draws_right // STEPS
    placing = jax.random.permutation(key_order, total_frames)
    levels = levels.at[placing[0]].set(STEPS - 1)
    levels = levels.at[placing[1]].set(0)
    return levels.reshape(CLIPS, CLIP_LEN).astype(jnp.int32)


def block_scale(own_key, shape, shards, smallest, largest):
    level, own = 1.0, jax.random.fold_in(own_key, 6)
    for dim, shards_of in shards:
        steps = jnp.exp(jax.random.uniform(jax.random.fold_in(own, dim), (shards_of,), jnp.float32, smallest / len(shards), largest / len(shards)))
        level = level * jnp.repeat(steps, shape[dim] // shards_of).reshape([-1 if axis == dim else 1 for axis in range(len(shape))])
    return level


def gaussian(own_key, extent, scale, most, cuts=(), kind=jnp.bfloat16):
    entries = jax.random.normal(own_key, extent, jnp.float32) * scale
    if len(cuts) > 0:
        entries = block_scale(own_key, extent, cuts, -0.22, 0.18) * entries
    return jnp.clip(entries, min=-most, max=most).astype(kind)


def setup_inputs(seed: int = 0) -> dict:
    key_list = jax.random.split(jax.random.key(seed), 11)
    return {
        "tokens": gaussian(key_list[0], (CLIPS, CLIP_LEN, GRID, GRID, D), 1.0, 6.0, ((1, 4), (2, 8))),
        "timesteps": draw_timesteps(jax.random.fold_in(key_list[10], 71), 0),
        "noise_table": gaussian(key_list[2], (STEPS, D), 1.0, 5.0),
        "mod_weight": gaussian(key_list[3], (D, 6 * D), D ** -0.5, 0.1875, ((1, 8),)),
        "mod_bias": gaussian(key_list[4], (6 * D,), 0.5, 3.0, ((0, 8),)),
        "attn_in": gaussian(key_list[5], (D, 4 * D), D ** -0.5, 0.1875, ((0, 8),)),
        "out_weight": gaussian(key_list[6], (D, D), 0.7, 4.0, ((0, 8),)),
        "up_weight": gaussian(key_list[7], (D, FF), D ** -0.5, 0.1875, ((0, 8),)),
        "down_weight": gaussian(key_list[8], (D, FF), FF ** -0.5, 0.09375, ((0, 8),)),
        "cotangent": gaussian(key_list[9], (CLIPS, CLIP_LEN, GRID, GRID, D), 1.0, 6.0, ((1, 4), (2, 8))),
    }


@jax.custom_vjp
def low(v):
    return lax.optimization_barrier(v.astype(jnp.bfloat16)).astype(jnp.float32)

@jax.custom_vjp
def low_back(v):
    return v

def low_keep(v):
    return (low(v), None)

def low_pass(kept, grad):
    return (grad,)

def back_keep(v):
    return (v, None)

def back_low(kept, grad):
    return (low(grad),)
low.defvjp(low_keep, low_pass)
low_back.defvjp(back_keep, back_low)
HIGHEST = lax.Precision.HIGHEST
EPS = 1e-06

def rotary_freqs(pair_count):
    third_count = pair_count // 3
    group_sizes = [pair_count - 2 * third_count, third_count, third_count]
    tables = []
    offset = 0
    for group_index in range(3):
        freq_table = np.zeros((pair_count,), np.float32)
        for inner_index in range(group_sizes[group_index]):
            freq_table[offset + inner_index] = 10000.0 ** (-inner_index / group_sizes[group_index])
        offset += group_sizes[group_index]
        tables.append(freq_table)
    return tables

def rotary_angles(frame_pos, row_pos, col_pos, pair_count):
    frame_freq, row_freq, col_freq = rotary_freqs(pair_count)
    return frame_pos[..., None] * frame_freq + row_pos[..., None] * row_freq + col_pos[..., None] * col_freq

def rotate(values, cosines, sines):
    half_dim = values.shape[-1] // 2
    upper_half = values[..., :half_dim]
    lower_half = values[..., half_dim:]
    return jnp.concatenate([upper_half * cosines - lower_half * sines, upper_half * sines + lower_half * cosines], axis=-1)

def layer_norm(values):
    row_mean = lax.optimization_barrier(jnp.mean(values, axis=-1, keepdims=True))
    centered = values - row_mean
    row_var = lax.optimization_barrier(jnp.mean(centered * centered, axis=-1, keepdims=True))
    return centered * lax.rsqrt(row_var + EPS)

def modulate(values, shift, scale_part):
    return layer_norm(values) * (1.0 + scale_part) + shift

def attention(query_rot, key_rot, value_low):
    clip_count, clip_len, grid_side = (query_rot.shape[0], query_rot.shape[1], query_rot.shape[2])
    length = clip_len * grid_side * grid_side

    def flatten(tensor):
        return jnp.transpose(tensor, (0, 4, 1, 2, 3, 5)).reshape(-1, length, tensor.shape[-1])
    frames_of = jnp.arange(length) // (grid_side * grid_side)
    allowed = frames_of[None, :] <= frames_of[:, None]
    score_scale = HEAD_DIM ** (-0.5)

    def one_head(head_items):
        query_head, key_head, value_head = head_items
        scores = low_back(jnp.dot(query_head, key_head.T, precision=HIGHEST) * score_scale)
        scores = jnp.where(allowed, scores, -1e+30)
        weights = low(jax.nn.softmax(scores, axis=-1))
        return jnp.dot(weights, value_head, precision=HIGHEST)
    result = lax.map(jax.checkpoint(one_head), (flatten(query_rot), flatten(key_rot), flatten(value_low)))
    result = result.reshape(clip_count, HEADS, clip_len, grid_side, grid_side, HEAD_DIM)
    return jnp.transpose(result, (0, 2, 3, 4, 1, 5))

def layer(token_f, table_f, mod_weight, mod_bias, attn_in, out_weight, up_weight, down_weight, timesteps):
    clip_count, clip_len, grid_side = (token_f.shape[0], token_f.shape[1], token_f.shape[2])
    model_width = token_f.shape[4]
    embedding = table_f[timesteps]
    silu_low = low(jax.nn.silu(embedding))
    modulation = jnp.einsum('cld,de->cle', silu_low, mod_weight, precision=HIGHEST) + mod_bias
    modulation = low_back(low(modulation)).reshape(clip_count, clip_len, 6, 1, 1, model_width)
    shift_one = modulation[:, :, 0]
    scale_one = modulation[:, :, 1]
    gate_one = modulation[:, :, 2]
    shift_two = modulation[:, :, 3]
    scale_two = modulation[:, :, 4]
    gate_two = modulation[:, :, 5]
    hidden_one = low(modulate(token_f, shift_one, scale_one))
    mixed_in = low_back(jnp.einsum('clrwd,de->clrwe', hidden_one, attn_in, precision=HIGHEST))
    head_shape = (clip_count, clip_len, grid_side, grid_side, HEADS, HEAD_DIM)
    query_raw = mixed_in[..., :model_width].reshape(head_shape)
    key_raw = mixed_in[..., model_width:2 * model_width].reshape(head_shape)
    value_raw = mixed_in[..., 2 * model_width:3 * model_width].reshape(head_shape)
    gate_raw = mixed_in[..., 3 * model_width:]
    grid_shape = (clip_len, grid_side, grid_side)
    frame_pos = lax.broadcasted_iota(jnp.float32, grid_shape, 0)
    row_pos = lax.broadcasted_iota(jnp.float32, grid_shape, 1)
    col_pos = lax.broadcasted_iota(jnp.float32, grid_shape, 2)
    angles = rotary_angles(frame_pos, row_pos, col_pos, HEAD_DIM // 2)[None, :, :, :, None, :]
    cosines = jnp.cos(angles)
    sines = jnp.sin(angles)
    query_rot = low_back(low(rotate(query_raw, cosines, sines)))
    key_rot = low_back(low(rotate(key_raw, cosines, sines)))
    value_low = low_back(low(value_raw))
    attended = attention(query_rot, key_rot, value_low)
    attended = low_back(low(attended)).reshape(clip_count, clip_len, grid_side, grid_side, model_width)
    gated = low(attended * jax.nn.sigmoid(gate_raw))
    branch_one = low_back(jnp.einsum('clrwd,de->clrwe', gated, out_weight, precision=HIGHEST))
    after_one = token_f + gate_one * branch_one
    hidden_two = low(modulate(after_one, shift_two, scale_two))
    pre_act = low_back(jnp.einsum('clrwd,df->clrwf', hidden_two, up_weight, precision=HIGHEST))
    act_low = low(jax.nn.gelu(pre_act, approximate=True))
    branch_two = low_back(jnp.einsum('clrwf,df->clrwd', act_low, down_weight, precision=HIGHEST))
    return after_one + gate_two * branch_two

def reference(tokens, timesteps, noise_table, mod_weight, mod_bias, attn_in, out_weight, up_weight, down_weight, cotangent):

    def forward(token_f, table_f, mod_weight_f, mod_bias_f, attn_in_f, out_weight_f, up_weight_f, down_weight_f):
        return layer(token_f, table_f, mod_weight_f, mod_bias_f, attn_in_f, out_weight_f, up_weight_f, down_weight_f, timesteps)
    floats = [array_in.astype(jnp.float32) for array_in in (tokens, noise_table, mod_weight, mod_bias, attn_in, out_weight, up_weight, down_weight)]
    mixed, pull_back = jax.vjp(forward, *floats)
    all_grads = pull_back(cotangent.astype(jnp.float32))
    return (mixed.astype(jnp.bfloat16), all_grads[0].astype(jnp.bfloat16), all_grads[1], all_grads[2], all_grads[3], all_grads[4], all_grads[5], all_grads[6], all_grads[7])
```

```python
from functools import partial

import jax
import jax.numpy as jnp
import numpy as np
from jax import lax
from jax.experimental import pallas as pl
from jax.experimental.pallas import tpu as pltpu
from jax.sharding import PartitionSpec as P

HEADS = 16
EPS = 1e-06
LOG2E = 1.4426950408889634
F32 = jnp.float32
BF = jnp.bfloat16
LANES = 128
MIB = 1 << 20


def rotary_freqs(pair_count):
    third_count = pair_count // 3
    group_sizes = [pair_count - 2 * third_count, third_count, third_count]
    tables = []
    offset = 0
    for group_index in range(3):
        freq_table = np.zeros((pair_count,), np.float32)
        for inner_index in range(group_sizes[group_index]):
            freq_table[offset + inner_index] = 10000.0 ** (-inner_index / group_sizes[group_index])
        offset += group_sizes[group_index]
        tables.append(freq_table)
    return tables


def layer_norm(values):
    row_mean = jnp.mean(values, axis=-1, keepdims=True)
    centered = values - row_mean
    row_var = jnp.mean(centered * centered, axis=-1, keepdims=True)
    return centered * lax.rsqrt(row_var + EPS)


def modulate(values, shift, scale_part):
    return layer_norm(values) * (1.0 + scale_part) + shift


def dot(left, right, left_dim, right_dim):
    return lax.dot_general(
        left, right, (((left_dim,), (right_dim,)), ((), ())), preferred_element_type=F32
    )


def swap_halves(values):
    lane = lax.broadcasted_iota(jnp.int32, values.shape, 1)
    width = values.shape[1]
    return jnp.where(
        (lane % 64) < 32, pltpu.roll(values, width - 32, 1), pltpu.roll(values, 32, 1)
    )


def low_lanes(shape):
    return lax.broadcasted_iota(jnp.int32, shape, len(shape) - 1) < 64


def qkv_kernel(heads, hid_ref, w_ref, cos_ref, sin_ref, pack_ref, gate_ref):
    clip, quarter = pl.program_id(0), pl.program_id(1)
    width = heads * 64
    mixed = jnp.dot(hid_ref[...], w_ref[...], preferred_element_type=F32)
    cos, sin = cos_ref[...], sin_ref[...]
    rows = mixed.shape[0]
    half = rows // 2
    gate_ref[...] = mixed[:, 3 * width :]
    low = low_lanes((rows, LANES))
    low_half = low_lanes((half, LANES))
    query_set = jnp.where((quarter == 0) | (quarter == 3), 0, 1)
    slot = quarter // 2
    for pair in range(heads // 2):
        cut = slice(pair * LANES, (pair + 1) * LANES)
        query = mixed[:, cut]
        key = mixed[:, width + pair * LANES : width + (pair + 1) * LANES]
        value = mixed[:, 2 * width + pair * LANES : 2 * width + (pair + 1) * LANES]
        query = query * cos + swap_halves(query) * sin
        key = key * cos + swap_halves(key) * sin
        key_turn = pltpu.roll(key, 64, 1)
        value_turn = pltpu.roll(value, 64, 1)
        query_turn = pltpu.roll(query, 64, 1)
        packs = (
            (
                jnp.where(low, key, value_turn),
                jnp.where(low_half, query[:half], query_turn[half:]),
            ),
            (
                jnp.where(low, key_turn, value),
                jnp.where(low_half, query_turn[:half], query[half:]),
            ),
        )
        for inner, (key_value, queries) in enumerate(packs):
            head = 2 * pair + inner
            pack_ref[clip, head, query_set, slot] = queries.astype(BF)
            key_value = key_value.astype(BF)
            first = 2 + 2 * (quarter % 2)
            pack_ref[clip, head, quarter // 2, first] = key_value[:half]
            pack_ref[clip, head, quarter // 2, first + 1] = key_value[half:]


def qkv_project(hidden, weight, cos, sin, clips, heads):
    tokens, width = hidden.shape
    quarter = tokens // clips // 4
    one = pl.Buffered(1)
    return pl.pallas_call(
        partial(qkv_kernel, heads),
        grid=(clips, 4),
        in_specs=[
            pl.BlockSpec((quarter, width), lambda c, i: (c * 4 + i, 0)),
            pl.BlockSpec(weight.shape, lambda c, i: (0, 0), pipeline_mode=one),
            pl.BlockSpec((quarter, LANES), lambda c, i: (i, 0)),
            pl.BlockSpec((quarter, LANES), lambda c, i: (i, 0)),
        ],
        out_specs=[
            pl.BlockSpec(
                (clips, heads, 2, 6, quarter // 2, LANES), lambda c, i: (0, 0, 0, 0, 0, 0)
            ),
            pl.BlockSpec((quarter, heads * 64), lambda c, i: (c * 4 + i, 0)),
        ],
        out_shape=[
            jax.ShapeDtypeStruct((clips, heads, 2, 6, quarter // 2, LANES), BF),
            jax.ShapeDtypeStruct((tokens, heads * 64), F32),
        ],
        compiler_params=pltpu.CompilerParams(
            dimension_semantics=("arbitrary", "arbitrary"), vmem_limit_bytes=48 * MIB
        ),
        name="qkv_project",
    )(hidden, weight, cos, sin)


def qkv_back_kernel(heads, pack_ref, dgate_ref, w_ref, cos_ref, sin_ref, mixed_ref, hid_ref):
    clip, quarter = pl.program_id(0), pl.program_id(1)
    width = heads * 64
    cos, sin = cos_ref[...], sin_ref[...]
    rows = cos.shape[0]
    half = rows // 2
    low_half = low_lanes((half, LANES))
    query_set = jnp.where((quarter == 0) | (quarter == 3), 0, 1)
    slot = quarter // 2
    first = 2 + 2 * (quarter % 2)
    low = low_lanes((rows, LANES))
    for pair in range(heads // 2):
        even, odd = 2 * pair, 2 * pair + 1
        query_even = pack_ref[clip, even, query_set, slot].astype(F32)
        query_odd = pack_ref[clip, odd, query_set, slot].astype(F32)
        query = jnp.concatenate(
            [
                jnp.where(low_half, query_even, pltpu.roll(query_odd, 64, 1)),
                jnp.where(low_half, pltpu.roll(query_even, 64, 1), query_odd),
            ],
            axis=0,
        )
        both = []
        for head in (even, odd):
            both.append(
                jnp.concatenate(
                    [
                        pack_ref[clip, head, quarter // 2, first].astype(F32),
                        pack_ref[clip, head, quarter // 2, first + 1].astype(F32),
                    ],
                    axis=0,
                )
            )
        key = jnp.where(low, both[0], pltpu.roll(both[1], 64, 1))
        value = jnp.where(low, pltpu.roll(both[0], 64, 1), both[1])
        query = query * cos - swap_halves(query) * sin
        key = key * cos - swap_halves(key) * sin
        for part, values in enumerate((query, key, value)):
            start = part * width + pair * LANES
            mixed_ref[:, start : start + LANES] = values.astype(BF)
    mixed_ref[:, 3 * width :] = dgate_ref[...]
    hid_ref[...] = dot(mixed_ref[...], w_ref[...], 1, 1).astype(BF)


def qkv_back(pack, dgate, weight, cos, sin, clips, heads):
    tokens = dgate.shape[0]
    width = weight.shape[0]
    quarter = tokens // clips // 4
    one = pl.Buffered(1)
    return pl.pallas_call(
        partial(qkv_back_kernel, heads),
        grid=(clips, 4),
        in_specs=[
            pl.BlockSpec(pack.shape, lambda c, i: (0, 0, 0, 0, 0, 0), pipeline_mode=one),
            pl.BlockSpec((quarter, heads * 64), lambda c, i: (c * 4 + i, 0)),
            pl.BlockSpec(weight.shape, lambda c, i: (0, 0), pipeline_mode=one),
            pl.BlockSpec((quarter, LANES), lambda c, i: (i, 0)),
            pl.BlockSpec((quarter, LANES), lambda c, i: (i, 0)),
        ],
        out_specs=[
            pl.BlockSpec((quarter, 4 * heads * 64), lambda c, i: (c * 4 + i, 0)),
            pl.BlockSpec((quarter, width), lambda c, i: (c * 4 + i, 0)),
        ],
        out_shape=[
            jax.ShapeDtypeStruct((tokens, 4 * heads * 64), BF),
            jax.ShapeDtypeStruct((tokens, width), BF),
        ],
        compiler_params=pltpu.CompilerParams(
            dimension_semantics=("arbitrary", "arbitrary"), vmem_limit_bytes=48 * MIB
        ),
        name="qkv_back",
    )(pack, dgate, weight, cos, sin)


def unpack_pair(even, odd):
    low = low_lanes(even.shape)
    return jnp.concatenate(
        [
            jnp.where(low, even, pltpu.roll(odd, 64, 1)),
            jnp.where(low, pltpu.roll(even, 64, 1), odd),
        ],
        axis=0,
    )


def gate_kernel(heads, pack_ref, gate_ref, gated_ref, attended_ref):
    clip, quarter = pl.program_id(0), pl.program_id(1)
    query_set = jnp.where((quarter == 0) | (quarter == 3), 0, 1)
    slot = quarter // 2
    for pair in range(heads // 2):
        cut = slice(pair * LANES, (pair + 1) * LANES)
        attended = unpack_pair(
            pack_ref[clip, 2 * pair, query_set, slot].astype(F32),
            pack_ref[clip, 2 * pair + 1, query_set, slot].astype(F32),
        )
        attended_ref[:, cut] = attended.astype(BF)
        gated_ref[:, cut] = (attended * jax.nn.sigmoid(gate_ref[:, cut])).astype(BF)


def gate_forward(pack, gate, clips, heads):
    tokens = gate.shape[0]
    quarter = tokens // clips // 4
    block = pl.BlockSpec((quarter, heads * 64), lambda c, i: (c * 4 + i, 0))
    return pl.pallas_call(
        partial(gate_kernel, heads),
        grid=(clips, 4),
        in_specs=[
            pl.BlockSpec(pack.shape, lambda c, i: (0, 0, 0, 0, 0, 0), pipeline_mode=pl.Buffered(1)),
            block,
        ],
        out_specs=[block, block],
        out_shape=[jax.ShapeDtypeStruct((tokens, heads * 64), BF)] * 2,
        compiler_params=pltpu.CompilerParams(dimension_semantics=("arbitrary", "arbitrary")),
        name="gate_forward",
    )(pack, gate)


def gate_back_kernel(heads, grad_ref, gate_ref, attended_ref, pack_ref, dgate_ref):
    clip, quarter = pl.program_id(0), pl.program_id(1)
    query_set = jnp.where((quarter == 0) | (quarter == 3), 0, 1)
    slot = quarter // 2
    rows = grad_ref.shape[0]
    half = rows // 2
    low = low_lanes((half, LANES))
    for pair in range(heads // 2):
        cut = slice(pair * LANES, (pair + 1) * LANES)
        sig = jax.nn.sigmoid(gate_ref[:, cut])
        grad = grad_ref[:, cut].astype(F32)
        dgate = grad * attended_ref[:, cut].astype(F32) * sig * (1.0 - sig)
        dgate_ref[:, cut] = dgate.astype(BF)
        down = grad * sig
        turn = pltpu.roll(down, 64, 1)
        pack_ref[clip, 2 * pair, query_set, slot] = jnp.where(low, down[:half], turn[half:]).astype(
            BF
        )
        pack_ref[clip, 2 * pair + 1, query_set, slot] = jnp.where(
            low, turn[:half], down[half:]
        ).astype(BF)


def gate_back(grad, gate, attended, clips, heads):
    tokens = gate.shape[0]
    quarter = tokens // clips // 4
    block = pl.BlockSpec((quarter, heads * 64), lambda c, i: (c * 4 + i, 0))
    pack_shape = (clips, heads, 2, 2, quarter // 2, LANES)
    return pl.pallas_call(
        partial(gate_back_kernel, heads),
        grid=(clips, 4),
        in_specs=[block, block, block],
        out_specs=[pl.BlockSpec(pack_shape, lambda c, i: (0, 0, 0, 0, 0, 0)), block],
        out_shape=[
            jax.ShapeDtypeStruct(pack_shape, BF),
            jax.ShapeDtypeStruct((tokens, heads * 64), BF),
        ],
        compiler_params=pltpu.CompilerParams(dimension_semantics=("arbitrary", "arbitrary")),
        name="gate_back",
    )(grad, gate, attended)


def tile_index(step):
    core = lax.axis_index("row") % 2
    slot = step // 2
    quarter = jnp.where(core == 0, 3 * slot, 1 + slot)
    return 2 * quarter + step % 2


def frame_mask(tile, per_frame):
    key = lax.broadcasted_iota(jnp.int32, (tile, 1), 0) // per_frame
    query = lax.broadcasted_iota(jnp.int32, (1, tile), 1) // per_frame
    return key <= query


def attend_kernel(tile, per_frame, scale, q_ref, kv_ref, out_ref, out_t_ref, lse_ref, vt_ref):
    step = pl.program_id(0)
    steps_of = scale * LOG2E

    @pl.when(step == 0)
    def _():
        vt_ref[64:72, :] = jnp.ones((8, vt_ref.shape[1]), BF)

        @pl.loop(0, kv_ref.shape[0] // tile)
        def _(j):
            rows = pl.ds(pl.multiple_of(j * tile, tile), tile)
            vt_ref[0:64, rows] = kv_ref[rows, :].T[64:, :]

    low = low_lanes((tile, LANES))
    packed = q_ref[...].astype(F32)
    packed = jnp.where(step % 2 == 0, packed, pltpu.roll(packed, 64, 1))
    query = jnp.where(low, packed, 0.0).astype(BF)

    def advance(j, carry, masked):
        top, total = carry
        rows = pl.ds(pl.multiple_of(j * tile, tile), tile)
        scores = dot(kv_ref[rows, :], query, 1, 1) * steps_of
        if masked:
            scores = jnp.where(frame_mask(tile, per_frame), scores, -1e30)
        new_top = jnp.maximum(top, jnp.max(scores, axis=0, keepdims=True))
        probs = jnp.exp2(scores - new_top).astype(BF)
        total = total * jnp.exp2(top - new_top) + dot(vt_ref[:, rows], probs, 1, 0)
        return new_top, total

    last = tile_index(step)
    carry = (jnp.full((1, tile), -1e30, F32), jnp.zeros((72, tile), F32))
    carry = lax.fori_loop(0, last, lambda j, c: advance(j, c, False), carry)
    top, total = advance(last, carry, True)
    norm = total[64:65, :]
    lse_ref[0] = top + jnp.log2(norm)
    result = (total[:64, :] / norm).astype(BF)

    @pl.when(step % 2 == 0)
    def _():
        out_t_ref[0, 0:64, :] = result

    @pl.when(step % 2 == 1)
    def _():
        out_t_ref[0, 64:128, :] = result
        out_ref[...] = out_t_ref[0].T


def attend(queries, keys_values, tile, per_frame, scale):
    one = pl.Buffered(1)
    return pl.pallas_call(
        partial(attend_kernel, tile, per_frame, scale),
        grid=(4,),
        in_specs=[
            pl.BlockSpec((tile, LANES), lambda i: (i // 2, 0)),
            pl.BlockSpec(keys_values.shape, lambda i: (0, 0), pipeline_mode=one),
        ],
        out_specs=[
            pl.BlockSpec((tile, LANES), lambda i: (i // 2, 0)),
            pl.BlockSpec((1, LANES, tile), lambda i: (i // 2, 0, 0)),
            pl.BlockSpec((1, 1, tile), lambda i: (i, 0, 0)),
        ],
        out_shape=[
            jax.ShapeDtypeStruct((2 * tile, LANES), BF),
            jax.ShapeDtypeStruct((2, LANES, tile), BF),
            jax.ShapeDtypeStruct((4, 1, tile), F32),
        ],
        scratch_shapes=[pltpu.VMEM((72, keys_values.shape[0]), BF)],
        compiler_params=pltpu.CompilerParams(
            dimension_semantics=("arbitrary",), vmem_limit_bytes=60 * MIB
        ),
        cost_estimate=pl.CostEstimate(
            flops=20_000_000_000, bytes_accessed=8_000_000, transcendentals=20_000_000
        ),
        name="attend",
    )(queries, keys_values)


def attend_back_kernel(
    tile,
    width,
    per_frame,
    scale,
    q_ref,
    do_ref,
    lse_ref,
    out_t_ref,
    kv_ref,
    dq_ref,
    dkv_ref,
    kt_ref,
    acc_ref,
    dq_t_ref,
    delta_ref,
):
    step = pl.program_id(0)
    steps_of = scale * LOG2E

    @pl.when(step == 0)
    def _():
        @pl.loop(0, kv_ref.shape[0] // tile)
        def _(j):
            rows = pl.ds(pl.multiple_of(j * tile, tile), tile)
            kt_ref[:, rows] = kv_ref[rows, :].T[:64, :]
            acc_ref[rows, :] = jnp.zeros((tile, LANES), F32)

    @pl.when(step % 2 == 0)
    def _():
        prod = do_ref[...].astype(F32).T * out_t_ref[0].astype(F32)
        delta_ref[0] = jnp.sum(prod[:64], axis=0, keepdims=True)
        delta_ref[1] = jnp.sum(prod[64:], axis=0, keepdims=True)

    low = low_lanes((tile, LANES))
    first = step % 2 == 0
    packed = q_ref[...].astype(F32)
    packed = jnp.where(first, packed, pltpu.roll(packed, 64, 1))
    query = jnp.where(low, packed, 0.0).astype(BF)
    packed = do_ref[...].astype(F32)
    packed = jnp.where(first, pltpu.roll(packed, 64, 1), packed)
    down = jnp.where(low, 0.0, packed).astype(BF)
    lse = lse_ref[0]
    delta = delta_ref[step % 2]

    def advance(j, dq, masked):
        rows = pl.ds(pl.multiple_of(j * width, width), width)
        pieces = kv_ref[rows, :]
        probs = jnp.exp2(dot(pieces, query, 1, 1) * steps_of - lse)
        if masked is not None:
            key = lax.broadcasted_iota(jnp.int32, (width, 1), 0) + masked
            ask = lax.broadcasted_iota(jnp.int32, (1, tile), 1)
            probs = jnp.where(key // per_frame <= ask // per_frame, probs, 0.0)
        dscore = (probs * (dot(pieces, down, 1, 1) - delta)).astype(BF)
        acc_ref[rows, :] += dot(dscore, query, 1, 0) + dot(probs.astype(BF), down, 1, 0)
        return dq + dot(kt_ref[:, rows], dscore, 1, 0)

    last = tile_index(step)
    parts = tile // width
    dq = jnp.zeros((64, tile), F32)
    dq = lax.fori_loop(0, last * parts, lambda j, c: advance(j, c, None), dq)
    for part in range(parts):
        dq = advance(last * parts + part, dq, part * width)
    dq = dq * scale

    @pl.when(step % 2 == 0)
    def _():
        dq_t_ref[0:64, :] = dq

    @pl.when(step % 2 == 1)
    def _():
        dq_t_ref[64:128, :] = dq
        dq_ref[...] = dq_t_ref[...].T.astype(BF)

    @pl.when(step == 3)
    def _():
        @pl.loop(0, kv_ref.shape[0] // tile)
        def _(j):
            rows = pl.ds(pl.multiple_of(j * tile, tile), tile)
            total = acc_ref[rows, :]
            dkv_ref[rows, :] = jnp.where(low_lanes((tile, LANES)), total * scale, total).astype(BF)


def attend_back(queries, downs, lse, out_t, keys_values, tile, per_frame, scale):
    one = pl.Buffered(1)
    keys = keys_values.shape[0]
    packed = pl.BlockSpec((tile, LANES), lambda i: (i // 2, 0))
    whole = pl.BlockSpec(keys_values.shape, lambda i: (0, 0), pipeline_mode=one)
    return pl.pallas_call(
        partial(attend_back_kernel, tile, tile // 2, per_frame, scale),
        grid=(4,),
        in_specs=[
            packed,
            packed,
            pl.BlockSpec((1, 1, tile), lambda i: (i, 0, 0)),
            pl.BlockSpec((1, LANES, tile), lambda i: (i // 2, 0, 0)),
            whole,
        ],
        out_specs=[packed, pl.BlockSpec(keys_values.shape, lambda i: (0, 0))],
        out_shape=[
            jax.ShapeDtypeStruct((2 * tile, LANES), BF),
            jax.ShapeDtypeStruct(keys_values.shape, BF),
        ],
        scratch_shapes=[
            pltpu.VMEM((64, keys), BF),
            pltpu.VMEM((keys, LANES), F32),
            pltpu.VMEM((LANES, tile), F32),
            pltpu.VMEM((2, 1, tile), F32),
        ],
        compiler_params=pltpu.CompilerParams(
            dimension_semantics=("arbitrary",), vmem_limit_bytes=60 * MIB
        ),
        cost_estimate=pl.CostEstimate(
            flops=50_000_000_000, bytes_accessed=12_000_000, transcendentals=20_000_000
        ),
        name="attend_back",
    )(queries, downs, lse, out_t, keys_values)


def on_device(
    tokens,
    timesteps,
    noise_table,
    mod_weight,
    mod_bias,
    attn_in,
    out_weight,
    up_weight,
    down_weight,
    cotangent,
):
    clips, frames, rows_dev, grid_side, width = tokens.shape
    frame_index = lax.axis_index("frame")
    row_index = lax.axis_index("row")
    frame_devs, row_devs = lax.axis_size("frame"), lax.axis_size("row")
    core = row_index % 2
    clip_len = frames * frame_devs
    head_dim = width // HEADS
    heads = HEADS // frame_devs
    slice_width = width // frame_devs
    per_frame_dev = rows_dev * grid_side
    per_frame = grid_side * grid_side
    token_count = clips * frames * per_frame_dev
    group_count = token_count * frame_devs
    tile = clip_len // 8 * per_frame
    scale = head_dim ** (-0.5)
    step_count = noise_table.shape[0]
    assert head_dim == 64 and row_devs == 2 * clips * heads

    def gather_frames(values):
        full = lax.all_gather(values, "frame", axis=1, tiled=True)
        return full.reshape(group_count, values.shape[-1])

    def scatter_frames(values):
        parts = values.reshape(clips, frame_devs, frames * per_frame_dev, width)
        parts = jnp.transpose(parts, (1, 0, 2, 3)).reshape(group_count, width)
        return lax.psum_scatter(parts, "frame", scatter_dimension=0, tiled=True).reshape(
            tokens.shape
        )

    def take_slice(weight, groups):
        cut = weight.reshape(weight.shape[0], groups, frame_devs, -1)
        cut = lax.dynamic_index_in_dim(cut, frame_index, 2, keepdims=False)
        return cut.reshape(weight.shape[0], -1)

    weight_in = lax.all_gather(take_slice(attn_in, 4), "row", axis=0, tiled=True)

    steps_iota = lax.broadcasted_iota(jnp.int32, (1, 1, step_count), 2)
    one_hot = (timesteps[:, :, None] == steps_iota).astype(BF)
    embedding = jnp.einsum("cls,sd->cld", one_hot, noise_table, preferred_element_type=F32)
    silu_low = jax.nn.silu(embedding).astype(BF)
    mod_local = jnp.einsum(
        "cld,de->cle", silu_low, mod_weight, preferred_element_type=F32
    ) + mod_bias.astype(F32)
    modulation = lax.all_gather(mod_local.astype(BF), "row", axis=2, tiled=True).astype(F32)
    modulation = modulation.reshape(clips, frames, 6, 1, 1, width)
    shift_one, scale_one, gate_one, shift_two, scale_two, gate_two = [
        modulation[:, :, part] for part in range(6)
    ]

    frame_freq, row_freq, col_freq = [np.tile(t, 4) for t in rotary_freqs(head_dim // 2)]
    shape_three = (clip_len, rows_dev, grid_side, LANES)
    frame_pos = lax.broadcasted_iota(F32, shape_three, 0)
    row_pos = (row_index * rows_dev + lax.broadcasted_iota(jnp.int32, shape_three, 1)).astype(F32)
    col_pos = lax.broadcasted_iota(F32, shape_three, 2)
    angles = (frame_pos * frame_freq + row_pos * row_freq + col_pos * col_freq).reshape(-1, LANES)
    sign = np.where(np.arange(LANES) % 64 < 32, -1.0, 1.0).astype(np.float32)
    cosines = jnp.cos(angles)
    sines = jnp.sin(angles) * sign

    token_f = tokens.astype(F32)
    hidden_one, norm_one_pull = jax.vjp(modulate, token_f, shift_one, scale_one)
    hidden_group = gather_frames(hidden_one.astype(BF))

    grad_out = cotangent.astype(F32)
    grad_branch_two = (grad_out * gate_two).astype(BF)

    pack, gate_raw = qkv_project(hidden_group, weight_in, cosines, sines, clips, heads)

    def exchange(values):
        return lax.all_to_all(values, "row", split_axis=0, concat_axis=0, tiled=True)

    half = tile // row_devs
    pairs = [(r, r ^ 1) for r in range(row_devs)]

    def to_heads(packed, count):
        parts = packed.reshape(row_devs, count, -1, per_frame_dev, LANES)
        return jnp.transpose(parts, (1, 2, 0, 3, 4)).reshape(-1, LANES)

    def to_tokens(values, count):
        parts = values.reshape(count, -1, row_devs, per_frame_dev, LANES)
        return jnp.transpose(parts, (2, 0, 1, 3, 4)).reshape(row_devs, count, half, LANES)

    arrived = exchange(pack.reshape(row_devs, 6, half, LANES))
    queries = to_heads(arrived[:, :2], 2)
    own_half = to_heads(arrived[:, 2:], 4)
    other_half = lax.ppermute(own_half, "row", pairs)
    keys_values = jnp.where(
        core == 0,
        jnp.concatenate([own_half, other_half], axis=0),
        jnp.concatenate([other_half, own_half], axis=0),
    )

    rest = jnp.concatenate([out_weight, take_slice(up_weight, 1), take_slice(down_weight, 1)], 1)
    rest = lax.all_gather(rest, "row", axis=0, tiled=True)
    full_out = rest[:, :width]
    weight_up = rest[:, width : width + up_weight.shape[1] // frame_devs]
    weight_down = rest[:, width + up_weight.shape[1] // frame_devs :]
    grad_two_group = gather_frames(grad_branch_two)

    attended_heads, attended_t, lse = attend(queries, keys_values, tile, per_frame, scale)
    pack_shape = (clips, heads, 2, 2, half, LANES)
    arrived = exchange(to_tokens(attended_heads, 2)).reshape(pack_shape)
    gated_group, attended = gate_forward(arrived, gate_raw, clips, heads)

    def group_split(values):
        parts = values.reshape(clips, frame_devs, frames * per_frame_dev, slice_width)
        parts = jnp.transpose(parts, (1, 0, 2, 3))
        return parts.reshape(frame_devs, token_count, slice_width)

    def group_join(values):
        parts = values.reshape(frame_devs, clips, frames * per_frame_dev, slice_width)
        return jnp.transpose(parts, (1, 0, 2, 3)).reshape(group_count, slice_width)

    gated = lax.all_to_all(group_split(gated_group), "frame", 0, 0, tiled=True)
    gated = jnp.transpose(gated, (1, 0, 2)).reshape(token_count, width)
    branch_one = jnp.dot(gated, full_out, preferred_element_type=F32).reshape(tokens.shape)
    after_one = token_f + gate_one * branch_one
    hidden_two, norm_two_pull = jax.vjp(modulate, after_one, shift_two, scale_two)
    hidden_two_group = gather_frames(hidden_two.astype(BF))

    pre_act = jnp.dot(hidden_two_group, weight_up, preferred_element_type=F32)
    act_values, gelu_pull = jax.vjp(partial(jax.nn.gelu, approximate=True), pre_act)
    act_low = act_values.astype(BF)
    grad_act = jnp.dot(grad_two_group, weight_down, preferred_element_type=F32)
    (grad_pre,) = gelu_pull(grad_act)
    grad_pre = grad_pre.astype(BF)
    grad_hidden_two = scatter_frames(dot(grad_pre, weight_up, 1, 1).astype(BF)).astype(F32)
    branch_two = scatter_frames(dot(act_low, weight_down, 1, 1).astype(BF)).astype(F32)
    mixed = (after_one + gate_two * branch_two).astype(BF)
    grad_gate_two = jnp.sum(grad_out * branch_two, axis=(2, 3), keepdims=True)

    grad_after_part, grad_shift_two, grad_scale_two = norm_two_pull(grad_hidden_two)
    grad_after = grad_out + grad_after_part
    grad_gate_one = jnp.sum(grad_after * branch_one, axis=(2, 3), keepdims=True)
    grad_branch_one = (grad_after * gate_one).astype(BF).reshape(token_count, width)
    grad_gated = dot(grad_branch_one, full_out, 1, 1).astype(BF)
    grad_gated = jnp.transpose(
        grad_gated.reshape(token_count, frame_devs, slice_width), (1, 0, 2)
    )
    grad_gated = group_join(lax.all_to_all(grad_gated, "frame", 0, 0, tiled=True))
    down_pack, grad_gate = gate_back(grad_gated, gate_raw, attended, clips, heads)
    downs = to_heads(exchange(down_pack.reshape(row_devs, 2, half, LANES)), 2)

    mlp_grads = jnp.concatenate(
        [
            dot(hidden_two_group, grad_pre, 0, 0),
            dot(grad_two_group, act_low, 0, 0),
            dot(gated, grad_branch_one, 0, 0),
        ],
        axis=1,
    ).astype(BF)
    mlp_grads = lax.psum_scatter(mlp_grads, "row", scatter_dimension=0, tiled=True)

    grad_queries, grad_kv = attend_back(
        queries, downs, lse, attended_t, keys_values, tile, per_frame, scale
    )
    grad_kv = grad_kv.reshape(2, -1, LANES)
    keep = lax.dynamic_index_in_dim(grad_kv, core, 0, keepdims=False)
    give = lax.dynamic_index_in_dim(grad_kv, 1 - core, 0, keepdims=False)
    got = lax.ppermute(give, "row", pairs)
    grad_kv = (keep.astype(F32) + got.astype(F32)).astype(BF)
    back_pack = jnp.concatenate([to_tokens(grad_queries, 2), to_tokens(grad_kv, 4)], axis=1)
    back_pack = exchange(back_pack).reshape(clips, heads, 2, 6, half, LANES)
    grad_mixed, grad_hidden = qkv_back(
        back_pack, grad_gate, weight_in, cosines, sines, clips, heads
    )
    grad_hidden_one = scatter_frames(grad_hidden).astype(F32)
    in_grad = lax.psum_scatter(
        dot(hidden_group, grad_mixed, 0, 0).astype(BF), "row", scatter_dimension=0, tiled=True
    )

    grad_token_part, grad_shift_one, grad_scale_one = norm_one_pull(grad_hidden_one)
    tokens_grad = (grad_after + grad_token_part).astype(BF)

    grad_mod = jnp.stack(
        [
            grad_shift_one,
            grad_scale_one,
            grad_gate_one,
            grad_shift_two,
            grad_scale_two,
            grad_gate_two,
        ],
        axis=2,
    ).reshape(clips * frames, 6 * width)
    grad_mod = lax.psum_scatter(grad_mod, "row", scatter_dimension=1, tiled=True).astype(BF)
    grad_mod_all = lax.all_gather(grad_mod, "frame", axis=0, tiled=True)
    steps_all = lax.all_gather(timesteps.reshape(-1), "frame", axis=0, tiled=True)
    hot_all = steps_all[:, None] == lax.broadcasted_iota(jnp.int32, (1, step_count), 1)
    embed_all = jnp.dot(hot_all.astype(BF), noise_table, preferred_element_type=F32)
    silu_all, silu_pull = jax.vjp(jax.nn.silu, embed_all)
    mod_weight_grad = dot(silu_all.astype(BF), grad_mod_all, 0, 0)
    mod_bias_grad = jnp.sum(grad_mod_all.astype(F32), axis=0)
    grad_silu = lax.psum(dot(grad_mod_all, mod_weight, 1, 1), "row")
    (grad_embedding,) = silu_pull(grad_silu)
    noise_table_grad = lax.dot_general(
        hot_all.astype(F32),
        grad_embedding,
        (((0,), (0,)), ((), ())),
        precision=lax.Precision.HIGHEST,
    )

    hidden_slice = up_weight.shape[1] // frame_devs
    up_part, down_part = mlp_grads[:, :hidden_slice], mlp_grads[:, hidden_slice : 2 * hidden_slice]
    out_weight_grad = lax.psum(mlp_grads[:, 2 * hidden_slice :], "frame").astype(F32)
    mlp_all = lax.all_gather(jnp.stack([up_part, down_part]), "frame", axis=0, tiled=False)

    def join_columns(parts):
        return jnp.transpose(parts, (1, 0, 2)).reshape(parts.shape[1], -1).astype(F32)

    up_weight_grad = join_columns(mlp_all[:, 0])
    down_weight_grad = join_columns(mlp_all[:, 1])
    in_all = lax.all_gather(in_grad, "frame", axis=0, tiled=False)
    in_all = in_all.reshape(frame_devs, in_grad.shape[0], 4, slice_width)
    attn_in_grad = jnp.transpose(in_all, (1, 2, 0, 3)).reshape(attn_in.shape).astype(F32)
    return (
        mixed,
        tokens_grad,
        noise_table_grad,
        mod_weight_grad,
        mod_bias_grad,
        attn_in_grad,
        out_weight_grad,
        up_weight_grad,
        down_weight_grad,
    )


def solution(mesh):
    in_specs = (
        P(None, "frame", "row", None, None),
        P(None, "frame"),
        P(),
        P(None, "row"),
        P("row"),
        P("row", None),
        P("row", None),
        P("row", None),
        P("row", None),
        P(None, "frame", "row", None, None),
    )
    out_specs = (
        P(None, "frame", "row", None, None),
        P(None, "frame", "row", None, None),
        P(),
        P(None, "row"),
        P("row"),
        P("row", None),
        P("row", None),
        P("row", None),
        P("row", None),
    )
    return jax.shard_map(
        on_device, mesh=mesh, in_specs=in_specs, out_specs=out_specs, check_vma=False
    )
```

```python
from functools import partial

import jax
import jax.numpy as jnp
import numpy as np
from jax import lax
from jax.experimental import pallas as pl
from jax.experimental.pallas import tpu as pltpu
from jax.sharding import PartitionSpec as P

HEADS = 16
EPS = 1e-06
LOG2E = 1.4426950408889634
F32 = jnp.float32
BF = jnp.bfloat16
LANES = 128
MIB = 1 << 20


def rotary_freqs(pair_count):
    third_count = pair_count // 3
    group_sizes = [pair_count - 2 * third_count, third_count, third_count]
    tables = []
    offset = 0
    for group_index in range(3):
        freq_table = np.zeros((pair_count,), np.float32)
        for inner_index in range(group_sizes[group_index]):
            freq_table[offset + inner_index] = 10000.0 ** (-inner_index / group_sizes[group_index])
        offset += group_sizes[group_index]
        tables.append(freq_table)
    return tables


def layer_norm(values):
    row_mean = jnp.mean(values, axis=-1, keepdims=True)
    centered = values - row_mean
    row_var = jnp.mean(centered * centered, axis=-1, keepdims=True)
    return centered * lax.rsqrt(row_var + EPS)


def modulate(values, shift, scale_part):
    return layer_norm(values) * (1.0 + scale_part) + shift


def dot(left, right, left_dim, right_dim):
    return lax.dot_general(
        left, right, (((left_dim,), (right_dim,)), ((), ())), preferred_element_type=F32
    )


def swap_halves(values):
    lane = lax.broadcasted_iota(jnp.int32, values.shape, 1)
    width = values.shape[1]
    return jnp.where(
        (lane % 64) < 32, pltpu.roll(values, width - 32, 1), pltpu.roll(values, 32, 1)
    )


def low_lanes(shape):
    return lax.broadcasted_iota(jnp.int32, shape, len(shape) - 1) < 64


def qkv_kernel(heads, hid_ref, w_ref, cos_ref, sin_ref, pack_ref, gate_ref):
    clip, quarter = pl.program_id(0), pl.program_id(1)
    width = heads * 64
    mixed = jnp.dot(hid_ref[...], w_ref[...], preferred_element_type=F32)
    cos, sin = cos_ref[...], sin_ref[...]
    rows = mixed.shape[0]
    half = rows // 2
    gate_ref[...] = mixed[:, 3 * width :]
    low = low_lanes((rows, LANES))
    low_half = low_lanes((half, LANES))
    query_set = jnp.where((quarter == 0) | (quarter == 3), 0, 1)
    slot = quarter // 2
    for pair in range(heads // 2):
        cut = slice(pair * LANES, (pair + 1) * LANES)
        query = mixed[:, cut]
        key = mixed[:, width + pair * LANES : width + (pair + 1) * LANES]
        value = mixed[:, 2 * width + pair * LANES : 2 * width + (pair + 1) * LANES]
        query = query * cos + swap_halves(query) * sin
        key = key * cos + swap_halves(key) * sin
        key_turn = pltpu.roll(key, 64, 1)
        value_turn = pltpu.roll(value, 64, 1)
        query_turn = pltpu.roll(query, 64, 1)
        packs = (
            (
                jnp.where(low, key, value_turn),
                jnp.where(low_half, query[:half], query_turn[half:]),
            ),
            (
                jnp.where(low, key_turn, value),
                jnp.where(low_half, query_turn[:half], query[half:]),
            ),
        )
        for inner, (key_value, queries) in enumerate(packs):
            head = 2 * pair + inner
            pack_ref[clip, head, query_set, slot] = queries.astype(BF)
            key_value = key_value.astype(BF)
            first = 2 + 2 * (quarter % 2)
            pack_ref[clip, head, quarter // 2, first] = key_value[:half]
            pack_ref[clip, head, quarter // 2, first + 1] = key_value[half:]


def qkv_project(hidden, weight, cos, sin, clips, heads):
    tokens, width = hidden.shape
    quarter = tokens // clips // 4
    one = pl.Buffered(1)
    return pl.pallas_call(
        partial(qkv_kernel, heads),
        grid=(clips, 4),
        in_specs=[
            pl.BlockSpec((quarter, width), lambda c, i: (c * 4 + i, 0)),
            pl.BlockSpec(weight.shape, lambda c, i: (0, 0), pipeline_mode=one),
            pl.BlockSpec((quarter, LANES), lambda c, i: (i, 0)),
            pl.BlockSpec((quarter, LANES), lambda c, i: (i, 0)),
        ],
        out_specs=[
            pl.BlockSpec(
                (clips, heads, 2, 6, quarter // 2, LANES), lambda c, i: (0, 0, 0, 0, 0, 0)
            ),
            pl.BlockSpec((quarter, heads * 64), lambda c, i: (c * 4 + i, 0)),
        ],
        out_shape=[
            jax.ShapeDtypeStruct((clips, heads, 2, 6, quarter // 2, LANES), BF),
            jax.ShapeDtypeStruct((tokens, heads * 64), F32),
        ],
        compiler_params=pltpu.CompilerParams(
            dimension_semantics=("arbitrary", "arbitrary"), vmem_limit_bytes=48 * MIB
        ),
        name="qkv_project",
    )(hidden, weight, cos, sin)


def qkv_back_kernel(heads, pack_ref, dgate_ref, w_ref, cos_ref, sin_ref, mixed_ref, hid_ref):
    clip, quarter = pl.program_id(0), pl.program_id(1)
    width = heads * 64
    cos, sin = cos_ref[...], sin_ref[...]
    rows = cos.shape[0]
    half = rows // 2
    low_half = low_lanes((half, LANES))
    query_set = jnp.where((quarter == 0) | (quarter == 3), 0, 1)
    slot = quarter // 2
    first = 2 + 2 * (quarter % 2)
    low = low_lanes((rows, LANES))
    for pair in range(heads // 2):
        even, odd = 2 * pair, 2 * pair + 1
        query_even = pack_ref[clip, even, query_set, slot].astype(F32)
        query_odd = pack_ref[clip, odd, query_set, slot].astype(F32)
        query = jnp.concatenate(
            [
                jnp.where(low_half, query_even, pltpu.roll(query_odd, 64, 1)),
                jnp.where(low_half, pltpu.roll(query_even, 64, 1), query_odd),
            ],
            axis=0,
        )
        both = []
        for head in (even, odd):
            both.append(
                jnp.concatenate(
                    [
                        pack_ref[clip, head, quarter // 2, first].astype(F32),
                        pack_ref[clip, head, quarter // 2, first + 1].astype(F32),
                    ],
                    axis=0,
                )
            )
        key = jnp.where(low, both[0], pltpu.roll(both[1], 64, 1))
        value = jnp.where(low, pltpu.roll(both[0], 64, 1), both[1])
        query = query * cos - swap_halves(query) * sin
        key = key * cos - swap_halves(key) * sin
        for part, values in enumerate((query, key, value)):
            start = part * width + pair * LANES
            mixed_ref[:, start : start + LANES] = values.astype(BF)
    mixed_ref[:, 3 * width :] = dgate_ref[...]
    hid_ref[...] = dot(mixed_ref[...], w_ref[...], 1, 1).astype(BF)


def qkv_back(pack, dgate, weight, cos, sin, clips, heads):
    tokens = dgate.shape[0]
    width = weight.shape[0]
    quarter = tokens // clips // 4
    one = pl.Buffered(1)
    return pl.pallas_call(
        partial(qkv_back_kernel, heads),
        grid=(clips, 4),
        in_specs=[
            pl.BlockSpec(pack.shape, lambda c, i: (0, 0, 0, 0, 0, 0), pipeline_mode=one),
            pl.BlockSpec((quarter, heads * 64), lambda c, i: (c * 4 + i, 0)),
            pl.BlockSpec(weight.shape, lambda c, i: (0, 0), pipeline_mode=one),
            pl.BlockSpec((quarter, LANES), lambda c, i: (i, 0)),
            pl.BlockSpec((quarter, LANES), lambda c, i: (i, 0)),
        ],
        out_specs=[
            pl.BlockSpec((quarter, 4 * heads * 64), lambda c, i: (c * 4 + i, 0)),
            pl.BlockSpec((quarter, width), lambda c, i: (c * 4 + i, 0)),
        ],
        out_shape=[
            jax.ShapeDtypeStruct((tokens, 4 * heads * 64), BF),
            jax.ShapeDtypeStruct((tokens, width), BF),
        ],
        compiler_params=pltpu.CompilerParams(
            dimension_semantics=("arbitrary", "arbitrary"), vmem_limit_bytes=48 * MIB
        ),
        name="qkv_back",
    )(pack, dgate, weight, cos, sin)


def unpack_pair(even, odd):
    low = low_lanes(even.shape)
    return jnp.concatenate(
        [
            jnp.where(low, even, pltpu.roll(odd, 64, 1)),
            jnp.where(low, pltpu.roll(even, 64, 1), odd),
        ],
        axis=0,
    )


def gate_kernel(heads, pack_ref, gate_ref, gated_ref, attended_ref):
    clip, quarter = pl.program_id(0), pl.program_id(1)
    query_set = jnp.where((quarter == 0) | (quarter == 3), 0, 1)
    slot = quarter // 2
    for pair in range(heads // 2):
        cut = slice(pair * LANES, (pair + 1) * LANES)
        attended = unpack_pair(
            pack_ref[clip, 2 * pair, query_set, slot].astype(F32),
            pack_ref[clip, 2 * pair + 1, query_set, slot].astype(F32),
        )
        attended_ref[:, cut] = attended.astype(BF)
        gated_ref[:, cut] = (attended * jax.nn.sigmoid(gate_ref[:, cut])).astype(BF)


def gate_forward(pack, gate, clips, heads):
    tokens = gate.shape[0]
    quarter = tokens // clips // 4
    block = pl.BlockSpec((quarter, heads * 64), lambda c, i: (c * 4 + i, 0))
    return pl.pallas_call(
        partial(gate_kernel, heads),
        grid=(clips, 4),
        in_specs=[
            pl.BlockSpec(pack.shape, lambda c, i: (0, 0, 0, 0, 0, 0), pipeline_mode=pl.Buffered(1)),
            block,
        ],
        out_specs=[block, block],
        out_shape=[jax.ShapeDtypeStruct((tokens, heads * 64), BF)] * 2,
        compiler_params=pltpu.CompilerParams(dimension_semantics=("arbitrary", "arbitrary")),
        name="gate_forward",
    )(pack, gate)


def gate_back_kernel(heads, grad_ref, gate_ref, attended_ref, pack_ref, dgate_ref):
    clip, quarter = pl.program_id(0), pl.program_id(1)
    query_set = jnp.where((quarter == 0) | (quarter == 3), 0, 1)
    slot = quarter // 2
    rows = grad_ref.shape[0]
    half = rows // 2
    low = low_lanes((half, LANES))
    for pair in range(heads // 2):
        cut = slice(pair * LANES, (pair + 1) * LANES)
        sig = jax.nn.sigmoid(gate_ref[:, cut])
        grad = grad_ref[:, cut].astype(F32)
        dgate = grad * attended_ref[:, cut].astype(F32) * sig * (1.0 - sig)
        dgate_ref[:, cut] = dgate.astype(BF)
        down = grad * sig
        turn = pltpu.roll(down, 64, 1)
        pack_ref[clip, 2 * pair, query_set, slot] = jnp.where(low, down[:half], turn[half:]).astype(
            BF
        )
        pack_ref[clip, 2 * pair + 1, query_set, slot] = jnp.where(
            low, turn[:half], down[half:]
        ).astype(BF)


def gate_back(grad, gate, attended, clips, heads):
    tokens = gate.shape[0]
    quarter = tokens // clips // 4
    block = pl.BlockSpec((quarter, heads * 64), lambda c, i: (c * 4 + i, 0))
    pack_shape = (clips, heads, 2, 2, quarter // 2, LANES)
    return pl.pallas_call(
        partial(gate_back_kernel, heads),
        grid=(clips, 4),
        in_specs=[block, block, block],
        out_specs=[pl.BlockSpec(pack_shape, lambda c, i: (0, 0, 0, 0, 0, 0)), block],
        out_shape=[
            jax.ShapeDtypeStruct(pack_shape, BF),
            jax.ShapeDtypeStruct((tokens, heads * 64), BF),
        ],
        compiler_params=pltpu.CompilerParams(dimension_semantics=("arbitrary", "arbitrary")),
        name="gate_back",
    )(grad, gate, attended)


def tile_index(step):
    core = lax.axis_index("row") % 2
    slot = step // 2
    quarter = jnp.where(core == 0, 3 * slot, 1 + slot)
    return 2 * quarter + step % 2


def frame_mask(tile, per_frame):
    key = lax.broadcasted_iota(jnp.int32, (tile, 1), 0) // per_frame
    query = lax.broadcasted_iota(jnp.int32, (1, tile), 1) // per_frame
    return key <= query


def attend_kernel(tile, per_frame, scale, q_ref, kv_ref, out_ref, out_t_ref, lse_ref, vt_ref):
    step = pl.program_id(0)
    steps_of = scale * LOG2E

    @pl.when(step == 0)
    def _():
        vt_ref[64:72, :] = jnp.ones((8, vt_ref.shape[1]), BF)

        @pl.loop(0, kv_ref.shape[0] // tile)
        def _(j):
            rows = pl.ds(pl.multiple_of(j * tile, tile), tile)
            vt_ref[0:64, rows] = kv_ref[rows, :].T[64:, :]

    low = low_lanes((tile, LANES))
    packed = q_ref[...].astype(F32)
    packed = jnp.where(step % 2 == 0, packed, pltpu.roll(packed, 64, 1))
    query = jnp.where(low, packed, 0.0).astype(BF)

    def advance(j, carry, masked):
        top, total = carry
        rows = pl.ds(pl.multiple_of(j * tile, tile), tile)
        scores = dot(kv_ref[rows, :], query, 1, 1) * steps_of
        if masked:
            scores = jnp.where(frame_mask(tile, per_frame), scores, -1e30)
        new_top = jnp.maximum(top, jnp.max(scores, axis=0, keepdims=True))
        probs = jnp.exp2(scores - new_top).astype(BF)
        total = total * jnp.exp2(top - new_top) + dot(vt_ref[:, rows], probs, 1, 0)
        return new_top, total

    last = tile_index(step)
    carry = (jnp.full((1, tile), -1e30, F32), jnp.zeros((72, tile), F32))
    carry = lax.fori_loop(0, last, lambda j, c: advance(j, c, False), carry)
    top, total = advance(last, carry, True)
    norm = total[64:65, :]
    lse_ref[0] = top + jnp.log2(norm)
    result = (total[:64, :] / norm).astype(BF)

    @pl.when(step % 2 == 0)
    def _():
        out_t_ref[0, 0:64, :] = result

    @pl.when(step % 2 == 1)
    def _():
        out_t_ref[0, 64:128, :] = result
        out_ref[...] = out_t_ref[0].T


def attend(queries, keys_values, tile, per_frame, scale):
    one = pl.Buffered(1)
    return pl.pallas_call(
        partial(attend_kernel, tile, per_frame, scale),
        grid=(4,),
        in_specs=[
            pl.BlockSpec((tile, LANES), lambda i: (i // 2, 0)),
            pl.BlockSpec(keys_values.shape, lambda i: (0, 0), pipeline_mode=one),
        ],
        out_specs=[
            pl.BlockSpec((tile, LANES), lambda i: (i // 2, 0)),
            pl.BlockSpec((1, LANES, tile), lambda i: (i // 2, 0, 0)),
            pl.BlockSpec((1, 1, tile), lambda i: (i, 0, 0)),
        ],
        out_shape=[
            jax.ShapeDtypeStruct((2 * tile, LANES), BF),
            jax.ShapeDtypeStruct((2, LANES, tile), BF),
            jax.ShapeDtypeStruct((4, 1, tile), F32),
        ],
        scratch_shapes=[pltpu.VMEM((72, keys_values.shape[0]), BF)],
        compiler_params=pltpu.CompilerParams(
            dimension_semantics=("arbitrary",), vmem_limit_bytes=60 * MIB
        ),
        cost_estimate=pl.CostEstimate(
            flops=20_000_000_000, bytes_accessed=8_000_000, transcendentals=20_000_000
        ),
        name="attend",
    )(queries, keys_values)


def attend_back_kernel(
    tile,
    width,
    per_frame,
    scale,
    q_ref,
    do_ref,
    lse_ref,
    out_t_ref,
    kv_ref,
    dq_ref,
    dkv_ref,
    kt_ref,
    acc_ref,
    dq_t_ref,
    delta_ref,
):
    step = pl.program_id(0)
    steps_of = scale * LOG2E

    @pl.when(step == 0)
    def _():
        @pl.loop(0, kv_ref.shape[0] // tile)
        def _(j):
            rows = pl.ds(pl.multiple_of(j * tile, tile), tile)
            kt_ref[:, rows] = kv_ref[rows, :].T[:64, :]
            acc_ref[rows, :] = jnp.zeros((tile, LANES), F32)

    @pl.when(step % 2 == 0)
    def _():
        prod = do_ref[...].astype(F32).T * out_t_ref[0].astype(F32)
        delta_ref[0] = jnp.sum(prod[:64], axis=0, keepdims=True)
        delta_ref[1] = jnp.sum(prod[64:], axis=0, keepdims=True)

    low = low_lanes((tile, LANES))
    first = step % 2 == 0
    packed = q_ref[...].astype(F32)
    packed = jnp.where(first, packed, pltpu.roll(packed, 64, 1))
    query = jnp.where(low, packed, 0.0).astype(BF)
    packed = do_ref[...].astype(F32)
    packed = jnp.where(first, pltpu.roll(packed, 64, 1), packed)
    down = jnp.where(low, 0.0, packed).astype(BF)
    lse = lse_ref[0]
    delta = delta_ref[step % 2]

    def advance(j, dq, masked):
        rows = pl.ds(pl.multiple_of(j * width, width), width)
        pieces = kv_ref[rows, :]
        probs = jnp.exp2(dot(pieces, query, 1, 1) * steps_of - lse)
        if masked is not None:
            key = lax.broadcasted_iota(jnp.int32, (width, 1), 0) + masked
            ask = lax.broadcasted_iota(jnp.int32, (1, tile), 1)
            probs = jnp.where(key // per_frame <= ask // per_frame, probs, 0.0)
        dscore = (probs * (dot(pieces, down, 1, 1) - delta)).astype(BF)
        acc_ref[rows, :] += dot(dscore, query, 1, 0) + dot(probs.astype(BF), down, 1, 0)
        return dq + dot(kt_ref[:, rows], dscore, 1, 0)

    last = tile_index(step)
    parts = tile // width
    dq = jnp.zeros((64, tile), F32)
    dq = lax.fori_loop(0, last * parts, lambda j, c: advance(j, c, None), dq)
    for part in range(parts):
        dq = advance(last * parts + part, dq, part * width)
    dq = dq * scale

    @pl.when(step % 2 == 0)
    def _():
        dq_t_ref[0:64, :] = dq

    @pl.when(step % 2 == 1)
    def _():
        dq_t_ref[64:128, :] = dq
        dq_ref[...] = dq_t_ref[...].T.astype(BF)

    @pl.when(step == 3)
    def _():
        @pl.loop(0, kv_ref.shape[0] // tile)
        def _(j):
            rows = pl.ds(pl.multiple_of(j * tile, tile), tile)
            total = acc_ref[rows, :]
            dkv_ref[rows, :] = jnp.where(low_lanes((tile, LANES)), total * scale, total).astype(BF)


def attend_back(queries, downs, lse, out_t, keys_values, tile, per_frame, scale):
    one = pl.Buffered(1)
    keys = keys_values.shape[0]
    packed = pl.BlockSpec((tile, LANES), lambda i: (i // 2, 0))
    whole = pl.BlockSpec(keys_values.shape, lambda i: (0, 0), pipeline_mode=one)
    return pl.pallas_call(
        partial(attend_back_kernel, tile, tile // 2, per_frame, scale),
        grid=(4,),
        in_specs=[
            packed,
            packed,
            pl.BlockSpec((1, 1, tile), lambda i: (i, 0, 0)),
            pl.BlockSpec((1, LANES, tile), lambda i: (i // 2, 0, 0)),
            whole,
        ],
        out_specs=[packed, pl.BlockSpec(keys_values.shape, lambda i: (0, 0))],
        out_shape=[
            jax.ShapeDtypeStruct((2 * tile, LANES), BF),
            jax.ShapeDtypeStruct(keys_values.shape, BF),
        ],
        scratch_shapes=[
            pltpu.VMEM((64, keys), BF),
            pltpu.VMEM((keys, LANES), F32),
            pltpu.VMEM((LANES, tile), F32),
            pltpu.VMEM((2, 1, tile), F32),
        ],
        compiler_params=pltpu.CompilerParams(
            dimension_semantics=("arbitrary",), vmem_limit_bytes=60 * MIB
        ),
        cost_estimate=pl.CostEstimate(
            flops=50_000_000_000, bytes_accessed=12_000_000, transcendentals=20_000_000
        ),
        name="attend_back",
    )(queries, downs, lse, out_t, keys_values)


def exchange_kernel(axis, moves, sources, results, pair_of, finish, *refs):
    in_refs, refs = refs[:sources], refs[sources:]
    out_refs, refs = refs[:results], refs[results:]
    send_sem, recv_sem, own_sem = refs[-3:]
    scratch = refs[:-3]
    dests = scratch if finish is not None else out_refs
    me, count = lax.axis_index(axis), lax.axis_size(axis)
    barrier = pltpu.get_barrier_semaphore()
    for step in range(1, count):
        pl.semaphore_signal(
            barrier,
            inc=1,
            device_id={axis: lax.rem(me + step, count)},
            device_id_type=pl.DeviceIdType.MESH,
        )
    pl.semaphore_wait(barrier, count - 1)
    copies = []
    for step in range(1, count):
        peer = lax.rem(me + step, count)
        for index, (source, dest, take, place) in enumerate(moves):
            copies.append(
                pltpu.make_async_remote_copy(
                    src_ref=take(in_refs[source], peer),
                    dst_ref=place(dests[dest], me, peer),
                    send_sem=send_sem.at[index, step - 1],
                    recv_sem=recv_sem.at[index, step - 1],
                    device_id={axis: peer},
                    device_id_type=pl.DeviceIdType.MESH,
                )
            )
            copies[-1].start()
    for index, (source, dest, take, place) in enumerate(moves):
        copies.append(
            pltpu.make_async_copy(
                take(in_refs[source], me), place(dests[dest], me, me), own_sem.at[index]
            )
        )
        copies[-1].start()
    for copy in copies:
        copy.wait()
    if pair_of is not None:
        core = lax.rem(me, 2)
        ref = dests[pair_of].at[core]
        copy = pltpu.make_async_remote_copy(
            src_ref=ref,
            dst_ref=ref,
            send_sem=own_sem.at[len(moves)],
            recv_sem=own_sem.at[len(moves) + 1],
            device_id={axis: me + 1 - 2 * core},
            device_id_type=pl.DeviceIdType.MESH,
        )
        copy.start()
        copy.wait()
    if finish is not None:
        finish(dests, out_refs)


def exchange(name, axis, number, moves, arrays, shapes, pair_of=None, finish=None, landing=()):
    count = lax.axis_size(axis)
    vmem = pl.BlockSpec(memory_space=pltpu.VMEM)
    sent = sum(a.size * a.dtype.itemsize for a in arrays)
    return pl.pallas_call(
        partial(exchange_kernel, axis, moves, len(arrays), len(shapes), pair_of, finish),
        in_specs=[vmem] * len(arrays),
        out_specs=[vmem] * len(shapes),
        out_shape=[jax.ShapeDtypeStruct(*shape) for shape in shapes],
        scratch_shapes=[pltpu.VMEM(*shape) for shape in landing]
        + [
            pltpu.SemaphoreType.DMA((len(moves), count - 1)),
            pltpu.SemaphoreType.DMA((len(moves), count - 1)),
            pltpu.SemaphoreType.DMA((len(moves) + 2,)),
        ],
        compiler_params=pltpu.CompilerParams(
            collective_id=number, has_side_effects=True, vmem_limit_bytes=40 * MIB
        ),
        cost_estimate=pl.CostEstimate(
            flops=0, bytes_accessed=20_000_000 + 30 * sent, transcendentals=0
        ),
        name=name,
    )(*arrays)


def all_of(ref, peer):
    return ref


def block_of(ref, peer):
    return ref.at[peer]


def at_sender(ref, me, peer):
    return ref.at[me]


def lanes_of(size):
    def view(ref, peer):
        return ref.at[:, pl.ds(pl.multiple_of(peer * size, LANES), size)]

    return view


def lanes_at(size):
    def view(ref, me, peer):
        return ref.at[:, pl.ds(pl.multiple_of(me * size, LANES), size)]

    return view


def add_landed(dests, out_refs):
    landed, out = dests[0], out_refs[0]
    rows = out.shape[0]
    step = 32 if rows % 32 == 0 else rows

    @pl.loop(0, rows // step)
    def _(j):
        cut = pl.ds(pl.multiple_of(j * step, step), step)
        total = landed[0, cut, :].astype(F32)
        for other in range(1, landed.shape[0]):
            total += landed[other, cut, :].astype(F32)
        out[cut, :] = total.astype(out.dtype)


def gather(name, axis, number, arrays):
    count = lax.axis_size(axis)
    moves = [(i, i, all_of, at_sender) for i in range(len(arrays))]
    return exchange(
        name, axis, number, moves, arrays, [((count,) + a.shape, a.dtype) for a in arrays]
    )


def scatter_sum(name, axis, number, parts, dtype=F32):
    return exchange(
        name,
        axis,
        number,
        [(0, 0, block_of, at_sender)],
        [parts],
        [(parts.shape[1:], dtype)],
        finish=add_landed,
        landing=[(parts.shape, parts.dtype)],
    )[0]


def mlp_grads_kernel(cut, *refs):
    out_ref = refs[-1]
    start = 0
    for part in range(len(refs) // 2):
        left, right = refs[2 * part], refs[2 * part + 1]
        columns = right.shape[1]
        result = dot(left[...], right[...], 0, 0).astype(BF)
        for block in range(out_ref.shape[0]):
            out_ref[block, :, start : start + columns] = result[block * cut : (block + 1) * cut]
        start += columns


def mlp_grads(pairs, row_devs):
    cut = pairs[0][0].shape[1] // row_devs
    block = max(cut, LANES)
    in_specs = []
    for left, right in pairs:
        in_specs.append(pl.BlockSpec((left.shape[0], block), lambda i: (0, i)))
        in_specs.append(pl.BlockSpec(right.shape, lambda i: (0, 0), pipeline_mode=pl.Buffered(1)))
    columns = sum(right.shape[1] for _, right in pairs)
    return pl.pallas_call(
        partial(mlp_grads_kernel, cut),
        grid=(row_devs * cut // block,),
        in_specs=in_specs,
        out_specs=pl.BlockSpec((block // cut, cut, columns), lambda i: (i, 0, 0)),
        out_shape=jax.ShapeDtypeStruct((row_devs, cut, columns), BF),
        compiler_params=pltpu.CompilerParams(
            dimension_semantics=("arbitrary",), vmem_limit_bytes=48 * MIB
        ),
        cost_estimate=pl.CostEstimate(
            flops=5_000_000_000, bytes_accessed=18_000_000, transcendentals=0
        ),
        name="mlp_grads",
    )(*[array for pair in pairs for array in pair])


def on_device(
    tokens,
    timesteps,
    noise_table,
    mod_weight,
    mod_bias,
    attn_in,
    out_weight,
    up_weight,
    down_weight,
    cotangent,
):
    clips, frames, rows_dev, grid_side, width = tokens.shape
    frame_index = lax.axis_index("frame")
    row_index = lax.axis_index("row")
    frame_devs, row_devs = lax.axis_size("frame"), lax.axis_size("row")
    core = row_index % 2
    clip_len = frames * frame_devs
    head_dim = width // HEADS
    heads = HEADS // frame_devs
    slice_width = width // frame_devs
    per_frame_dev = rows_dev * grid_side
    per_frame = grid_side * grid_side
    token_count = clips * frames * per_frame_dev
    group_count = token_count * frame_devs
    tile = clip_len // 8 * per_frame
    scale = head_dim ** (-0.5)
    step_count = noise_table.shape[0]
    assert head_dim == 64 and row_devs == 2 * clips * heads

    def by_frames(values):
        parts = values.reshape(frame_devs, clips, frames * per_frame_dev, -1)
        return jnp.transpose(parts, (1, 0, 2, 3)).reshape(group_count, values.shape[-1])

    def to_frames(values):
        parts = values.reshape(clips, frame_devs, frames * per_frame_dev, -1)
        return jnp.transpose(parts, (1, 0, 2, 3)).reshape(frame_devs, token_count, -1)

    def gather_frames(values):
        full = lax.all_gather(values, "frame", axis=1, tiled=True)
        return full.reshape(group_count, values.shape[-1])

    def scatter_frames(values):
        parts = to_frames(values).reshape(group_count, width)
        return lax.psum_scatter(parts, "frame", scatter_dimension=0, tiled=True).reshape(
            tokens.shape
        )

    def take_slice(weight, groups):
        cut = weight.reshape(weight.shape[0], groups, frame_devs, -1)
        cut = lax.dynamic_index_in_dim(cut, frame_index, 2, keepdims=False)
        return cut.reshape(weight.shape[0], -1)

    weight_in = lax.all_gather(take_slice(attn_in, 4), "row", axis=0, tiled=True)

    steps_iota = lax.broadcasted_iota(jnp.int32, (1, 1, step_count), 2)
    one_hot = (timesteps[:, :, None] == steps_iota).astype(BF)
    embedding = jnp.einsum("cls,sd->cld", one_hot, noise_table, preferred_element_type=F32)
    silu_low = jax.nn.silu(embedding).astype(BF)
    mod_local = jnp.einsum(
        "cld,de->cle", silu_low, mod_weight, preferred_element_type=F32
    ) + mod_bias.astype(F32)
    mod_width = mod_local.shape[2]
    modulation = exchange(
        "gather_mod",
        "row",
        0,
        [(0, 0, all_of, lanes_at(mod_width))],
        [mod_local.astype(BF).reshape(clips * frames, mod_width)],
        [((clips * frames, mod_width * row_devs), BF)],
    )[0].astype(F32)
    modulation = modulation.reshape(clips, frames, 6, 1, 1, width)
    shift_one, scale_one, gate_one, shift_two, scale_two, gate_two = [
        modulation[:, :, part] for part in range(6)
    ]

    frame_freq, row_freq, col_freq = [np.tile(t, 4) for t in rotary_freqs(head_dim // 2)]
    shape_three = (clip_len, rows_dev, grid_side, LANES)
    frame_pos = lax.broadcasted_iota(F32, shape_three, 0)
    row_pos = (row_index * rows_dev + lax.broadcasted_iota(jnp.int32, shape_three, 1)).astype(F32)
    col_pos = lax.broadcasted_iota(F32, shape_three, 2)
    angles = (frame_pos * frame_freq + row_pos * row_freq + col_pos * col_freq).reshape(-1, LANES)
    sign = np.where(np.arange(LANES) % 64 < 32, -1.0, 1.0).astype(np.float32)
    cosines = jnp.cos(angles)
    sines = jnp.sin(angles) * sign

    token_f = tokens.astype(F32)
    hidden_one, norm_one_pull = jax.vjp(modulate, token_f, shift_one, scale_one)
    steps_wide = jnp.broadcast_to(timesteps.reshape(-1, 1), (clips * frames, LANES))
    hidden_parts, steps_parts = gather(
        "gather_one",
        "frame",
        1,
        [hidden_one.astype(BF).reshape(token_count, width), steps_wide],
    )
    hidden_group = by_frames(hidden_parts)

    grad_out = cotangent.astype(F32)
    grad_branch_two = (grad_out * gate_two).astype(BF)

    pack, gate_raw = qkv_project(hidden_group, weight_in, cosines, sines, clips, heads)

    half = tile // row_devs
    pairs = [(r, r ^ 1) for r in range(row_devs)]

    spans = half // per_frame_dev
    by_token = (spans, per_frame_dev, LANES)
    by_head = (spans, row_devs, per_frame_dev, LANES)

    def peer_rows(ref, peer):
        return ref.at[:, :, peer]

    queries, keys_values = exchange(
        "to_heads",
        "row",
        2,
        [
            (0, 0, lambda r, p: r.at[p, 0:2], lambda r, me, p: r.at[:, :, me]),
            (0, 1, lambda r, p: r.at[p, 2:6], lambda r, me, p: r.at[p % 2, :, :, me]),
        ],
        [pack.reshape((row_devs, 6) + by_token)],
        [((2,) + by_head, BF), ((2, 4) + by_head, BF)],
        pair_of=1,
    )
    queries = queries.reshape(-1, LANES)
    keys_values = keys_values.reshape(-1, LANES)

    rest = jnp.concatenate([out_weight, take_slice(up_weight, 1), take_slice(down_weight, 1)], 1)
    rest = lax.all_gather(rest, "row", axis=0, tiled=True)
    full_out = rest[:, :width]
    weight_up = rest[:, width : width + up_weight.shape[1] // frame_devs]
    weight_down = rest[:, width + up_weight.shape[1] // frame_devs :]
    grad_two_group = gather_frames(grad_branch_two)

    attended_heads, attended_t, lse = attend(queries, keys_values, tile, per_frame, scale)
    pack_shape = (clips, heads, 2, 2, half, LANES)
    (arrived,) = exchange(
        "to_tokens",
        "row",
        3,
        [(0, 0, peer_rows, at_sender)],
        [attended_heads.reshape((2,) + by_head)],
        [((row_devs, 2) + by_token, BF)],
    )
    arrived = arrived.reshape(pack_shape)
    gated_group, attended = gate_forward(arrived, gate_raw, clips, heads)

    (gated,) = exchange(
        "gated_back",
        "frame",
        4,
        [(0, 0, block_of, lanes_at(slice_width))],
        [to_frames(gated_group)],
        [((token_count, width), BF)],
    )
    branch_one = jnp.dot(gated, full_out, preferred_element_type=F32).reshape(tokens.shape)
    after_one = token_f + gate_one * branch_one
    hidden_two, norm_two_pull = jax.vjp(modulate, after_one, shift_two, scale_two)
    (hidden_two_parts,) = gather(
        "gather_two", "frame", 5, [hidden_two.astype(BF).reshape(token_count, width)]
    )
    hidden_two_group = by_frames(hidden_two_parts)

    pre_act = jnp.dot(hidden_two_group, weight_up, preferred_element_type=F32)
    act_values, gelu_pull = jax.vjp(partial(jax.nn.gelu, approximate=True), pre_act)
    act_low = act_values.astype(BF)
    grad_act = jnp.dot(grad_two_group, weight_down, preferred_element_type=F32)
    (grad_pre,) = gelu_pull(grad_act)
    grad_pre = grad_pre.astype(BF)
    grad_hidden_two = scatter_sum(
        "scatter_two", "frame", 6, to_frames(dot(grad_pre, weight_up, 1, 1).astype(BF))
    ).reshape(tokens.shape)
    branch_two = scatter_frames(dot(act_low, weight_down, 1, 1).astype(BF)).astype(F32)
    mixed = (after_one + gate_two * branch_two).astype(BF)
    grad_gate_two = jnp.sum(grad_out * branch_two, axis=(2, 3), keepdims=True)

    grad_after_part, grad_shift_two, grad_scale_two = norm_two_pull(grad_hidden_two)
    grad_after = grad_out + grad_after_part
    grad_gate_one = jnp.sum(grad_after * branch_one, axis=(2, 3), keepdims=True)
    grad_branch_one = (grad_after * gate_one).astype(BF).reshape(token_count, width)
    grad_gated = dot(grad_branch_one, full_out, 1, 1).astype(BF)
    (grad_gated,) = exchange(
        "grad_gated",
        "frame",
        7,
        [(0, 0, lanes_of(slice_width), at_sender)],
        [grad_gated],
        [((frame_devs, token_count, slice_width), BF)],
    )
    grad_gated = by_frames(grad_gated)
    down_pack, grad_gate = gate_back(grad_gated, gate_raw, attended, clips, heads)
    (downs,) = exchange(
        "grad_to_heads",
        "row",
        8,
        [(0, 0, block_of, lambda r, me, p: r.at[:, :, me])],
        [down_pack.reshape((row_devs, 2) + by_token)],
        [((2,) + by_head, BF)],
    )
    downs = downs.reshape(-1, LANES)

    weight_grads = mlp_grads(
        [(hidden_two_group, grad_pre), (grad_two_group, act_low), (gated, grad_branch_one)],
        row_devs,
    )
    downs, weight_grads = lax.optimization_barrier((downs, weight_grads))
    weight_grads = lax.psum_scatter(weight_grads, "row", scatter_dimension=0, tiled=True)

    grad_queries, grad_kv = attend_back(
        queries, downs, lse, attended_t, keys_values, tile, per_frame, scale
    )
    grad_kv = grad_kv.reshape(2, -1, LANES)
    keep = lax.dynamic_index_in_dim(grad_kv, core, 0, keepdims=False)
    give = lax.dynamic_index_in_dim(grad_kv, 1 - core, 0, keepdims=False)
    got = lax.ppermute(give, "row", pairs)
    grad_kv = (keep.astype(F32) + got.astype(F32)).astype(BF)
    (back_pack,) = exchange(
        "grad_to_tokens",
        "row",
        9,
        [
            (0, 0, peer_rows, lambda r, me, p: r.at[me, 0:2]),
            (1, 0, peer_rows, lambda r, me, p: r.at[me, 2:6]),
        ],
        [grad_queries.reshape((2,) + by_head), grad_kv.reshape((4,) + by_head)],
        [((row_devs, 6) + by_token, BF)],
    )
    back_pack = back_pack.reshape(clips, heads, 2, 6, half, LANES)
    grad_mixed, grad_hidden = qkv_back(
        back_pack, grad_gate, weight_in, cosines, sines, clips, heads
    )
    grad_mixed, weight_grads = lax.optimization_barrier((grad_mixed, weight_grads))
    grad_hidden_one = scatter_sum("scatter_one", "frame", 10, to_frames(grad_hidden)).reshape(
        tokens.shape
    )
    in_grad = lax.psum_scatter(
        dot(hidden_group, grad_mixed, 0, 0).astype(BF), "row", scatter_dimension=0, tiled=True
    )

    grad_token_part, grad_shift_one, grad_scale_one = norm_one_pull(grad_hidden_one)
    tokens_grad = (grad_after + grad_token_part).astype(BF)

    grad_mod = jnp.stack(
        [
            grad_shift_one,
            grad_scale_one,
            grad_gate_one,
            grad_shift_two,
            grad_scale_two,
            grad_gate_two,
        ],
        axis=2,
    ).reshape(clips * frames, 6 * width)
    grad_mod = jnp.transpose(
        grad_mod.reshape(clips * frames, row_devs, mod_width), (1, 0, 2)
    )
    grad_mod = scatter_sum("scatter_mod", "row", 11, grad_mod, BF)
    (grad_mod_all,) = gather("gather_grad_mod", "frame", 12, [grad_mod])
    grad_mod_all = grad_mod_all.reshape(-1, mod_width)
    steps_all = steps_parts.reshape(-1, LANES)[:, 0]
    hot_all = steps_all[:, None] == lax.broadcasted_iota(jnp.int32, (1, step_count), 1)
    embed_all = jnp.dot(hot_all.astype(BF), noise_table, preferred_element_type=F32)
    silu_all, silu_pull = jax.vjp(jax.nn.silu, embed_all)
    mod_weight_grad = dot(silu_all.astype(BF), grad_mod_all, 0, 0)
    mod_bias_grad = jnp.sum(grad_mod_all.astype(F32), axis=0)
    grad_silu = dot(grad_mod_all, mod_weight, 1, 1)
    frame_count, cut = grad_silu.shape[0], width // row_devs
    grad_silu = jnp.transpose(grad_silu.reshape(frame_count, row_devs, cut), (1, 0, 2))
    grad_silu = scatter_sum("scatter_silu", "row", 13, grad_silu)
    (grad_silu,) = gather("gather_silu", "row", 14, [grad_silu])
    grad_silu = jnp.transpose(grad_silu, (1, 0, 2)).reshape(frame_count, width)
    (grad_embedding,) = silu_pull(grad_silu)
    noise_table_grad = lax.dot_general(
        hot_all.astype(F32),
        grad_embedding,
        (((0,), (0,)), ((), ())),
        precision=lax.Precision.HIGHEST,
    )

    grads_all = lax.all_gather(weight_grads[0], "frame", axis=0, tiled=False)

    def join_columns(parts):
        return jnp.transpose(parts, (1, 0, 2)).reshape(parts.shape[1], -1).astype(F32)

    hidden_slice = up_weight.shape[1] // frame_devs
    up_weight_grad = join_columns(grads_all[:, :, :hidden_slice])
    down_weight_grad = join_columns(grads_all[:, :, hidden_slice : 2 * hidden_slice])
    out_weight_grad = jnp.sum(grads_all[:, :, 2 * hidden_slice :].astype(F32), axis=0)
    in_all = lax.all_gather(in_grad, "frame", axis=0, tiled=False)
    in_all = in_all.reshape(frame_devs, in_grad.shape[0], 4, slice_width)
    attn_in_grad = jnp.transpose(in_all, (1, 2, 0, 3)).reshape(attn_in.shape).astype(F32)
    return (
        mixed,
        tokens_grad,
        noise_table_grad,
        mod_weight_grad,
        mod_bias_grad,
        attn_in_grad,
        out_weight_grad,
        up_weight_grad,
        down_weight_grad,
    )


def solution(mesh):
    in_specs = (
        P(None, "frame", "row", None, None),
        P(None, "frame"),
        P(),
        P(None, "row"),
        P("row"),
        P("row", None),
        P("row", None),
        P("row", None),
        P("row", None),
        P(None, "frame", "row", None, None),
    )
    out_specs = (
        P(None, "frame", "row", None, None),
        P(None, "frame", "row", None, None),
        P(),
        P(None, "row"),
        P("row"),
        P("row", None),
        P("row", None),
        P("row", None),
        P("row", None),
    )
    return jax.shard_map(
        on_device, mesh=mesh, in_specs=in_specs, out_specs=out_specs, check_vma=False
    )
```

```python
from functools import partial

import jax
import jax.numpy as jnp
import numpy as np
from jax import lax
from jax.experimental import pallas as pl
from jax.experimental.pallas import tpu as pltpu
from jax.sharding import PartitionSpec as P

HEADS = 16
EPS = 1e-06
LOG2E = 1.4426950408889634
F32 = jnp.float32
BF = jnp.bfloat16
LANES = 128
MIB = 1 << 20


def rotary_freqs(pair_count):
    third_count = pair_count // 3
    group_sizes = [pair_count - 2 * third_count, third_count, third_count]
    tables = []
    offset = 0
    for group_index in range(3):
        freq_table = np.zeros((pair_count,), np.float32)
        for inner_index in range(group_sizes[group_index]):
            freq_table[offset + inner_index] = 10000.0 ** (-inner_index / group_sizes[group_index])
        offset += group_sizes[group_index]
        tables.append(freq_table)
    return tables


def layer_norm(values):
    row_mean = jnp.mean(values, axis=-1, keepdims=True)
    centered = values - row_mean
    row_var = jnp.mean(centered * centered, axis=-1, keepdims=True)
    return centered * lax.rsqrt(row_var + EPS)


def modulate(values, shift, scale_part):
    return layer_norm(values) * (1.0 + scale_part) + shift


def dot(left, right, left_dim, right_dim):
    return lax.dot_general(
        left, right, (((left_dim,), (right_dim,)), ((), ())), preferred_element_type=F32
    )


def swap_halves(values):
    lane = lax.broadcasted_iota(jnp.int32, values.shape, 1)
    width = values.shape[1]
    return jnp.where(
        (lane % 64) < 32, pltpu.roll(values, width - 32, 1), pltpu.roll(values, 32, 1)
    )


def low_lanes(shape):
    return lax.broadcasted_iota(jnp.int32, shape, len(shape) - 1) < 64


def qkv_kernel(heads, hid_ref, w_ref, cos_ref, sin_ref, pack_ref, gate_ref):
    clip, quarter = pl.program_id(0), pl.program_id(1)
    width = heads * 64
    mixed = jnp.dot(hid_ref[...], w_ref[...], preferred_element_type=F32)
    cos, sin = cos_ref[...], sin_ref[...]
    rows = mixed.shape[0]
    half = rows // 2
    gate_ref[...] = mixed[:, 3 * width :]
    low = low_lanes((rows, LANES))
    low_half = low_lanes((half, LANES))
    query_set = jnp.where((quarter == 0) | (quarter == 3), 0, 1)
    slot = quarter // 2
    for pair in range(heads // 2):
        cut = slice(pair * LANES, (pair + 1) * LANES)
        query = mixed[:, cut]
        key = mixed[:, width + pair * LANES : width + (pair + 1) * LANES]
        value = mixed[:, 2 * width + pair * LANES : 2 * width + (pair + 1) * LANES]
        query = query * cos + swap_halves(query) * sin
        key = key * cos + swap_halves(key) * sin
        key_turn = pltpu.roll(key, 64, 1)
        value_turn = pltpu.roll(value, 64, 1)
        query_turn = pltpu.roll(query, 64, 1)
        packs = (
            (
                jnp.where(low, key, value_turn),
                jnp.where(low_half, query[:half], query_turn[half:]),
            ),
            (
                jnp.where(low, key_turn, value),
                jnp.where(low_half, query_turn[:half], query[half:]),
            ),
        )
        for inner, (key_value, queries) in enumerate(packs):
            head = 2 * pair + inner
            pack_ref[clip, head, query_set, slot] = queries.astype(BF)
            key_value = key_value.astype(BF)
            first = 2 + 2 * (quarter % 2)
            pack_ref[clip, head, quarter // 2, first] = key_value[:half]
            pack_ref[clip, head, quarter // 2, first + 1] = key_value[half:]


def qkv_project(hidden, weight, cos, sin, clips, heads):
    tokens, width = hidden.shape
    quarter = tokens // clips // 4
    one = pl.Buffered(1)
    return pl.pallas_call(
        partial(qkv_kernel, heads),
        grid=(clips, 4),
        in_specs=[
            pl.BlockSpec((quarter, width), lambda c, i: (c * 4 + i, 0)),
            pl.BlockSpec(weight.shape, lambda c, i: (0, 0), pipeline_mode=one),
            pl.BlockSpec((quarter, LANES), lambda c, i: (i, 0)),
            pl.BlockSpec((quarter, LANES), lambda c, i: (i, 0)),
        ],
        out_specs=[
            pl.BlockSpec(
                (clips, heads, 2, 6, quarter // 2, LANES), lambda c, i: (0, 0, 0, 0, 0, 0)
            ),
            pl.BlockSpec((quarter, heads * 64), lambda c, i: (c * 4 + i, 0)),
        ],
        out_shape=[
            jax.ShapeDtypeStruct((clips, heads, 2, 6, quarter // 2, LANES), BF),
            jax.ShapeDtypeStruct((tokens, heads * 64), F32),
        ],
        compiler_params=pltpu.CompilerParams(
            dimension_semantics=("arbitrary", "arbitrary"), vmem_limit_bytes=48 * MIB
        ),
        name="qkv_project",
    )(hidden, weight, cos, sin)


def qkv_back_kernel(heads, pack_ref, dgate_ref, w_ref, cos_ref, sin_ref, mixed_ref, hid_ref):
    clip, quarter = pl.program_id(0), pl.program_id(1)
    width = heads * 64
    cos, sin = cos_ref[...], sin_ref[...]
    rows = cos.shape[0]
    half = rows // 2
    low_half = low_lanes((half, LANES))
    query_set = jnp.where((quarter == 0) | (quarter == 3), 0, 1)
    slot = quarter // 2
    first = 2 + 2 * (quarter % 2)
    low = low_lanes((rows, LANES))
    for pair in range(heads // 2):
        even, odd = 2 * pair, 2 * pair + 1
        query_even = pack_ref[clip, even, query_set, slot].astype(F32)
        query_odd = pack_ref[clip, odd, query_set, slot].astype(F32)
        query = jnp.concatenate(
            [
                jnp.where(low_half, query_even, pltpu.roll(query_odd, 64, 1)),
                jnp.where(low_half, pltpu.roll(query_even, 64, 1), query_odd),
            ],
            axis=0,
        )
        both = []
        for head in (even, odd):
            both.append(
                jnp.concatenate(
                    [
                        pack_ref[clip, head, quarter // 2, first].astype(F32),
                        pack_ref[clip, head, quarter // 2, first + 1].astype(F32),
                    ],
                    axis=0,
                )
            )
        key = jnp.where(low, both[0], pltpu.roll(both[1], 64, 1))
        value = jnp.where(low, pltpu.roll(both[0], 64, 1), both[1])
        query = query * cos - swap_halves(query) * sin
        key = key * cos - swap_halves(key) * sin
        for part, values in enumerate((query, key, value)):
            start = part * width + pair * LANES
            mixed_ref[:, start : start + LANES] = values.astype(BF)
    mixed_ref[:, 3 * width :] = dgate_ref[...]
    hid_ref[...] = dot(mixed_ref[...], w_ref[...], 1, 1).astype(BF)


def qkv_back(pack, dgate, weight, cos, sin, clips, heads):
    tokens = dgate.shape[0]
    width = weight.shape[0]
    quarter = tokens // clips // 4
    one = pl.Buffered(1)
    return pl.pallas_call(
        partial(qkv_back_kernel, heads),
        grid=(clips, 4),
        in_specs=[
            pl.BlockSpec(pack.shape, lambda c, i: (0, 0, 0, 0, 0, 0), pipeline_mode=one),
            pl.BlockSpec((quarter, heads * 64), lambda c, i: (c * 4 + i, 0)),
            pl.BlockSpec(weight.shape, lambda c, i: (0, 0), pipeline_mode=one),
            pl.BlockSpec((quarter, LANES), lambda c, i: (i, 0)),
            pl.BlockSpec((quarter, LANES), lambda c, i: (i, 0)),
        ],
        out_specs=[
            pl.BlockSpec((quarter, 4 * heads * 64), lambda c, i: (c * 4 + i, 0)),
            pl.BlockSpec((quarter, width), lambda c, i: (c * 4 + i, 0)),
        ],
        out_shape=[
            jax.ShapeDtypeStruct((tokens, 4 * heads * 64), BF),
            jax.ShapeDtypeStruct((tokens, width), BF),
        ],
        compiler_params=pltpu.CompilerParams(
            dimension_semantics=("arbitrary", "arbitrary"), vmem_limit_bytes=48 * MIB
        ),
        name="qkv_back",
    )(pack, dgate, weight, cos, sin)


def unpack_pair(even, odd):
    low = low_lanes(even.shape)
    return jnp.concatenate(
        [
            jnp.where(low, even, pltpu.roll(odd, 64, 1)),
            jnp.where(low, pltpu.roll(even, 64, 1), odd),
        ],
        axis=0,
    )


def gate_kernel(heads, pack_ref, gate_ref, gated_ref, attended_ref):
    clip, quarter = pl.program_id(0), pl.program_id(1)
    query_set = jnp.where((quarter == 0) | (quarter == 3), 0, 1)
    slot = quarter // 2
    for pair in range(heads // 2):
        cut = slice(pair * LANES, (pair + 1) * LANES)
        attended = unpack_pair(
            pack_ref[clip, 2 * pair, query_set, slot].astype(F32),
            pack_ref[clip, 2 * pair + 1, query_set, slot].astype(F32),
        )
        attended_ref[:, cut] = attended.astype(BF)
        gated_ref[:, cut] = (attended * jax.nn.sigmoid(gate_ref[:, cut])).astype(BF)


def gate_forward(pack, gate, clips, heads):
    tokens = gate.shape[0]
    quarter = tokens // clips // 4
    block = pl.BlockSpec((quarter, heads * 64), lambda c, i: (c * 4 + i, 0))
    return pl.pallas_call(
        partial(gate_kernel, heads),
        grid=(clips, 4),
        in_specs=[
            pl.BlockSpec(pack.shape, lambda c, i: (0, 0, 0, 0, 0, 0), pipeline_mode=pl.Buffered(1)),
            block,
        ],
        out_specs=[block, block],
        out_shape=[jax.ShapeDtypeStruct((tokens, heads * 64), BF)] * 2,
        compiler_params=pltpu.CompilerParams(dimension_semantics=("arbitrary", "arbitrary")),
        name="gate_forward",
    )(pack, gate)


def gate_back_kernel(heads, grad_ref, gate_ref, attended_ref, pack_ref, dgate_ref):
    clip, quarter = pl.program_id(0), pl.program_id(1)
    query_set = jnp.where((quarter == 0) | (quarter == 3), 0, 1)
    slot = quarter // 2
    rows = grad_ref.shape[0]
    half = rows // 2
    low = low_lanes((half, LANES))
    for pair in range(heads // 2):
        cut = slice(pair * LANES, (pair + 1) * LANES)
        sig = jax.nn.sigmoid(gate_ref[:, cut])
        grad = grad_ref[:, cut].astype(F32)
        dgate = grad * attended_ref[:, cut].astype(F32) * sig * (1.0 - sig)
        dgate_ref[:, cut] = dgate.astype(BF)
        down = grad * sig
        turn = pltpu.roll(down, 64, 1)
        pack_ref[clip, 2 * pair, query_set, slot] = jnp.where(low, down[:half], turn[half:]).astype(
            BF
        )
        pack_ref[clip, 2 * pair + 1, query_set, slot] = jnp.where(
            low, turn[:half], down[half:]
        ).astype(BF)


def gate_back(grad, gate, attended, clips, heads):
    tokens = gate.shape[0]
    quarter = tokens // clips // 4
    block = pl.BlockSpec((quarter, heads * 64), lambda c, i: (c * 4 + i, 0))
    pack_shape = (clips, heads, 2, 2, quarter // 2, LANES)
    return pl.pallas_call(
        partial(gate_back_kernel, heads),
        grid=(clips, 4),
        in_specs=[block, block, block],
        out_specs=[pl.BlockSpec(pack_shape, lambda c, i: (0, 0, 0, 0, 0, 0)), block],
        out_shape=[
            jax.ShapeDtypeStruct(pack_shape, BF),
            jax.ShapeDtypeStruct((tokens, heads * 64), BF),
        ],
        compiler_params=pltpu.CompilerParams(dimension_semantics=("arbitrary", "arbitrary")),
        name="gate_back",
    )(grad, gate, attended)


def tile_index(step):
    core = lax.axis_index("row") % 2
    slot = step // 2
    quarter = jnp.where(core == 0, 3 * slot, 1 + slot)
    return 2 * quarter + step % 2


def frame_mask(tile, per_frame):
    key = lax.broadcasted_iota(jnp.int32, (tile, 1), 0) // per_frame
    query = lax.broadcasted_iota(jnp.int32, (1, tile), 1) // per_frame
    return key <= query


def attend_kernel(tile, per_frame, scale, q_ref, kv_ref, out_ref, out_t_ref, lse_ref, vt_ref):
    step = pl.program_id(0)
    steps_of = scale * LOG2E

    @pl.when(step == 0)
    def _():
        vt_ref[64:72, :] = jnp.ones((8, vt_ref.shape[1]), BF)

        @pl.loop(0, kv_ref.shape[0] // tile)
        def _(j):
            rows = pl.ds(pl.multiple_of(j * tile, tile), tile)
            vt_ref[0:64, rows] = kv_ref[rows, :].T[64:, :]

    low = low_lanes((tile, LANES))
    packed = q_ref[...].astype(F32)
    packed = jnp.where(step % 2 == 0, packed, pltpu.roll(packed, 64, 1))
    query = jnp.where(low, packed, 0.0).astype(BF)

    def advance(j, carry, masked):
        top, total = carry
        rows = pl.ds(pl.multiple_of(j * tile, tile), tile)
        scores = dot(kv_ref[rows, :], query, 1, 1) * steps_of
        if masked:
            scores = jnp.where(frame_mask(tile, per_frame), scores, -1e30)
        new_top = jnp.maximum(top, jnp.max(scores, axis=0, keepdims=True))
        probs = jnp.exp2(scores - new_top).astype(BF)
        total = total * jnp.exp2(top - new_top) + dot(vt_ref[:, rows], probs, 1, 0)
        return new_top, total

    last = tile_index(step)
    carry = (jnp.full((1, tile), -1e30, F32), jnp.zeros((72, tile), F32))
    carry = lax.fori_loop(0, last, lambda j, c: advance(j, c, False), carry)
    top, total = advance(last, carry, True)
    norm = total[64:65, :]
    lse_ref[0] = top + jnp.log2(norm)
    result = (total[:64, :] / norm).astype(BF)

    @pl.when(step % 2 == 0)
    def _():
        out_t_ref[0, 0:64, :] = result

    @pl.when(step % 2 == 1)
    def _():
        out_t_ref[0, 64:128, :] = result
        out_ref[...] = out_t_ref[0].T


def attend(queries, keys_values, tile, per_frame, scale):
    one = pl.Buffered(1)
    return pl.pallas_call(
        partial(attend_kernel, tile, per_frame, scale),
        grid=(4,),
        in_specs=[
            pl.BlockSpec((tile, LANES), lambda i: (i // 2, 0)),
            pl.BlockSpec(keys_values.shape, lambda i: (0, 0), pipeline_mode=one),
        ],
        out_specs=[
            pl.BlockSpec((tile, LANES), lambda i: (i // 2, 0)),
            pl.BlockSpec((1, LANES, tile), lambda i: (i // 2, 0, 0)),
            pl.BlockSpec((1, 1, tile), lambda i: (i, 0, 0)),
        ],
        out_shape=[
            jax.ShapeDtypeStruct((2 * tile, LANES), BF),
            jax.ShapeDtypeStruct((2, LANES, tile), BF),
            jax.ShapeDtypeStruct((4, 1, tile), F32),
        ],
        scratch_shapes=[pltpu.VMEM((72, keys_values.shape[0]), BF)],
        compiler_params=pltpu.CompilerParams(
            dimension_semantics=("arbitrary",), vmem_limit_bytes=60 * MIB
        ),
        cost_estimate=pl.CostEstimate(
            flops=4_000_000_000, bytes_accessed=8_000_000, transcendentals=0
        ),
        name="attend",
    )(queries, keys_values)


def attend_back_kernel(
    tile,
    width,
    per_frame,
    scale,
    q_ref,
    do_ref,
    lse_ref,
    out_t_ref,
    kv_ref,
    dq_ref,
    dkv_ref,
    kt_ref,
    acc_ref,
    dq_t_ref,
    delta_ref,
):
    step = pl.program_id(0)
    steps_of = scale * LOG2E

    @pl.when(step == 0)
    def _():
        @pl.loop(0, kv_ref.shape[0] // tile)
        def _(j):
            rows = pl.ds(pl.multiple_of(j * tile, tile), tile)
            kt_ref[:, rows] = kv_ref[rows, :].T[:64, :]
            acc_ref[rows, :] = jnp.zeros((tile, LANES), F32)

    @pl.when(step % 2 == 0)
    def _():
        prod = do_ref[...].astype(F32).T * out_t_ref[0].astype(F32)
        delta_ref[0] = jnp.sum(prod[:64], axis=0, keepdims=True)
        delta_ref[1] = jnp.sum(prod[64:], axis=0, keepdims=True)

    low = low_lanes((tile, LANES))
    first = step % 2 == 0
    packed = q_ref[...].astype(F32)
    packed = jnp.where(first, packed, pltpu.roll(packed, 64, 1))
    query = jnp.where(low, packed, 0.0).astype(BF)
    packed = do_ref[...].astype(F32)
    packed = jnp.where(first, pltpu.roll(packed, 64, 1), packed)
    down = jnp.where(low, 0.0, packed).astype(BF)
    lse = lse_ref[0]
    delta = delta_ref[step % 2]

    def advance(j, dq, masked):
        rows = pl.ds(pl.multiple_of(j * width, width), width)
        pieces = kv_ref[rows, :]
        probs = jnp.exp2(dot(pieces, query, 1, 1) * steps_of - lse)
        if masked is not None:
            key = lax.broadcasted_iota(jnp.int32, (width, 1), 0) + masked
            ask = lax.broadcasted_iota(jnp.int32, (1, tile), 1)
            probs = jnp.where(key // per_frame <= ask // per_frame, probs, 0.0)
        dscore = (probs * (dot(pieces, down, 1, 1) - delta)).astype(BF)
        acc_ref[rows, :] += dot(dscore, query, 1, 0) + dot(probs.astype(BF), down, 1, 0)
        return dq + dot(kt_ref[:, rows], dscore, 1, 0)

    last = tile_index(step)
    parts = tile // width
    dq = jnp.zeros((64, tile), F32)
    dq = lax.fori_loop(0, last * parts, lambda j, c: advance(j, c, None), dq)
    for part in range(parts):
        dq = advance(last * parts + part, dq, part * width)
    dq = dq * scale

    @pl.when(step % 2 == 0)
    def _():
        dq_t_ref[0:64, :] = dq

    @pl.when(step % 2 == 1)
    def _():
        dq_t_ref[64:128, :] = dq
        dq_ref[...] = dq_t_ref[...].T.astype(BF)

    @pl.when(step == 3)
    def _():
        @pl.loop(0, kv_ref.shape[0] // tile)
        def _(j):
            rows = pl.ds(pl.multiple_of(j * tile, tile), tile)
            total = acc_ref[rows, :]
            dkv_ref[rows, :] = jnp.where(low_lanes((tile, LANES)), total * scale, total).astype(BF)


def attend_back(queries, downs, lse, out_t, keys_values, tile, per_frame, scale):
    one = pl.Buffered(1)
    keys = keys_values.shape[0]
    packed = pl.BlockSpec((tile, LANES), lambda i: (i // 2, 0))
    whole = pl.BlockSpec(keys_values.shape, lambda i: (0, 0), pipeline_mode=one)
    return pl.pallas_call(
        partial(attend_back_kernel, tile, tile // 2, per_frame, scale),
        grid=(4,),
        in_specs=[
            packed,
            packed,
            pl.BlockSpec((1, 1, tile), lambda i: (i, 0, 0)),
            pl.BlockSpec((1, LANES, tile), lambda i: (i // 2, 0, 0)),
            whole,
        ],
        out_specs=[packed, pl.BlockSpec(keys_values.shape, lambda i: (0, 0))],
        out_shape=[
            jax.ShapeDtypeStruct((2 * tile, LANES), BF),
            jax.ShapeDtypeStruct(keys_values.shape, BF),
        ],
        scratch_shapes=[
            pltpu.VMEM((64, keys), BF),
            pltpu.VMEM((keys, LANES), F32),
            pltpu.VMEM((LANES, tile), F32),
            pltpu.VMEM((2, 1, tile), F32),
        ],
        compiler_params=pltpu.CompilerParams(
            dimension_semantics=("arbitrary",), vmem_limit_bytes=60 * MIB
        ),
        cost_estimate=pl.CostEstimate(
            flops=8_000_000_000, bytes_accessed=12_000_000, transcendentals=0
        ),
        name="attend_back",
    )(queries, downs, lse, out_t, keys_values)


def exchange_kernel(axis, moves, sources, results, pair_of, finish, *refs):
    in_refs, refs = refs[:sources], refs[sources:]
    out_refs, refs = refs[:results], refs[results:]
    send_sem, recv_sem, own_sem = refs[-3:]
    scratch = refs[:-3]
    dests = scratch if finish is not None else out_refs
    me, count = lax.axis_index(axis), lax.axis_size(axis)
    barrier = pltpu.get_barrier_semaphore()
    for step in range(1, count):
        pl.semaphore_signal(
            barrier,
            inc=1,
            device_id={axis: lax.rem(me + step, count)},
            device_id_type=pl.DeviceIdType.MESH,
        )
    pl.semaphore_wait(barrier, count - 1)
    copies = []
    for step in range(1, count):
        peer = lax.rem(me + step, count)
        for index, (source, dest, take, place) in enumerate(moves):
            copies.append(
                pltpu.make_async_remote_copy(
                    src_ref=take(in_refs[source], peer),
                    dst_ref=place(dests[dest], me, peer),
                    send_sem=send_sem.at[index, step - 1],
                    recv_sem=recv_sem.at[index, step - 1],
                    device_id={axis: peer},
                    device_id_type=pl.DeviceIdType.MESH,
                )
            )
            copies[-1].start()
    for index, (source, dest, take, place) in enumerate(moves):
        copies.append(
            pltpu.make_async_copy(
                take(in_refs[source], me), place(dests[dest], me, me), own_sem.at[index]
            )
        )
        copies[-1].start()
    for copy in copies:
        copy.wait()
    if pair_of is not None:
        core = lax.rem(me, 2)
        ref = dests[pair_of].at[core]
        copy = pltpu.make_async_remote_copy(
            src_ref=ref,
            dst_ref=ref,
            send_sem=own_sem.at[len(moves)],
            recv_sem=own_sem.at[len(moves) + 1],
            device_id={axis: me + 1 - 2 * core},
            device_id_type=pl.DeviceIdType.MESH,
        )
        copy.start()
        copy.wait()
    if finish is not None:
        finish(dests, out_refs)


def exchange(name, axis, number, moves, arrays, shapes, pair_of=None, finish=None, landing=()):
    count = lax.axis_size(axis)
    vmem = pl.BlockSpec(memory_space=pltpu.VMEM)
    sent = sum(a.size * a.dtype.itemsize for a in arrays)
    return pl.pallas_call(
        partial(exchange_kernel, axis, moves, len(arrays), len(shapes), pair_of, finish),
        in_specs=[vmem] * len(arrays),
        out_specs=[vmem] * len(shapes),
        out_shape=[jax.ShapeDtypeStruct(*shape) for shape in shapes],
        scratch_shapes=[pltpu.VMEM(*shape) for shape in landing]
        + [
            pltpu.SemaphoreType.DMA((len(moves), count - 1)),
            pltpu.SemaphoreType.DMA((len(moves), count - 1)),
            pltpu.SemaphoreType.DMA((len(moves) + 2,)),
        ],
        compiler_params=pltpu.CompilerParams(
            collective_id=number, has_side_effects=True, vmem_limit_bytes=40 * MIB
        ),
        cost_estimate=pl.CostEstimate(
            flops=0, bytes_accessed=20_000_000 + 30 * sent, transcendentals=0
        ),
        name=name,
    )(*arrays)


def all_of(ref, peer):
    return ref


def block_of(ref, peer):
    return ref.at[peer]


def at_sender(ref, me, peer):
    return ref.at[me]


def lanes_of(size):
    def view(ref, peer):
        return ref.at[:, pl.ds(pl.multiple_of(peer * size, LANES), size)]

    return view


def lanes_at(size):
    def view(ref, me, peer):
        return ref.at[:, pl.ds(pl.multiple_of(me * size, LANES), size)]

    return view


def add_landed(dests, out_refs):
    landed, out = dests[0], out_refs[0]
    rows = out.shape[0]
    step = 32 if rows % 32 == 0 else rows

    @pl.loop(0, rows // step)
    def _(j):
        cut = pl.ds(pl.multiple_of(j * step, step), step)
        total = landed[0, cut, :].astype(F32)
        for other in range(1, landed.shape[0]):
            total += landed[other, cut, :].astype(F32)
        out[cut, :] = total.astype(out.dtype)


def gather(name, axis, number, arrays):
    count = lax.axis_size(axis)
    moves = [(i, i, all_of, at_sender) for i in range(len(arrays))]
    return exchange(
        name, axis, number, moves, arrays, [((count,) + a.shape, a.dtype) for a in arrays]
    )


def square_gather_kernel(in_ref, out_ref, send_sem, recv_sem, own_sem):
    me = lax.axis_index("frame")
    near = (me + 1 - 2 * lax.rem(me, 2), me + 2 - 4 * (me // 2))
    barrier = pltpu.get_barrier_semaphore()
    for peer in near:
        pl.semaphore_signal(
            barrier, inc=1, device_id={"frame": peer}, device_id_type=pl.DeviceIdType.MESH
        )
    pl.semaphore_wait(barrier, 2)
    half = in_ref.shape[0] // 2
    cuts = (pl.ds(0, half), pl.ds(half, half))

    def copy_of(source, dest, way, index):
        return pltpu.make_async_remote_copy(
            src_ref=source,
            dst_ref=dest,
            send_sem=send_sem.at[way, index],
            recv_sem=recv_sem.at[way, index],
            device_id={"frame": near[way]},
            device_id_type=pl.DeviceIdType.MESH,
        )

    first, second, third = [], [], []
    for way in range(2):
        first.append(copy_of(in_ref.at[cuts[way]], out_ref.at[me, cuts[way]], way, 0))
        first[-1].start()
    for way in range(2):
        rest = cuts[1 - way]
        second.append(copy_of(in_ref.at[rest], out_ref.at[me, rest], way, 1))
        second[-1].start()
    own = pltpu.make_async_copy(in_ref, out_ref.at[me], own_sem)
    own.start()
    for way in range(2):
        first[way].wait_recv()
        block = out_ref.at[near[way], cuts[way]]
        third.append(copy_of(block, block, 1 - way, 2))
        third[-1].start()
    for way in range(2):
        first[way].wait_send()
        second[way].wait()
        third[way].wait()
    own.wait()


def gather_frame(name, number, array):
    if lax.axis_size("frame") != 4:
        return gather(name, "frame", number, [array])[0]
    vmem = pl.BlockSpec(memory_space=pltpu.VMEM)
    return pl.pallas_call(
        square_gather_kernel,
        in_specs=[vmem],
        out_specs=vmem,
        out_shape=jax.ShapeDtypeStruct((4,) + array.shape, array.dtype),
        scratch_shapes=[
            pltpu.SemaphoreType.DMA((2, 3)),
            pltpu.SemaphoreType.DMA((2, 3)),
            pltpu.SemaphoreType.DMA,
        ],
        compiler_params=pltpu.CompilerParams(
            collective_id=number, has_side_effects=True, vmem_limit_bytes=40 * MIB
        ),
        cost_estimate=pl.CostEstimate(flops=0, bytes_accessed=30_000_000, transcendentals=0),
        name=name,
    )(array)


def scatter_sum(name, axis, number, parts, dtype=F32):
    return exchange(
        name,
        axis,
        number,
        [(0, 0, block_of, at_sender)],
        [parts],
        [(parts.shape[1:], dtype)],
        finish=add_landed,
        landing=[(parts.shape, parts.dtype)],
    )[0]


def cut_kernel(slice_width, hidden_slice, in_ref, out_ref, up_ref, down_ref, *refs):
    own_in, own_rest, own_down, sems = refs
    frame = lax.axis_index("frame")
    width = out_ref.shape[1]
    hidden = pl.ds(pl.multiple_of(frame * hidden_slice, LANES), hidden_slice)
    pieces = [
        (out_ref, own_rest.at[:, 0:width]),
        (up_ref.at[:, hidden], own_rest.at[:, width : width + hidden_slice]),
        (down_ref.at[:, hidden], own_down),
    ]
    for part in range(4):
        start = pl.multiple_of(part * width + frame * slice_width, LANES)
        pieces.append(
            (
                in_ref.at[:, pl.ds(start, slice_width)],
                own_in.at[:, part * slice_width : (part + 1) * slice_width],
            )
        )
    copies = [
        pltpu.make_async_copy(source, dest, sems.at[index])
        for index, (source, dest) in enumerate(pieces)
    ]
    for copy in copies:
        copy.start()
    for copy in copies:
        copy.wait()


def cut_weights(attn_in, out_weight, up_weight, down_weight, slice_width, hidden_slice):
    rows, width = out_weight.shape
    vmem = pl.BlockSpec(memory_space=pltpu.VMEM)
    return pl.pallas_call(
        partial(cut_kernel, slice_width, hidden_slice),
        in_specs=[pl.BlockSpec(memory_space=pl.ANY)] * 4,
        out_specs=[vmem] * 3,
        out_shape=[
            jax.ShapeDtypeStruct((rows, 4 * slice_width), BF),
            jax.ShapeDtypeStruct((rows, width + hidden_slice), BF),
            jax.ShapeDtypeStruct((rows, hidden_slice), BF),
        ],
        scratch_shapes=[pltpu.SemaphoreType.DMA((7,))],
        name="cut_weights",
    )(attn_in, out_weight, up_weight, down_weight)


def join_kernel(hidden_slice, parts_ref, up_ref, down_ref, out_ref):
    total = None
    for part in range(parts_ref.shape[0]):
        cut = slice(part * hidden_slice, (part + 1) * hidden_slice)
        up_ref[:, cut] = parts_ref[part, :, :hidden_slice].astype(F32)
        down_ref[:, cut] = parts_ref[part, :, hidden_slice : 2 * hidden_slice].astype(F32)
        last = parts_ref[part, :, 2 * hidden_slice :].astype(F32)
        total = last if total is None else total + last
    out_ref[...] = total


def join_in_kernel(width, slice_width, parts_ref, in_ref):
    for part in range(parts_ref.shape[0]):
        for group in range(4):
            start = group * width + part * slice_width
            in_ref[:, start : start + slice_width] = parts_ref[
                part, :, group * slice_width : (group + 1) * slice_width
            ].astype(F32)


def join(name, body, parts, widths):
    count, rows, columns = parts.shape
    step = rows // 4
    return pl.pallas_call(
        body,
        grid=(4,),
        in_specs=[pl.BlockSpec((count, step, columns), lambda i: (0, i, 0))],
        out_specs=[pl.BlockSpec((step, w), lambda i: (i, 0)) for w in widths],
        out_shape=[jax.ShapeDtypeStruct((rows, w), F32) for w in widths],
        compiler_params=pltpu.CompilerParams(dimension_semantics=("arbitrary",)),
        cost_estimate=pl.CostEstimate(flops=0, bytes_accessed=8_000_000, transcendentals=0),
        name=name,
    )(parts)


def mlp_grads_kernel(cut, *refs):
    out_ref = refs[-1]
    start = 0
    for part in range(len(refs) // 2):
        left, right = refs[2 * part], refs[2 * part + 1]
        columns = right.shape[1]
        result = dot(left[...], right[...], 0, 0).astype(BF)
        for block in range(out_ref.shape[0]):
            out_ref[block, :, start : start + columns] = result[block * cut : (block + 1) * cut]
        start += columns


def mlp_grads(pairs, row_devs):
    cut = pairs[0][0].shape[1] // row_devs
    block = max(cut, LANES)
    in_specs = []
    for left, right in pairs:
        in_specs.append(pl.BlockSpec((left.shape[0], block), lambda i: (0, i)))
        in_specs.append(pl.BlockSpec(right.shape, lambda i: (0, 0), pipeline_mode=pl.Buffered(1)))
    columns = sum(right.shape[1] for _, right in pairs)
    return pl.pallas_call(
        partial(mlp_grads_kernel, cut),
        grid=(row_devs * cut // block,),
        in_specs=in_specs,
        out_specs=pl.BlockSpec((block // cut, cut, columns), lambda i: (i, 0, 0)),
        out_shape=jax.ShapeDtypeStruct((row_devs, cut, columns), BF),
        compiler_params=pltpu.CompilerParams(
            dimension_semantics=("arbitrary",), vmem_limit_bytes=48 * MIB
        ),
        cost_estimate=pl.CostEstimate(
            flops=5_000_000_000, bytes_accessed=18_000_000, transcendentals=0
        ),
        name="mlp_grads",
    )(*[array for pair in pairs for array in pair])


def on_device(
    tokens,
    timesteps,
    noise_table,
    mod_weight,
    mod_bias,
    attn_in,
    out_weight,
    up_weight,
    down_weight,
    cotangent,
):
    clips, frames, rows_dev, grid_side, width = tokens.shape
    frame_index = lax.axis_index("frame")
    row_index = lax.axis_index("row")
    frame_devs, row_devs = lax.axis_size("frame"), lax.axis_size("row")
    core = row_index % 2
    clip_len = frames * frame_devs
    head_dim = width // HEADS
    heads = HEADS // frame_devs
    slice_width = width // frame_devs
    per_frame_dev = rows_dev * grid_side
    per_frame = grid_side * grid_side
    token_count = clips * frames * per_frame_dev
    group_count = token_count * frame_devs
    tile = clip_len // 8 * per_frame
    scale = head_dim ** (-0.5)
    step_count = noise_table.shape[0]
    assert head_dim == 64 and row_devs == 2 * clips * heads

    def by_frames(values):
        parts = values.reshape(frame_devs, clips, frames * per_frame_dev, -1)
        return jnp.transpose(parts, (1, 0, 2, 3)).reshape(group_count, values.shape[-1])

    def to_frames(values):
        parts = values.reshape(clips, frame_devs, frames * per_frame_dev, -1)
        return jnp.transpose(parts, (1, 0, 2, 3)).reshape(frame_devs, token_count, -1)

    def gather_frames(values):
        full = lax.all_gather(values, "frame", axis=1, tiled=True)
        return full.reshape(group_count, values.shape[-1])

    def scatter_frames(values):
        parts = to_frames(values).reshape(group_count, width)
        return lax.psum_scatter(parts, "frame", scatter_dimension=0, tiled=True).reshape(
            tokens.shape
        )

    hidden_slice = up_weight.shape[1] // frame_devs
    own_in, own_rest, own_down = cut_weights(
        attn_in, out_weight, up_weight, down_weight, slice_width, hidden_slice
    )
    weight_in = lax.all_gather(own_in, "row", axis=0, tiled=True)

    steps_iota = lax.broadcasted_iota(jnp.int32, (1, 1, step_count), 2)
    one_hot = (timesteps[:, :, None] == steps_iota).astype(BF)
    embedding = jnp.einsum("cls,sd->cld", one_hot, noise_table, preferred_element_type=F32)
    silu_low = jax.nn.silu(embedding).astype(BF)
    mod_local = jnp.einsum(
        "cld,de->cle", silu_low, mod_weight, preferred_element_type=F32
    ) + mod_bias.astype(F32)
    mod_width = mod_local.shape[2]
    modulation = exchange(
        "gather_mod",
        "row",
        0,
        [(0, 0, all_of, lanes_at(mod_width))],
        [mod_local.astype(BF).reshape(clips * frames, mod_width)],
        [((clips * frames, mod_width * row_devs), BF)],
    )[0].astype(F32)
    modulation = modulation.reshape(clips, frames, 6, 1, 1, width)
    shift_one, scale_one, gate_one, shift_two, scale_two, gate_two = [
        modulation[:, :, part] for part in range(6)
    ]

    frame_freq, row_freq, col_freq = [np.tile(t, 4) for t in rotary_freqs(head_dim // 2)]
    shape_three = (clip_len, rows_dev, grid_side, LANES)
    frame_pos = lax.broadcasted_iota(F32, shape_three, 0)
    row_pos = (row_index * rows_dev + lax.broadcasted_iota(jnp.int32, shape_three, 1)).astype(F32)
    col_pos = lax.broadcasted_iota(F32, shape_three, 2)
    angles = (frame_pos * frame_freq + row_pos * row_freq + col_pos * col_freq).reshape(-1, LANES)
    sign = np.where(np.arange(LANES) % 64 < 32, -1.0, 1.0).astype(np.float32)
    cosines = jnp.cos(angles)
    sines = jnp.sin(angles) * sign

    token_f = tokens.astype(F32)
    hidden_one, norm_one_pull = jax.vjp(modulate, token_f, shift_one, scale_one)
    hidden_group = by_frames(
        gather_frame("gather_one", 1, hidden_one.astype(BF).reshape(token_count, width))
    )

    grad_out = cotangent.astype(F32)
    grad_branch_two = (grad_out * gate_two).astype(BF)
    hidden_group, grad_branch_two = lax.optimization_barrier((hidden_group, grad_branch_two))
    grad_two_group = gather_frames(grad_branch_two)

    pack, gate_raw = qkv_project(hidden_group, weight_in, cosines, sines, clips, heads)

    half = tile // row_devs
    pairs = [(r, r ^ 1) for r in range(row_devs)]

    spans = half // per_frame_dev
    by_token = (spans, per_frame_dev, LANES)
    by_head = (spans, row_devs, per_frame_dev, LANES)

    def peer_rows(ref, peer):
        return ref.at[:, :, peer]

    queries, keys_values = exchange(
        "to_heads",
        "row",
        2,
        [
            (0, 0, lambda r, p: r.at[p, 0:2], lambda r, me, p: r.at[:, :, me]),
            (0, 1, lambda r, p: r.at[p, 2:6], lambda r, me, p: r.at[p % 2, :, :, me]),
        ],
        [pack.reshape((row_devs, 6) + by_token)],
        [((2,) + by_head, BF), ((2, 4) + by_head, BF)],
        pair_of=1,
    )
    queries = queries.reshape(-1, LANES)
    keys_values = keys_values.reshape(-1, LANES)

    queries, keys_values, grad_two_group, own_rest, own_down = lax.optimization_barrier(
        (queries, keys_values, grad_two_group, own_rest, own_down)
    )
    rest = lax.all_gather(own_rest, "row", axis=0, tiled=True)
    full_out, weight_up = rest[:, :width], rest[:, width:]
    attended_heads, attended_t, lse = attend(queries, keys_values, tile, per_frame, scale)
    pack_shape = (clips, heads, 2, 2, half, LANES)
    (arrived,) = exchange(
        "to_tokens",
        "row",
        3,
        [(0, 0, peer_rows, at_sender)],
        [attended_heads.reshape((2,) + by_head)],
        [((row_devs, 2) + by_token, BF)],
    )
    arrived = arrived.reshape(pack_shape)
    gated_group, attended = gate_forward(arrived, gate_raw, clips, heads)

    steps_wide = jnp.broadcast_to(timesteps.reshape(-1, 1), (clips * frames, LANES))
    gated, steps_parts = exchange(
        "gated_back",
        "frame",
        4,
        [(0, 0, block_of, lanes_at(slice_width)), (1, 1, all_of, at_sender)],
        [to_frames(gated_group), steps_wide],
        [((token_count, width), BF), ((frame_devs,) + steps_wide.shape, jnp.int32)],
    )
    branch_one = jnp.dot(gated, full_out, preferred_element_type=F32).reshape(tokens.shape)
    after_one = token_f + gate_one * branch_one
    hidden_two, norm_two_pull = jax.vjp(modulate, after_one, shift_two, scale_two)
    hidden_two, own_down = lax.optimization_barrier((hidden_two, own_down))
    weight_down = lax.all_gather(own_down, "row", axis=0, tiled=True)
    hidden_two_group = by_frames(
        gather_frame("gather_two", 5, hidden_two.astype(BF).reshape(token_count, width))
    )

    pre_act = jnp.dot(hidden_two_group, weight_up, preferred_element_type=F32)
    act_values, gelu_pull = jax.vjp(partial(jax.nn.gelu, approximate=True), pre_act)
    act_low = act_values.astype(BF)
    grad_act = jnp.dot(grad_two_group, weight_down, preferred_element_type=F32)
    (grad_pre,) = gelu_pull(grad_act)
    grad_pre = grad_pre.astype(BF)
    grad_hidden_two = scatter_sum(
        "scatter_two", "frame", 6, to_frames(dot(grad_pre, weight_up, 1, 1).astype(BF))
    ).reshape(tokens.shape)
    branch_two = dot(act_low, weight_down, 1, 1).astype(BF)
    grad_hidden_two, branch_two = lax.optimization_barrier((grad_hidden_two, branch_two))
    branch_two = scatter_frames(branch_two)
    grad_after_part, grad_shift_two, grad_scale_two = norm_two_pull(grad_hidden_two)
    grad_after = grad_out + grad_after_part
    grad_gate_one = jnp.sum(grad_after * branch_one, axis=(2, 3), keepdims=True)
    grad_branch_one = (grad_after * gate_one).astype(BF).reshape(token_count, width)
    grad_gated = dot(grad_branch_one, full_out, 1, 1).astype(BF)
    weight_grads = mlp_grads(
        [(hidden_two_group, grad_pre), (grad_two_group, act_low), (gated, grad_branch_one)],
        row_devs,
    )
    grad_gated, weight_grads = lax.optimization_barrier((grad_gated, weight_grads))
    weight_grads = lax.psum_scatter(weight_grads, "row", scatter_dimension=0, tiled=True)
    (grad_gated,) = exchange(
        "grad_gated",
        "frame",
        7,
        [(0, 0, lanes_of(slice_width), at_sender)],
        [grad_gated],
        [((frame_devs, token_count, slice_width), BF)],
    )
    grad_gated = by_frames(grad_gated)
    down_pack, grad_gate = gate_back(grad_gated, gate_raw, attended, clips, heads)
    (downs,) = exchange(
        "grad_to_heads",
        "row",
        8,
        [(0, 0, block_of, lambda r, me, p: r.at[:, :, me])],
        [down_pack.reshape((row_devs, 2) + by_token)],
        [((2,) + by_head, BF)],
    )
    downs = downs.reshape(-1, LANES)
    downs, branch_two = lax.optimization_barrier((downs, branch_two))
    branch_two = branch_two.astype(F32)
    mixed = (after_one + gate_two * branch_two).astype(BF)
    grad_gate_two = jnp.sum(grad_out * branch_two, axis=(2, 3), keepdims=True)

    grad_queries, grad_kv = attend_back(
        queries, downs, lse, attended_t, keys_values, tile, per_frame, scale
    )
    grad_kv = grad_kv.reshape(2, -1, LANES)
    keep = lax.dynamic_index_in_dim(grad_kv, core, 0, keepdims=False)
    give = lax.dynamic_index_in_dim(grad_kv, 1 - core, 0, keepdims=False)
    got = lax.ppermute(give, "row", pairs)
    grad_kv = (keep.astype(F32) + got.astype(F32)).astype(BF)
    grad_kv, weight_grads = lax.optimization_barrier((grad_kv, weight_grads))
    grads_all = lax.all_gather(weight_grads[0], "frame", axis=0, tiled=False)
    (back_pack,) = exchange(
        "grad_to_tokens",
        "row",
        9,
        [
            (0, 0, peer_rows, lambda r, me, p: r.at[me, 0:2]),
            (1, 0, peer_rows, lambda r, me, p: r.at[me, 2:6]),
        ],
        [grad_queries.reshape((2,) + by_head), grad_kv.reshape((4,) + by_head)],
        [((row_devs, 6) + by_token, BF)],
    )
    back_pack = back_pack.reshape(clips, heads, 2, 6, half, LANES)
    grad_mixed, grad_hidden = qkv_back(
        back_pack, grad_gate, weight_in, cosines, sines, clips, heads
    )
    grad_mixed, grads_all = lax.optimization_barrier((grad_mixed, grads_all))
    grad_hidden_one = scatter_sum("scatter_one", "frame", 10, to_frames(grad_hidden)).reshape(
        tokens.shape
    )
    in_grad = lax.psum_scatter(
        dot(hidden_group, grad_mixed, 0, 0).astype(BF), "row", scatter_dimension=0, tiled=True
    )

    grad_token_part, grad_shift_one, grad_scale_one = norm_one_pull(grad_hidden_one)
    tokens_grad = (grad_after + grad_token_part).astype(BF)

    grad_mod = jnp.stack(
        [
            grad_shift_one,
            grad_scale_one,
            grad_gate_one,
            grad_shift_two,
            grad_scale_two,
            grad_gate_two,
        ],
        axis=2,
    ).reshape(clips * frames, 6 * width)
    grad_mod = jnp.transpose(
        grad_mod.reshape(clips * frames, row_devs, mod_width), (1, 0, 2)
    )
    grad_mod = scatter_sum("scatter_mod", "row", 11, grad_mod, BF)
    grad_mod, in_grad = lax.optimization_barrier((grad_mod, in_grad))
    (grad_mod_all,) = gather("gather_grad_mod", "frame", 12, [grad_mod])
    grad_mod_all = grad_mod_all.reshape(-1, mod_width)
    steps_all = steps_parts.reshape(-1, LANES)[:, 0]
    hot_all = steps_all[:, None] == lax.broadcasted_iota(jnp.int32, (1, step_count), 1)
    embed_all = jnp.dot(hot_all.astype(BF), noise_table, preferred_element_type=F32)
    silu_all, silu_pull = jax.vjp(jax.nn.silu, embed_all)
    mod_weight_grad = dot(silu_all.astype(BF), grad_mod_all, 0, 0)
    mod_bias_grad = jnp.sum(grad_mod_all.astype(F32), axis=0)
    grad_silu = dot(grad_mod_all, mod_weight, 1, 1)
    frame_count, cut = grad_silu.shape[0], width // row_devs
    grad_silu = jnp.transpose(grad_silu.reshape(frame_count, row_devs, cut), (1, 0, 2))
    grad_silu = scatter_sum("scatter_silu", "row", 13, grad_silu)
    (grad_silu,) = gather("gather_silu", "row", 14, [grad_silu])
    grad_silu = jnp.transpose(grad_silu, (1, 0, 2)).reshape(frame_count, width)
    (grad_embedding,) = silu_pull(grad_silu)
    noise_table_grad = lax.dot_general(
        hot_all.astype(F32),
        grad_embedding,
        (((0,), (0,)), ((), ())),
        precision=lax.Precision.HIGHEST,
    )

    up_weight_grad, down_weight_grad, out_weight_grad = join(
        "join_grads",
        partial(join_kernel, hidden_slice),
        grads_all,
        (up_weight.shape[1], down_weight.shape[1], width),
    )
    in_all = lax.all_gather(in_grad, "frame", axis=0, tiled=False)
    (attn_in_grad,) = join(
        "join_in", partial(join_in_kernel, width, slice_width), in_all, (attn_in.shape[1],)
    )
    return (
        mixed,
        tokens_grad,
        noise_table_grad,
        mod_weight_grad,
        mod_bias_grad,
        attn_in_grad,
        out_weight_grad,
        up_weight_grad,
        down_weight_grad,
    )


def solution(mesh):
    in_specs = (
        P(None, "frame", "row", None, None),
        P(None, "frame"),
        P(),
        P(None, "row"),
        P("row"),
        P("row", None),
        P("row", None),
        P("row", None),
        P("row", None),
        P(None, "frame", "row", None, None),
    )
    out_specs = (
        P(None, "frame", "row", None, None),
        P(None, "frame", "row", None, None),
        P(),
        P(None, "row"),
        P("row"),
        P("row", None),
        P("row", None),
        P("row", None),
        P("row", None),
    )
    return jax.shard_map(
        on_device, mesh=mesh, in_specs=in_specs, out_specs=out_specs, check_vma=False
    )
```

```python
from functools import partial

import jax
import jax.numpy as jnp
import numpy as np
from jax import lax
from jax.experimental import pallas as pl
from jax.experimental.pallas import tpu as pltpu
from jax.sharding import PartitionSpec as P

HEADS = 16
EPS = 1e-06
LOG2E = 1.4426950408889634
F32 = jnp.float32
BF = jnp.bfloat16
LANES = 128
MIB = 1 << 20


def rotary_freqs(pair_count):
    third_count = pair_count // 3
    group_sizes = [pair_count - 2 * third_count, third_count, third_count]
    tables = []
    offset = 0
    for group_index in range(3):
        freq_table = np.zeros((pair_count,), np.float32)
        for inner_index in range(group_sizes[group_index]):
            freq_table[offset + inner_index] = 10000.0 ** (-inner_index / group_sizes[group_index])
        offset += group_sizes[group_index]
        tables.append(freq_table)
    return tables


def layer_norm(values):
    row_mean = jnp.mean(values, axis=-1, keepdims=True)
    centered = values - row_mean
    row_var = jnp.mean(centered * centered, axis=-1, keepdims=True)
    return centered * lax.rsqrt(row_var + EPS)


def modulate(values, shift, scale_part):
    return layer_norm(values) * (1.0 + scale_part) + shift


def dot(left, right, left_dim, right_dim):
    return lax.dot_general(
        left, right, (((left_dim,), (right_dim,)), ((), ())), preferred_element_type=F32
    )


def swap_halves(values):
    lane = lax.broadcasted_iota(jnp.int32, values.shape, 1)
    width = values.shape[1]
    return jnp.where(
        (lane % 64) < 32, pltpu.roll(values, width - 32, 1), pltpu.roll(values, 32, 1)
    )


def low_lanes(shape):
    return lax.broadcasted_iota(jnp.int32, shape, len(shape) - 1) < 64


def qkv_kernel(heads, hid_ref, w_ref, cos_ref, sin_ref, pack_ref, gate_ref):
    clip, quarter = pl.program_id(0), pl.program_id(1)
    width = heads * 64
    mixed = jnp.dot(hid_ref[...], w_ref[...], preferred_element_type=F32)
    cos, sin = cos_ref[...], sin_ref[...]
    rows = mixed.shape[0]
    half = rows // 2
    gate_ref[...] = mixed[:, 3 * width :]
    low = low_lanes((rows, LANES))
    low_half = low_lanes((half, LANES))
    query_set = jnp.where((quarter == 0) | (quarter == 3), 0, 1)
    slot = quarter // 2
    for pair in range(heads // 2):
        cut = slice(pair * LANES, (pair + 1) * LANES)
        query = mixed[:, cut]
        key = mixed[:, width + pair * LANES : width + (pair + 1) * LANES]
        value = mixed[:, 2 * width + pair * LANES : 2 * width + (pair + 1) * LANES]
        query = query * cos + swap_halves(query) * sin
        key = key * cos + swap_halves(key) * sin
        key_turn = pltpu.roll(key, 64, 1)
        value_turn = pltpu.roll(value, 64, 1)
        query_turn = pltpu.roll(query, 64, 1)
        packs = (
            (
                jnp.where(low, key, value_turn),
                jnp.where(low_half, query[:half], query_turn[half:]),
            ),
            (
                jnp.where(low, key_turn, value),
                jnp.where(low_half, query_turn[:half], query[half:]),
            ),
        )
        for inner, (key_value, queries) in enumerate(packs):
            head = 2 * pair + inner
            pack_ref[clip, head, query_set, slot] = queries.astype(BF)
            key_value = key_value.astype(BF)
            first = 2 + 2 * (quarter % 2)
            pack_ref[clip, head, quarter // 2, first] = key_value[:half]
            pack_ref[clip, head, quarter // 2, first + 1] = key_value[half:]


def qkv_project(hidden, weight, cos, sin, clips, heads):
    tokens, width = hidden.shape
    quarter = tokens // clips // 4
    one = pl.Buffered(1)
    return pl.pallas_call(
        partial(qkv_kernel, heads),
        grid=(clips, 4),
        in_specs=[
            pl.BlockSpec((quarter, width), lambda c, i: (c * 4 + i, 0)),
            pl.BlockSpec(weight.shape, lambda c, i: (0, 0), pipeline_mode=one),
            pl.BlockSpec((quarter, LANES), lambda c, i: (i, 0)),
            pl.BlockSpec((quarter, LANES), lambda c, i: (i, 0)),
        ],
        out_specs=[
            pl.BlockSpec(
                (clips, heads, 2, 6, quarter // 2, LANES), lambda c, i: (0, 0, 0, 0, 0, 0)
            ),
            pl.BlockSpec((quarter, heads * 64), lambda c, i: (c * 4 + i, 0)),
        ],
        out_shape=[
            jax.ShapeDtypeStruct((clips, heads, 2, 6, quarter // 2, LANES), BF),
            jax.ShapeDtypeStruct((tokens, heads * 64), F32),
        ],
        compiler_params=pltpu.CompilerParams(
            dimension_semantics=("arbitrary", "arbitrary"), vmem_limit_bytes=48 * MIB
        ),
        name="qkv_project",
    )(hidden, weight, cos, sin)


def qkv_back_kernel(heads, pack_ref, dgate_ref, w_ref, cos_ref, sin_ref, mixed_ref, hid_ref):
    clip, quarter = pl.program_id(0), pl.program_id(1)
    width = heads * 64
    cos, sin = cos_ref[...], sin_ref[...]
    rows = cos.shape[0]
    half = rows // 2
    low_half = low_lanes((half, LANES))
    query_set = jnp.where((quarter == 0) | (quarter == 3), 0, 1)
    slot = quarter // 2
    first = 2 + 2 * (quarter % 2)
    low = low_lanes((rows, LANES))
    for pair in range(heads // 2):
        even, odd = 2 * pair, 2 * pair + 1
        query_even = pack_ref[clip, even, query_set, slot].astype(F32)
        query_odd = pack_ref[clip, odd, query_set, slot].astype(F32)
        query = jnp.concatenate(
            [
                jnp.where(low_half, query_even, pltpu.roll(query_odd, 64, 1)),
                jnp.where(low_half, pltpu.roll(query_even, 64, 1), query_odd),
            ],
            axis=0,
        )
        both = []
        for head in (even, odd):
            both.append(
                jnp.concatenate(
                    [
                        pack_ref[clip, head, quarter // 2, first].astype(F32),
                        pack_ref[clip, head, quarter // 2, first + 1].astype(F32),
                    ],
                    axis=0,
                )
            )
        key = jnp.where(low, both[0], pltpu.roll(both[1], 64, 1))
        value = jnp.where(low, pltpu.roll(both[0], 64, 1), both[1])
        query = query * cos - swap_halves(query) * sin
        key = key * cos - swap_halves(key) * sin
        for part, values in enumerate((query, key, value)):
            start = part * width + pair * LANES
            mixed_ref[:, start : start + LANES] = values.astype(BF)
    mixed_ref[:, 3 * width :] = dgate_ref[...]
    hid_ref[...] = dot(mixed_ref[...], w_ref[...], 1, 1).astype(BF)


def qkv_back(pack, dgate, weight, cos, sin, clips, heads):
    tokens = dgate.shape[0]
    width = weight.shape[0]
    quarter = tokens // clips // 4
    one = pl.Buffered(1)
    return pl.pallas_call(
        partial(qkv_back_kernel, heads),
        grid=(clips, 4),
        in_specs=[
            pl.BlockSpec(pack.shape, lambda c, i: (0, 0, 0, 0, 0, 0), pipeline_mode=one),
            pl.BlockSpec((quarter, heads * 64), lambda c, i: (c * 4 + i, 0)),
            pl.BlockSpec(weight.shape, lambda c, i: (0, 0), pipeline_mode=one),
            pl.BlockSpec((quarter, LANES), lambda c, i: (i, 0)),
            pl.BlockSpec((quarter, LANES), lambda c, i: (i, 0)),
        ],
        out_specs=[
            pl.BlockSpec((quarter, 4 * heads * 64), lambda c, i: (c * 4 + i, 0)),
            pl.BlockSpec((quarter, width), lambda c, i: (c * 4 + i, 0)),
        ],
        out_shape=[
            jax.ShapeDtypeStruct((tokens, 4 * heads * 64), BF),
            jax.ShapeDtypeStruct((tokens, width), BF),
        ],
        compiler_params=pltpu.CompilerParams(
            dimension_semantics=("arbitrary", "arbitrary"), vmem_limit_bytes=48 * MIB
        ),
        name="qkv_back",
    )(pack, dgate, weight, cos, sin)


def unpack_pair(even, odd):
    low = low_lanes(even.shape)
    return jnp.concatenate(
        [
            jnp.where(low, even, pltpu.roll(odd, 64, 1)),
            jnp.where(low, pltpu.roll(even, 64, 1), odd),
        ],
        axis=0,
    )


def gate_landed(clips, heads):
    def finish(dests, in_refs, out_refs):
        pack_ref, gate_ref, (gated_ref, attended_ref) = dests[0], in_refs[1], out_refs
        quarter = gate_ref.shape[0] // clips // 4
        for clip in range(clips):
            for index in range(4):
                query_set, slot = (0, 1, 1, 0)[index], index // 2
                rows = pl.ds((clip * 4 + index) * quarter, quarter)
                for pair in range(heads // 2):
                    cut = slice(pair * LANES, (pair + 1) * LANES)
                    even, odd = [
                        pack_ref[(clip * heads + head) * 2 + query_set, slot]
                        .reshape(quarter // 2, LANES)
                        .astype(F32)
                        for head in (2 * pair, 2 * pair + 1)
                    ]
                    attended = unpack_pair(even, odd)
                    attended_ref[rows, cut] = attended.astype(BF)
                    gate = jax.nn.sigmoid(gate_ref[rows, cut])
                    gated_ref[rows, cut] = (attended * gate).astype(BF)

    return finish


def gate_back_kernel(heads, grad_ref, gate_ref, attended_ref, pack_ref, dgate_ref):
    clip, quarter = pl.program_id(0), pl.program_id(1)
    query_set = jnp.where((quarter == 0) | (quarter == 3), 0, 1)
    slot = quarter // 2
    rows = grad_ref.shape[0]
    half = rows // 2
    low = low_lanes((half, LANES))
    for pair in range(heads // 2):
        cut = slice(pair * LANES, (pair + 1) * LANES)
        sig = jax.nn.sigmoid(gate_ref[:, cut])
        grad = grad_ref[:, cut].astype(F32)
        dgate = grad * attended_ref[:, cut].astype(F32) * sig * (1.0 - sig)
        dgate_ref[:, cut] = dgate.astype(BF)
        down = grad * sig
        turn = pltpu.roll(down, 64, 1)
        pack_ref[clip, 2 * pair, query_set, slot] = jnp.where(low, down[:half], turn[half:]).astype(
            BF
        )
        pack_ref[clip, 2 * pair + 1, query_set, slot] = jnp.where(
            low, turn[:half], down[half:]
        ).astype(BF)


def gate_back(grad, gate, attended, clips, heads):
    tokens = gate.shape[0]
    quarter = tokens // clips // 4
    block = pl.BlockSpec((quarter, heads * 64), lambda c, i: (c * 4 + i, 0))
    pack_shape = (clips, heads, 2, 2, quarter // 2, LANES)
    return pl.pallas_call(
        partial(gate_back_kernel, heads),
        grid=(clips, 4),
        in_specs=[block, block, block],
        out_specs=[pl.BlockSpec(pack_shape, lambda c, i: (0, 0, 0, 0, 0, 0)), block],
        out_shape=[
            jax.ShapeDtypeStruct(pack_shape, BF),
            jax.ShapeDtypeStruct((tokens, heads * 64), BF),
        ],
        compiler_params=pltpu.CompilerParams(dimension_semantics=("arbitrary", "arbitrary")),
        name="gate_back",
    )(grad, gate, attended)


def tile_index(step):
    core = lax.axis_index("row") % 2
    slot = step // 2
    quarter = jnp.where(core == 0, 3 * slot, 1 + slot)
    return 2 * quarter + step % 2


def attend_kernel(tile, width, per_frame, scale, q_ref, kv_ref, out_ref, out_t_ref, lse_ref, vt_ref, sa_ref, sb_ref):
    step = pl.program_id(0)
    steps_of = scale * LOG2E
    @pl.when(step == 0)
    def _():
        vt_ref[64:72, :] = jnp.ones((8, vt_ref.shape[1]), BF)
        @pl.loop(0, kv_ref.shape[0] // tile)
        def _(j):
            rows = pl.ds(pl.multiple_of(j * tile, tile), tile)
            vt_ref[0:64, rows] = kv_ref[rows, :].T[64:, :]
    low = low_lanes((tile, LANES))
    packed = q_ref[...].astype(F32)
    packed = jnp.where(step % 2 == 0, packed, pltpu.roll(packed, 64, 1))
    query = jnp.where(low, packed, 0.0).astype(BF)
    def rows_of(part):
        return pl.ds(pl.multiple_of(part * width, width), width)
    def score(part, ref):
        ref[...] = dot(kv_ref[rows_of(part), :], query, 1, 1)
    def absorb(part, ref, carry, start):
        top, total = carry
        scores = ref[...] * steps_of
        if start is not None:
            key = (lax.broadcasted_iota(jnp.int32, (width, 1), 0) + start) // per_frame
            ask = lax.broadcasted_iota(jnp.int32, (1, tile), 1) // per_frame
            scores = jnp.where(key <= ask, scores, -1e30)
        new_top = jnp.maximum(top, jnp.max(scores, axis=0, keepdims=True))
        probs = jnp.exp2(scores - new_top).astype(BF)
        total = total * jnp.exp2(top - new_top) + dot(vt_ref[:, rows_of(part)], probs, 1, 0)
        return new_top, total
    last = tile_index(step)
    score(0, sa_ref)
    def body(j, carry):
        score(2 * j + 1, sb_ref)
        carry = absorb(2 * j, sa_ref, carry, None)
        score(2 * j + 2, sa_ref)
        return absorb(2 * j + 1, sb_ref, carry, None)
    carry = (jnp.full((1, tile), -1e30, F32), jnp.zeros((72, tile), F32))
    carry = lax.fori_loop(0, last, body, carry)
    score(2 * last + 1, sb_ref)
    carry = absorb(2 * last, sa_ref, carry, 0)
    top, total = absorb(2 * last + 1, sb_ref, carry, width)
    norm = total[64:65, :]
    lse_ref[0] = top + jnp.log2(norm)
    result = (total[:64, :] / norm).astype(BF)
    @pl.when(step % 2 == 0)
    def _():
        out_t_ref[0, 0:64, :] = result
    @pl.when(step % 2 == 1)
    def _():
        out_t_ref[0, 64:128, :] = result
        out_ref[...] = out_t_ref[0].T


def attend(queries, keys_values, tile, per_frame, scale):
    one = pl.Buffered(1)
    return pl.pallas_call(
        partial(attend_kernel, tile, tile // 2, per_frame, scale),
        grid=(4,),
        in_specs=[
            pl.BlockSpec((tile, LANES), lambda i: (i // 2, 0)),
            pl.BlockSpec(keys_values.shape, lambda i: (0, 0), pipeline_mode=one),
        ],
        out_specs=[
            pl.BlockSpec((tile, LANES), lambda i: (i // 2, 0)),
            pl.BlockSpec((1, LANES, tile), lambda i: (i // 2, 0, 0)),
            pl.BlockSpec((1, 1, tile), lambda i: (i, 0, 0)),
        ],
        out_shape=[
            jax.ShapeDtypeStruct((2 * tile, LANES), BF),
            jax.ShapeDtypeStruct((2, LANES, tile), BF),
            jax.ShapeDtypeStruct((4, 1, tile), F32),
        ],
        scratch_shapes=[
            pltpu.VMEM((72, keys_values.shape[0]), BF),
            pltpu.VMEM((tile // 2, tile), F32),
            pltpu.VMEM((tile // 2, tile), F32),
        ],
        compiler_params=pltpu.CompilerParams(
            dimension_semantics=("arbitrary",), vmem_limit_bytes=60 * MIB
        ),
        cost_estimate=pl.CostEstimate(
            flops=4_000_000_000, bytes_accessed=8_000_000, transcendentals=0
        ),
        name="attend",
    )(queries, keys_values)


def attend_back_kernel(tile, width, per_frame, scale, q_ref, do_ref, lse_ref, out_t_ref, kv_ref, dq_ref, dkv_ref, kt_ref, acc_ref, dq_t_ref, delta_ref, sa, pa, sb, pb):
    step = pl.program_id(0)
    steps_of = scale * LOG2E
    @pl.when(step == 0)
    def _():
        @pl.loop(0, kv_ref.shape[0] // tile)
        def _(j):
            rows = pl.ds(pl.multiple_of(j * tile, tile), tile)
            kt_ref[:, rows] = kv_ref[rows, :].T[:64, :]
            acc_ref[rows, :] = jnp.zeros((tile, LANES), F32)
    @pl.when(step % 2 == 0)
    def _():
        prod = do_ref[...].astype(F32).T * out_t_ref[0].astype(F32)
        delta_ref[0] = jnp.sum(prod[:64], axis=0, keepdims=True)
        delta_ref[1] = jnp.sum(prod[64:], axis=0, keepdims=True)
    low = low_lanes((tile, LANES))
    first = step % 2 == 0
    packed = q_ref[...].astype(F32)
    packed = jnp.where(first, packed, pltpu.roll(packed, 64, 1))
    query = jnp.where(low, packed, 0.0).astype(BF)
    packed = do_ref[...].astype(F32)
    packed = jnp.where(first, pltpu.roll(packed, 64, 1), packed)
    down = jnp.where(low, 0.0, packed).astype(BF)
    lse = lse_ref[0]
    delta = delta_ref[step % 2]
    def rows_of(part):
        return pl.ds(pl.multiple_of(part * width, width), width)
    def score(part, s, p):
        pieces = kv_ref[rows_of(part), :]
        s[...] = dot(pieces, query, 1, 1)
        p[...] = dot(pieces, down, 1, 1)
    def absorb(part, s, p, dq, start):
        rows = rows_of(part)
        probs = jnp.exp2(s[...] * steps_of - lse)
        if start is not None:
            key = lax.broadcasted_iota(jnp.int32, (width, 1), 0) + start
            ask = lax.broadcasted_iota(jnp.int32, (1, tile), 1)
            probs = jnp.where(key // per_frame <= ask // per_frame, probs, 0.0)
        dscore = (probs * (p[...] - delta)).astype(BF)
        acc_ref[rows, :] += dot(dscore, query, 1, 0) + dot(probs.astype(BF), down, 1, 0)
        return dq + dot(kt_ref[:, rows], dscore, 1, 0)
    last = tile_index(step)
    parts = tile // width
    dq = jnp.zeros((64, tile), F32)
    slots = ((sa, pa), (sb, pb))
    score(0, *slots[0])
    def body(j, dq):
        for i in range(parts):
            score(j * parts + i + 1, *slots[(i + 1) % 2])
            dq = absorb(j * parts + i, *slots[i % 2], dq, None)
        return dq
    dq = lax.fori_loop(0, last, body, dq)
    for i in range(parts):
        if i + 1 < parts:
            score(last * parts + i + 1, *slots[(i + 1) % 2])
        dq = absorb(last * parts + i, *slots[i % 2], dq, i * width)
    dq = dq * scale
    @pl.when(step % 2 == 0)
    def _():
        dq_t_ref[0:64, :] = dq
    @pl.when(step % 2 == 1)
    def _():
        dq_t_ref[64:128, :] = dq
        dq_ref[...] = dq_t_ref[...].T.astype(BF)
    @pl.when(step == 3)
    def _():
        @pl.loop(0, kv_ref.shape[0] // tile)
        def _(j):
            rows = pl.ds(pl.multiple_of(j * tile, tile), tile)
            total = acc_ref[rows, :]
            dkv_ref[rows, :] = jnp.where(low_lanes((tile, LANES)), total * scale, total).astype(BF)


def attend_back(queries, downs, lse, out_t, keys_values, tile, per_frame, scale):
    one = pl.Buffered(1)
    keys = keys_values.shape[0]
    packed = pl.BlockSpec((tile, LANES), lambda i: (i // 2, 0))
    whole = pl.BlockSpec(keys_values.shape, lambda i: (0, 0), pipeline_mode=one)
    return pl.pallas_call(
        partial(attend_back_kernel, tile, tile // 2, per_frame, scale),
        grid=(4,),
        in_specs=[
            packed,
            packed,
            pl.BlockSpec((1, 1, tile), lambda i: (i, 0, 0)),
            pl.BlockSpec((1, LANES, tile), lambda i: (i // 2, 0, 0)),
            whole,
        ],
        out_specs=[packed, pl.BlockSpec(keys_values.shape, lambda i: (0, 0))],
        out_shape=[
            jax.ShapeDtypeStruct((2 * tile, LANES), BF),
            jax.ShapeDtypeStruct(keys_values.shape, BF),
        ],
        scratch_shapes=[
            pltpu.VMEM((64, keys), BF),
            pltpu.VMEM((keys, LANES), F32),
            pltpu.VMEM((LANES, tile), F32),
            pltpu.VMEM((2, 1, tile), F32),
        ]
        + [pltpu.VMEM((tile // 2, tile), F32)] * 4,
        compiler_params=pltpu.CompilerParams(
            dimension_semantics=("arbitrary",), vmem_limit_bytes=60 * MIB
        ),
        cost_estimate=pl.CostEstimate(
            flops=8_000_000_000, bytes_accessed=12_000_000, transcendentals=0
        ),
        name="attend_back",
    )(queries, downs, lse, out_t, keys_values)


def exchange_kernel(axis, moves, sources, results, pair_of, work, finish, *refs):
    in_refs, refs = refs[:sources], refs[sources:]
    out_refs, refs = refs[:results], refs[results:]
    send_sem, recv_sem, own_sem = refs[-3:]
    scratch = refs[:-3]
    dests = scratch if finish is not None else out_refs
    me, count = lax.axis_index(axis), lax.axis_size(axis)
    barrier = pltpu.get_barrier_semaphore()
    for step in range(1, count):
        pl.semaphore_signal(
            barrier,
            inc=1,
            device_id={axis: lax.rem(me + step, count)},
            device_id_type=pl.DeviceIdType.MESH,
        )
    pl.semaphore_wait(barrier, count - 1)
    copies = []
    for step in range(1, count):
        peer = lax.rem(me + step, count)
        for index, (source, dest, take, place) in enumerate(moves):
            copies.append(
                pltpu.make_async_remote_copy(
                    src_ref=take(in_refs[source], peer),
                    dst_ref=place(dests[dest], me, peer),
                    send_sem=send_sem.at[index, step - 1],
                    recv_sem=recv_sem.at[index, step - 1],
                    device_id={axis: peer},
                    device_id_type=pl.DeviceIdType.MESH,
                )
            )
            copies[-1].start()
    for index, (source, dest, take, place) in enumerate(moves):
        copies.append(
            pltpu.make_async_copy(
                take(in_refs[source], me), place(dests[dest], me, me), own_sem.at[index]
            )
        )
        copies[-1].start()
    if work is not None:
        work(in_refs, out_refs)
    for copy in copies:
        copy.wait()
    if pair_of is not None:
        core = lax.rem(me, 2)
        ref = dests[pair_of].at[core]
        copy = pltpu.make_async_remote_copy(
            src_ref=ref,
            dst_ref=ref,
            send_sem=own_sem.at[len(moves)],
            recv_sem=own_sem.at[len(moves) + 1],
            device_id={axis: me + 1 - 2 * core},
            device_id_type=pl.DeviceIdType.MESH,
        )
        copy.start()
        copy.wait()
    if finish is not None:
        finish(dests, in_refs, out_refs)


def exchange(
    name,
    axis,
    number,
    moves,
    arrays,
    shapes,
    pair_of=None,
    work=None,
    finish=None,
    landing=(),
    away=False,
    limit=40,
):
    count = lax.axis_size(axis)
    vmem = pl.BlockSpec(memory_space=pltpu.VMEM)
    out_spec = pl.BlockSpec(memory_space=pltpu.HBM) if away else vmem
    sent = sum(a.size * a.dtype.itemsize for a in arrays)
    return pl.pallas_call(
        partial(
            exchange_kernel, axis, moves, len(arrays), len(shapes), pair_of, work, finish
        ),
        in_specs=[vmem] * len(arrays),
        out_specs=[out_spec] * len(shapes),
        out_shape=[jax.ShapeDtypeStruct(*shape) for shape in shapes],
        scratch_shapes=[pltpu.VMEM(*shape) for shape in landing]
        + [
            pltpu.SemaphoreType.DMA((len(moves), count - 1)),
            pltpu.SemaphoreType.DMA((len(moves), count - 1)),
            pltpu.SemaphoreType.DMA((len(moves) + 2,)),
        ],
        compiler_params=pltpu.CompilerParams(
            collective_id=number, has_side_effects=True, vmem_limit_bytes=limit * MIB
        ),
        cost_estimate=pl.CostEstimate(
            flops=0, bytes_accessed=20_000_000 + 30 * sent, transcendentals=0
        ),
        name=name,
    )(*arrays)


def all_of(ref, peer):
    return ref


def block_of(ref, peer):
    return ref.at[peer]


def at_sender(ref, me, peer):
    return ref.at[me]


def lanes_of(size):
    def view(ref, peer):
        return ref.at[:, pl.ds(pl.multiple_of(peer * size, LANES), size)]

    return view


def lanes_at(size):
    def view(ref, me, peer):
        return ref.at[:, pl.ds(pl.multiple_of(me * size, LANES), size)]

    return view


def add_landed(dests, in_refs, out_refs):
    landed, out = dests[0], out_refs[0]
    rows = out.shape[0]
    step = 32 if rows % 32 == 0 else rows

    @pl.loop(0, rows // step)
    def _(j):
        cut = pl.ds(pl.multiple_of(j * step, step), step)
        total = landed[0, cut, :].astype(F32)
        for other in range(1, landed.shape[0]):
            total += landed[other, cut, :].astype(F32)
        out[cut, :] = total.astype(out.dtype)


def gather(name, axis, number, arrays):
    count = lax.axis_size(axis)
    moves = [(i, i, all_of, at_sender) for i in range(len(arrays))]
    return exchange(
        name, axis, number, moves, arrays, [((count,) + a.shape, a.dtype) for a in arrays]
    )


def back_kernel(
    q_ref, kv_ref, out_ref, landed, summed, send_sem, recv_sem, own_sem, pair_sem
):
    me, count = lax.axis_index("row"), lax.axis_size("row")
    core = lax.rem(me, 2)
    barrier = pltpu.get_barrier_semaphore()
    for step in range(1, count):
        pl.semaphore_signal(
            barrier,
            inc=1,
            device_id={"row": lax.rem(me + step, count)},
            device_id_type=pl.DeviceIdType.MESH,
        )
    pl.semaphore_wait(barrier, count - 1)
    half = pltpu.make_async_remote_copy(
        src_ref=kv_ref.at[1 - core],
        dst_ref=landed,
        send_sem=pair_sem.at[0],
        recv_sem=pair_sem.at[1],
        device_id={"row": me + 1 - 2 * core},
        device_id_type=pl.DeviceIdType.MESH,
    )
    half.start()

    def send(index, source, dest, step):
        peer = lax.rem(me + step, count)
        copy = pltpu.make_async_remote_copy(
            src_ref=source.at[:, :, peer],
            dst_ref=dest,
            send_sem=send_sem.at[index, step - 1],
            recv_sem=recv_sem.at[index, step - 1],
            device_id={"row": peer},
            device_id_type=pl.DeviceIdType.MESH,
        )
        copy.start()
        return copy

    copies = [send(0, q_ref, out_ref.at[me, 0:2], step) for step in range(1, count)]
    copies.append(
        pltpu.make_async_copy(q_ref.at[:, :, me], out_ref.at[me, 0:2], own_sem.at[0])
    )
    copies[-1].start()
    half.wait()
    for part in range(summed.shape[0]):

        @pl.loop(0, summed.shape[1])
        def _(j):
            total = kv_ref[core, part, j].astype(F32) + landed[part, j].astype(F32)
            summed[part, j] = total.astype(BF)

    copies += [send(1, summed, out_ref.at[me, 2:6], step) for step in range(1, count)]
    copies.append(
        pltpu.make_async_copy(summed.at[:, :, me], out_ref.at[me, 2:6], own_sem.at[1])
    )
    copies[-1].start()
    for copy in copies:
        copy.wait()


def exchange_back(number, queries, keys_values, shape):
    count = lax.axis_size("row")
    vmem = pl.BlockSpec(memory_space=pltpu.VMEM)
    return pl.pallas_call(
        back_kernel,
        in_specs=[vmem] * 2,
        out_specs=vmem,
        out_shape=jax.ShapeDtypeStruct(*shape),
        scratch_shapes=[
            pltpu.VMEM(keys_values.shape[1:], BF),
            pltpu.VMEM(keys_values.shape[1:], BF),
            pltpu.SemaphoreType.DMA((2, count - 1)),
            pltpu.SemaphoreType.DMA((2, count - 1)),
            pltpu.SemaphoreType.DMA((2,)),
            pltpu.SemaphoreType.DMA((2,)),
        ],
        compiler_params=pltpu.CompilerParams(
            collective_id=number, has_side_effects=True, vmem_limit_bytes=40 * MIB
        ),
        cost_estimate=pl.CostEstimate(flops=0, bytes_accessed=80_000_000, transcendentals=0),
        name="grad_to_tokens",
    )(queries, keys_values)


def square_gather_kernel(in_ref, out_ref, send_sem, recv_sem, own_sem):
    me = lax.axis_index("frame")
    near = (me + 1 - 2 * lax.rem(me, 2), me + 2 - 4 * (me // 2))
    barrier = pltpu.get_barrier_semaphore()
    for peer in near:
        pl.semaphore_signal(
            barrier, inc=1, device_id={"frame": peer}, device_id_type=pl.DeviceIdType.MESH
        )
    pl.semaphore_wait(barrier, 2)
    half = in_ref.shape[0] // 2
    cuts = (pl.ds(0, half), pl.ds(half, half))

    def copy_of(source, dest, way, index):
        return pltpu.make_async_remote_copy(
            src_ref=source,
            dst_ref=dest,
            send_sem=send_sem.at[way, index],
            recv_sem=recv_sem.at[way, index],
            device_id={"frame": near[way]},
            device_id_type=pl.DeviceIdType.MESH,
        )

    first, second, third = [], [], []
    for way in range(2):
        first.append(copy_of(in_ref.at[cuts[way]], out_ref.at[me, cuts[way]], way, 0))
        first[-1].start()
    for way in range(2):
        rest = cuts[1 - way]
        second.append(copy_of(in_ref.at[rest], out_ref.at[me, rest], way, 1))
        second[-1].start()
    own = pltpu.make_async_copy(in_ref, out_ref.at[me], own_sem)
    own.start()
    for way in range(2):
        first[way].wait_recv()
        block = out_ref.at[near[way], cuts[way]]
        third.append(copy_of(block, block, 1 - way, 2))
        third[-1].start()
    for way in range(2):
        first[way].wait_send()
        second[way].wait()
        third[way].wait()
    own.wait()


def gather_frame(name, number, array):
    if lax.axis_size("frame") != 4:
        return gather(name, "frame", number, [array])[0]
    vmem = pl.BlockSpec(memory_space=pltpu.VMEM)
    return pl.pallas_call(
        square_gather_kernel,
        in_specs=[vmem],
        out_specs=vmem,
        out_shape=jax.ShapeDtypeStruct((4,) + array.shape, array.dtype),
        scratch_shapes=[
            pltpu.SemaphoreType.DMA((2, 3)),
            pltpu.SemaphoreType.DMA((2, 3)),
            pltpu.SemaphoreType.DMA,
        ],
        compiler_params=pltpu.CompilerParams(
            collective_id=number, has_side_effects=True, vmem_limit_bytes=40 * MIB
        ),
        cost_estimate=pl.CostEstimate(flops=0, bytes_accessed=30_000_000, transcendentals=0),
        name=name,
    )(array)


def scatter_sum(name, axis, number, parts, dtype=F32):
    return exchange(
        name,
        axis,
        number,
        [(0, 0, block_of, at_sender)],
        [parts],
        [(parts.shape[1:], dtype)],
        finish=add_landed,
        landing=[(parts.shape, parts.dtype)],
    )[0]


def cut_kernel(slice_width, hidden_slice, in_ref, out_ref, up_ref, down_ref, *refs):
    own_in, own_rest, own_down, sems = refs
    frame = lax.axis_index("frame")
    width = out_ref.shape[1]
    hidden = pl.ds(pl.multiple_of(frame * hidden_slice, LANES), hidden_slice)
    pieces = [
        (out_ref, own_rest.at[:, 0:width]),
        (up_ref.at[:, hidden], own_rest.at[:, width : width + hidden_slice]),
        (down_ref.at[:, hidden], own_down),
    ]
    for part in range(4):
        start = pl.multiple_of(part * width + frame * slice_width, LANES)
        pieces.append(
            (
                in_ref.at[:, pl.ds(start, slice_width)],
                own_in.at[:, part * slice_width : (part + 1) * slice_width],
            )
        )
    copies = [
        pltpu.make_async_copy(source, dest, sems.at[index])
        for index, (source, dest) in enumerate(pieces)
    ]
    for copy in copies:
        copy.start()
    for copy in copies:
        copy.wait()


def cut_weights(attn_in, out_weight, up_weight, down_weight, slice_width, hidden_slice):
    rows, width = out_weight.shape
    vmem = pl.BlockSpec(memory_space=pltpu.VMEM)
    return pl.pallas_call(
        partial(cut_kernel, slice_width, hidden_slice),
        in_specs=[pl.BlockSpec(memory_space=pl.ANY)] * 4,
        out_specs=[vmem] * 3,
        out_shape=[
            jax.ShapeDtypeStruct((rows, 4 * slice_width), BF),
            jax.ShapeDtypeStruct((rows, width + hidden_slice), BF),
            jax.ShapeDtypeStruct((rows, hidden_slice), BF),
        ],
        scratch_shapes=[pltpu.SemaphoreType.DMA((7,))],
        name="cut_weights",
    )(attn_in, out_weight, up_weight, down_weight)


def join_kernel(hidden_slice, parts_ref, up_ref, down_ref, out_ref):
    total = None
    for part in range(parts_ref.shape[0]):
        cut = slice(part * hidden_slice, (part + 1) * hidden_slice)
        up_ref[:, cut] = parts_ref[part, :, :hidden_slice].astype(F32)
        down_ref[:, cut] = parts_ref[part, :, hidden_slice : 2 * hidden_slice].astype(F32)
        last = parts_ref[part, :, 2 * hidden_slice :].astype(F32)
        total = last if total is None else total + last
    out_ref[...] = total


def join_in_kernel(width, slice_width, parts_ref, in_ref):
    for part in range(parts_ref.shape[0]):
        for group in range(4):
            start = group * width + part * slice_width
            in_ref[:, start : start + slice_width] = parts_ref[
                part, :, group * slice_width : (group + 1) * slice_width
            ].astype(F32)


def join(name, body, parts, widths):
    count, rows, columns = parts.shape
    step = rows // 4
    return pl.pallas_call(
        body,
        grid=(4,),
        in_specs=[pl.BlockSpec((count, step, columns), lambda i: (0, i, 0))],
        out_specs=[pl.BlockSpec((step, w), lambda i: (i, 0)) for w in widths],
        out_shape=[jax.ShapeDtypeStruct((rows, w), F32) for w in widths],
        compiler_params=pltpu.CompilerParams(dimension_semantics=("arbitrary",)),
        cost_estimate=pl.CostEstimate(flops=0, bytes_accessed=8_000_000, transcendentals=0),
        name=name,
    )(parts)


def grads_beside(cut):
    def work(in_refs, out_refs):
        hid_ref, pre_ref, cot_ref, act_ref, down_ref = in_refs[1:]
        grads_ref, branch_ref = out_refs[1:]
        columns = pre_ref.shape[1]
        block = max(cut, LANES)
        count = hid_ref.shape[1] // block
        rows = branch_ref.shape[0] // count

        @pl.loop(0, count)
        def _(i):
            lanes = pl.ds(pl.multiple_of(i * block, LANES), block)
            for part, (left, right) in enumerate(((hid_ref, pre_ref), (cot_ref, act_ref))):
                result = dot(left[:, lanes], right[...], 0, 0).astype(BF)
                for piece in range(block // cut):
                    grads_ref[
                        i * (block // cut) + piece, :, part * columns : (part + 1) * columns
                    ] = result[piece * cut : (piece + 1) * cut]
            own = pl.ds(pl.multiple_of(i * rows, rows), rows)
            branch_ref[own, :] = dot(act_ref[own, :], down_ref[...], 1, 1).astype(BF)

    return work


def out_grad_kernel(cut, gated_ref, grad_ref, before_ref, out_ref):
    result = dot(gated_ref[...], grad_ref[...], 0, 0).astype(BF)
    for piece in range(out_ref.shape[0]):
        out_ref[piece] = result[piece * cut : (piece + 1) * cut]


def add_out_grad(gated, grad, grads):
    row_devs, cut, columns = grads.shape
    tokens, width = gated.shape
    block = max(cut, LANES)
    last = (columns - width) // width
    assert columns % width == 0
    return pl.pallas_call(
        partial(out_grad_kernel, cut),
        grid=(width // block,),
        in_specs=[
            pl.BlockSpec((tokens, block), lambda i: (0, i)),
            pl.BlockSpec(grad.shape, lambda i: (0, 0), pipeline_mode=pl.Buffered(1)),
            pl.BlockSpec(memory_space=pl.ANY),
        ],
        out_specs=pl.BlockSpec((block // cut, cut, width), lambda i: (i, 0, last)),
        out_shape=jax.ShapeDtypeStruct(grads.shape, BF),
        input_output_aliases={2: 0},
        compiler_params=pltpu.CompilerParams(dimension_semantics=("arbitrary",)),
        cost_estimate=pl.CostEstimate(
            flops=600_000_000, bytes_accessed=5_000_000, transcendentals=0
        ),
        name="out_grad",
    )(gated, grad, grads)


def on_device(
    tokens,
    timesteps,
    noise_table,
    mod_weight,
    mod_bias,
    attn_in,
    out_weight,
    up_weight,
    down_weight,
    cotangent,
):
    clips, frames, rows_dev, grid_side, width = tokens.shape
    frame_index = lax.axis_index("frame")
    row_index = lax.axis_index("row")
    frame_devs, row_devs = lax.axis_size("frame"), lax.axis_size("row")
    core = row_index % 2
    clip_len = frames * frame_devs
    head_dim = width // HEADS
    heads = HEADS // frame_devs
    slice_width = width // frame_devs
    per_frame_dev = rows_dev * grid_side
    per_frame = grid_side * grid_side
    token_count = clips * frames * per_frame_dev
    group_count = token_count * frame_devs
    tile = clip_len // 8 * per_frame
    scale = head_dim ** (-0.5)
    step_count = noise_table.shape[0]
    assert head_dim == 64 and row_devs == 2 * clips * heads

    def by_frames(values):
        parts = values.reshape(frame_devs, clips, frames * per_frame_dev, -1)
        return jnp.transpose(parts, (1, 0, 2, 3)).reshape(group_count, values.shape[-1])

    def to_frames(values):
        parts = values.reshape(clips, frame_devs, frames * per_frame_dev, -1)
        return jnp.transpose(parts, (1, 0, 2, 3)).reshape(frame_devs, token_count, -1)

    def gather_frames(values):
        full = lax.all_gather(values, "frame", axis=1, tiled=True)
        return full.reshape(group_count, values.shape[-1])

    def scatter_frames(values):
        parts = to_frames(values).reshape(group_count, width)
        return lax.psum_scatter(parts, "frame", scatter_dimension=0, tiled=True).reshape(
            tokens.shape
        )

    hidden_slice = up_weight.shape[1] // frame_devs
    own_in, own_rest, own_down = cut_weights(
        attn_in, out_weight, up_weight, down_weight, slice_width, hidden_slice
    )
    weight_in = lax.all_gather(own_in, "row", axis=0, tiled=True)

    steps_iota = lax.broadcasted_iota(jnp.int32, (1, 1, step_count), 2)
    one_hot = (timesteps[:, :, None] == steps_iota).astype(BF)
    embedding = jnp.einsum("cls,sd->cld", one_hot, noise_table, preferred_element_type=F32)
    silu_low = jax.nn.silu(embedding).astype(BF)
    mod_local = jnp.einsum(
        "cld,de->cle", silu_low, mod_weight, preferred_element_type=F32
    ) + mod_bias.astype(F32)
    mod_width = mod_local.shape[2]
    modulation = exchange(
        "gather_mod",
        "row",
        0,
        [(0, 0, all_of, lanes_at(mod_width))],
        [mod_local.astype(BF).reshape(clips * frames, mod_width)],
        [((clips * frames, mod_width * row_devs), BF)],
    )[0].astype(F32)
    modulation = modulation.reshape(clips, frames, 6, 1, 1, width)
    shift_one, scale_one, gate_one, shift_two, scale_two, gate_two = [
        modulation[:, :, part] for part in range(6)
    ]

    frame_freq, row_freq, col_freq = [np.tile(t, 4) for t in rotary_freqs(head_dim // 2)]
    shape_three = (clip_len, rows_dev, grid_side, LANES)
    frame_pos = lax.broadcasted_iota(F32, shape_three, 0)
    row_pos = (row_index * rows_dev + lax.broadcasted_iota(jnp.int32, shape_three, 1)).astype(F32)
    col_pos = lax.broadcasted_iota(F32, shape_three, 2)
    angles = (frame_pos * frame_freq + row_pos * row_freq + col_pos * col_freq).reshape(-1, LANES)
    sign = np.where(np.arange(LANES) % 64 < 32, -1.0, 1.0).astype(np.float32)
    cosines = jnp.cos(angles)
    sines = jnp.sin(angles) * sign

    token_f = tokens.astype(F32)
    hidden_one, norm_one_pull = jax.vjp(modulate, token_f, shift_one, scale_one)
    hidden_group = by_frames(
        gather_frame("gather_one", 1, hidden_one.astype(BF).reshape(token_count, width))
    )

    grad_out = cotangent.astype(F32)
    grad_branch_two = (grad_out * gate_two).astype(BF)
    hidden_group, grad_branch_two = lax.optimization_barrier((hidden_group, grad_branch_two))
    grad_two_group = gather_frames(grad_branch_two)

    pack, gate_raw = qkv_project(hidden_group, weight_in, cosines, sines, clips, heads)

    half = tile // row_devs

    spans = half // per_frame_dev
    by_token = (spans, per_frame_dev, LANES)
    by_head = (spans, row_devs, per_frame_dev, LANES)

    def peer_rows(ref, peer):
        return ref.at[:, :, peer]

    queries, keys_values = exchange(
        "to_heads",
        "row",
        2,
        [
            (0, 0, lambda r, p: r.at[p, 0:2], lambda r, me, p: r.at[:, :, me]),
            (0, 1, lambda r, p: r.at[p, 2:6], lambda r, me, p: r.at[p % 2, :, :, me]),
        ],
        [pack.reshape((row_devs, 6) + by_token)],
        [((2,) + by_head, BF), ((2, 4) + by_head, BF)],
        pair_of=1,
        away=True,
    )
    queries = queries.reshape(-1, LANES)
    keys_values = keys_values.reshape(-1, LANES)

    queries, keys_values, grad_two_group, own_rest, own_down = lax.optimization_barrier(
        (queries, keys_values, grad_two_group, own_rest, own_down)
    )
    rest = lax.all_gather(own_rest, "row", axis=0, tiled=True)
    full_out, weight_up = rest[:, :width], rest[:, width:]
    attended_heads, attended_t, lse = attend(queries, keys_values, tile, per_frame, scale)
    gated_group, attended = exchange(
        "to_tokens",
        "row",
        3,
        [(0, 0, peer_rows, at_sender)],
        [attended_heads.reshape((2,) + by_head), gate_raw],
        [(gate_raw.shape, BF)] * 2,
        finish=gate_landed(clips, heads),
        landing=[((row_devs, 2) + by_token, BF)],
    )

    steps_wide = jnp.broadcast_to(timesteps.reshape(-1, 1), (clips * frames, LANES))
    gated, steps_parts = exchange(
        "gated_back",
        "frame",
        4,
        [(0, 0, block_of, lanes_at(slice_width)), (1, 1, all_of, at_sender)],
        [to_frames(gated_group), steps_wide],
        [((token_count, width), BF), ((frame_devs,) + steps_wide.shape, jnp.int32)],
    )
    branch_one = jnp.dot(gated, full_out, preferred_element_type=F32).reshape(tokens.shape)
    after_one = token_f + gate_one * branch_one
    hidden_two, norm_two_pull = jax.vjp(modulate, after_one, shift_two, scale_two)
    hidden_two, own_down = lax.optimization_barrier((hidden_two, own_down))
    weight_down = lax.all_gather(own_down, "row", axis=0, tiled=True)
    hidden_two_group = by_frames(
        gather_frame("gather_two", 5, hidden_two.astype(BF).reshape(token_count, width))
    )

    pre_act = jnp.dot(hidden_two_group, weight_up, preferred_element_type=F32)
    act_values, gelu_pull = jax.vjp(partial(jax.nn.gelu, approximate=True), pre_act)
    act_low = act_values.astype(BF)
    grad_act = jnp.dot(grad_two_group, weight_down, preferred_element_type=F32)
    (grad_pre,) = gelu_pull(grad_act)
    grad_pre = grad_pre.astype(BF)
    parts = to_frames(dot(grad_pre, weight_up, 1, 1).astype(BF))
    cut = width // row_devs
    grad_hidden_two, weight_grads, branch_two = exchange(
        "scatter_two",
        "frame",
        6,
        [(0, 0, block_of, at_sender)],
        [parts, hidden_two_group, grad_pre, grad_two_group, act_low, weight_down],
        [
            (parts.shape[1:], F32),
            ((row_devs, cut, 2 * hidden_slice + width), BF),
            ((group_count, width), BF),
        ],
        work=grads_beside(cut),
        finish=add_landed,
        landing=[(parts.shape, BF)],
        limit=56,
    )
    grad_hidden_two = grad_hidden_two.reshape(tokens.shape)
    branch_two = scatter_frames(branch_two)
    grad_after_part, grad_shift_two, grad_scale_two = norm_two_pull(grad_hidden_two)
    grad_after = grad_out + grad_after_part
    grad_gate_one = jnp.sum(grad_after * branch_one, axis=(2, 3), keepdims=True)
    grad_branch_one = (grad_after * gate_one).astype(BF).reshape(token_count, width)
    grad_gated = dot(grad_branch_one, full_out, 1, 1).astype(BF)
    weight_grads = add_out_grad(gated, grad_branch_one, weight_grads)
    grad_gated, weight_grads = lax.optimization_barrier((grad_gated, weight_grads))
    weight_grads = lax.psum_scatter(weight_grads, "row", scatter_dimension=0, tiled=True)
    (grad_gated,) = exchange(
        "grad_gated",
        "frame",
        7,
        [(0, 0, lanes_of(slice_width), at_sender)],
        [grad_gated],
        [((frame_devs, token_count, slice_width), BF)],
    )
    grad_gated = by_frames(grad_gated)
    down_pack, grad_gate = gate_back(grad_gated, gate_raw, attended, clips, heads)
    (downs,) = exchange(
        "grad_to_heads",
        "row",
        8,
        [(0, 0, block_of, lambda r, me, p: r.at[:, :, me])],
        [down_pack.reshape((row_devs, 2) + by_token)],
        [((2,) + by_head, BF)],
        away=True,
    )
    downs = downs.reshape(-1, LANES)
    downs, branch_two = lax.optimization_barrier((downs, branch_two))
    branch_two = branch_two.astype(F32)
    mixed = (after_one + gate_two * branch_two).astype(BF)
    grad_gate_two = jnp.sum(grad_out * branch_two, axis=(2, 3), keepdims=True)

    grad_queries, grad_kv = attend_back(
        queries, downs, lse, attended_t, keys_values, tile, per_frame, scale
    )
    grad_kv, weight_grads = lax.optimization_barrier((grad_kv, weight_grads))
    grads_all = lax.all_gather(weight_grads[0], "frame", axis=0, tiled=False)
    back_pack = exchange_back(
        9,
        grad_queries.reshape((2,) + by_head),
        grad_kv.reshape((2, 4) + by_head),
        ((row_devs, 6) + by_token, BF),
    )
    back_pack = back_pack.reshape(clips, heads, 2, 6, half, LANES)
    grad_mixed, grad_hidden = qkv_back(
        back_pack, grad_gate, weight_in, cosines, sines, clips, heads
    )
    grad_mixed, grads_all = lax.optimization_barrier((grad_mixed, grads_all))
    grad_hidden_one = scatter_sum("scatter_one", "frame", 10, to_frames(grad_hidden)).reshape(
        tokens.shape
    )
    in_grad = lax.psum_scatter(
        dot(hidden_group, grad_mixed, 0, 0).astype(BF), "row", scatter_dimension=0, tiled=True
    )

    grad_token_part, grad_shift_one, grad_scale_one = norm_one_pull(grad_hidden_one)
    tokens_grad = (grad_after + grad_token_part).astype(BF)

    grad_mod = jnp.stack(
        [
            grad_shift_one,
            grad_scale_one,
            grad_gate_one,
            grad_shift_two,
            grad_scale_two,
            grad_gate_two,
        ],
        axis=2,
    ).reshape(clips * frames, 6 * width)
    grad_mod = jnp.transpose(
        grad_mod.reshape(clips * frames, row_devs, mod_width), (1, 0, 2)
    )
    grad_mod = scatter_sum("scatter_mod", "row", 11, grad_mod, BF)
    grad_mod, in_grad = lax.optimization_barrier((grad_mod, in_grad))
    (grad_mod_all,) = gather("gather_grad_mod", "frame", 12, [grad_mod])
    grad_mod_all = grad_mod_all.reshape(-1, mod_width)
    steps_all = steps_parts.reshape(-1, LANES)[:, 0]
    hot_all = steps_all[:, None] == lax.broadcasted_iota(jnp.int32, (1, step_count), 1)
    embed_all = jnp.dot(hot_all.astype(BF), noise_table, preferred_element_type=F32)
    silu_all, silu_pull = jax.vjp(jax.nn.silu, embed_all)
    mod_weight_grad = dot(silu_all.astype(BF), grad_mod_all, 0, 0)
    mod_bias_grad = jnp.sum(grad_mod_all.astype(F32), axis=0)
    grad_silu = dot(grad_mod_all, mod_weight, 1, 1)
    frame_count, cut = grad_silu.shape[0], width // row_devs
    grad_silu = jnp.transpose(grad_silu.reshape(frame_count, row_devs, cut), (1, 0, 2))
    grad_silu = scatter_sum("scatter_silu", "row", 13, grad_silu)
    (grad_silu,) = gather("gather_silu", "row", 14, [grad_silu])
    grad_silu = jnp.transpose(grad_silu, (1, 0, 2)).reshape(frame_count, width)
    (grad_embedding,) = silu_pull(grad_silu)
    noise_table_grad = lax.dot_general(
        hot_all.astype(F32),
        grad_embedding,
        (((0,), (0,)), ((), ())),
        precision=lax.Precision.HIGHEST,
    )

    up_weight_grad, down_weight_grad, out_weight_grad = join(
        "join_grads",
        partial(join_kernel, hidden_slice),
        grads_all,
        (up_weight.shape[1], down_weight.shape[1], width),
    )
    in_all = lax.all_gather(in_grad, "frame", axis=0, tiled=False)
    (attn_in_grad,) = join(
        "join_in", partial(join_in_kernel, width, slice_width), in_all, (attn_in.shape[1],)
    )
    return (
        mixed,
        tokens_grad,
        noise_table_grad,
        mod_weight_grad,
        mod_bias_grad,
        attn_in_grad,
        out_weight_grad,
        up_weight_grad,
        down_weight_grad,
    )


def solution(mesh):
    in_specs = (
        P(None, "frame", "row", None, None),
        P(None, "frame"),
        P(),
        P(None, "row"),
        P("row"),
        P("row", None),
        P("row", None),
        P("row", None),
        P("row", None),
        P(None, "frame", "row", None, None),
    )
    out_specs = (
        P(None, "frame", "row", None, None),
        P(None, "frame", "row", None, None),
        P(),
        P(None, "row"),
        P("row"),
        P("row", None),
        P("row", None),
        P("row", None),
        P("row", None),
    )
    return jax.shard_map(
        on_device, mesh=mesh, in_specs=in_specs, out_specs=out_specs, check_vma=False
    )
```

```python
from functools import partial

import jax
import jax.numpy as jnp
import numpy as np
from jax import lax
from jax.experimental import pallas as pl
from jax.experimental.pallas import tpu as pltpu
from jax.sharding import PartitionSpec as P

HEADS = 16
EPS = 1e-06
LOG2E = 1.4426950408889634
F32 = jnp.float32
BF = jnp.bfloat16
LANES = 128
MIB = 1 << 20


def rotary_freqs(pair_count):
    third_count = pair_count // 3
    group_sizes = [pair_count - 2 * third_count, third_count, third_count]
    tables = []
    offset = 0
    for group_index in range(3):
        freq_table = np.zeros((pair_count,), np.float32)
        for inner_index in range(group_sizes[group_index]):
            freq_table[offset + inner_index] = 10000.0 ** (-inner_index / group_sizes[group_index])
        offset += group_sizes[group_index]
        tables.append(freq_table)
    return tables


def layer_norm(values):
    row_mean = jnp.mean(values, axis=-1, keepdims=True)
    centered = values - row_mean
    row_var = jnp.mean(centered * centered, axis=-1, keepdims=True)
    return centered * lax.rsqrt(row_var + EPS)


def modulate(values, shift, scale_part):
    return layer_norm(values) * (1.0 + scale_part) + shift


def dot(left, right, left_dim, right_dim):
    return lax.dot_general(
        left, right, (((left_dim,), (right_dim,)), ((), ())), preferred_element_type=F32
    )


def swap_halves(values):
    lane = lax.broadcasted_iota(jnp.int32, values.shape, 1)
    width = values.shape[1]
    return jnp.where(
        (lane % 64) < 32, pltpu.roll(values, width - 32, 1), pltpu.roll(values, 32, 1)
    )


def low_lanes(shape):
    return lax.broadcasted_iota(jnp.int32, shape, len(shape) - 1) < 64


def qkv_kernel(heads, hid_ref, w_ref, cos_ref, sin_ref, pack_ref, gate_ref):
    clip, quarter = pl.program_id(0), pl.program_id(1)
    width = heads * 64
    mixed = jnp.dot(hid_ref[...], w_ref[...], preferred_element_type=F32)
    cos, sin = cos_ref[...], sin_ref[...]
    rows = mixed.shape[0]
    half = rows // 2
    gate_ref[...] = mixed[:, 3 * width :]
    low = low_lanes((rows, LANES))
    low_half = low_lanes((half, LANES))
    query_set = jnp.where((quarter == 0) | (quarter == 3), 0, 1)
    slot = quarter // 2
    for pair in range(heads // 2):
        cut = slice(pair * LANES, (pair + 1) * LANES)
        query = mixed[:, cut]
        key = mixed[:, width + pair * LANES : width + (pair + 1) * LANES]
        value = mixed[:, 2 * width + pair * LANES : 2 * width + (pair + 1) * LANES]
        query = query * cos + swap_halves(query) * sin
        key = key * cos + swap_halves(key) * sin
        key_turn = pltpu.roll(key, 64, 1)
        value_turn = pltpu.roll(value, 64, 1)
        query_turn = pltpu.roll(query, 64, 1)
        packs = (
            (
                jnp.where(low, key, value_turn),
                jnp.where(low_half, query[:half], query_turn[half:]),
            ),
            (
                jnp.where(low, key_turn, value),
                jnp.where(low_half, query_turn[:half], query[half:]),
            ),
        )
        for inner, (key_value, queries) in enumerate(packs):
            head = 2 * pair + inner
            pack_ref[clip, head, query_set, slot] = queries.astype(BF)
            key_value = key_value.astype(BF)
            first = 2 + 2 * (quarter % 2)
            pack_ref[clip, head, quarter // 2, first] = key_value[:half]
            pack_ref[clip, head, quarter // 2, first + 1] = key_value[half:]


def qkv_project(hidden, weight, cos, sin, clips, heads):
    tokens, width = hidden.shape
    quarter = tokens // clips // 4
    one = pl.Buffered(1)
    return pl.pallas_call(
        partial(qkv_kernel, heads),
        grid=(clips, 4),
        in_specs=[
            pl.BlockSpec((quarter, width), lambda c, i: (c * 4 + i, 0)),
            pl.BlockSpec(weight.shape, lambda c, i: (0, 0), pipeline_mode=one),
            pl.BlockSpec((quarter, LANES), lambda c, i: (i, 0)),
            pl.BlockSpec((quarter, LANES), lambda c, i: (i, 0)),
        ],
        out_specs=[
            pl.BlockSpec(
                (clips, heads, 2, 6, quarter // 2, LANES), lambda c, i: (0, 0, 0, 0, 0, 0)
            ),
            pl.BlockSpec((quarter, heads * 64), lambda c, i: (c * 4 + i, 0)),
        ],
        out_shape=[
            jax.ShapeDtypeStruct((clips, heads, 2, 6, quarter // 2, LANES), BF),
            jax.ShapeDtypeStruct((tokens, heads * 64), F32),
        ],
        compiler_params=pltpu.CompilerParams(
            dimension_semantics=("arbitrary", "arbitrary"), vmem_limit_bytes=20 * MIB
        ),
        name="qkv_project",
    )(hidden, weight, cos, sin)


def qkv_back_kernel(heads, pack_ref, dgate_ref, w_ref, cos_ref, sin_ref, mixed_ref, hid_ref):
    clip, quarter = pl.program_id(0), pl.program_id(1)
    width = heads * 64
    cos, sin = cos_ref[...], sin_ref[...]
    rows = cos.shape[0]
    half = rows // 2
    low_half = low_lanes((half, LANES))
    query_set = jnp.where((quarter == 0) | (quarter == 3), 0, 1)
    slot = quarter // 2
    first = 2 + 2 * (quarter % 2)
    low = low_lanes((rows, LANES))
    for pair in range(heads // 2):
        even, odd = 2 * pair, 2 * pair + 1
        query_even = pack_ref[clip, even, query_set, slot].astype(F32)
        query_odd = pack_ref[clip, odd, query_set, slot].astype(F32)
        query = jnp.concatenate(
            [
                jnp.where(low_half, query_even, pltpu.roll(query_odd, 64, 1)),
                jnp.where(low_half, pltpu.roll(query_even, 64, 1), query_odd),
            ],
            axis=0,
        )
        both = []
        for head in (even, odd):
            both.append(
                jnp.concatenate(
                    [
                        pack_ref[clip, head, quarter // 2, first].astype(F32),
                        pack_ref[clip, head, quarter // 2, first + 1].astype(F32),
                    ],
                    axis=0,
                )
            )
        key = jnp.where(low, both[0], pltpu.roll(both[1], 64, 1))
        value = jnp.where(low, pltpu.roll(both[0], 64, 1), both[1])
        query = query * cos - swap_halves(query) * sin
        key = key * cos - swap_halves(key) * sin
        for part, values in enumerate((query, key, value)):
            start = part * width + pair * LANES
            mixed_ref[:, start : start + LANES] = values.astype(BF)
    mixed_ref[:, 3 * width :] = dgate_ref[...]
    hid_ref[...] = dot(mixed_ref[...], w_ref[...], 1, 1).astype(BF)


def qkv_back(pack, dgate, weight, cos, sin, clips, heads):
    tokens = dgate.shape[0]
    width = weight.shape[0]
    quarter = tokens // clips // 4
    one = pl.Buffered(1)
    return pl.pallas_call(
        partial(qkv_back_kernel, heads),
        grid=(clips, 4),
        in_specs=[
            pl.BlockSpec(pack.shape, lambda c, i: (0, 0, 0, 0, 0, 0), pipeline_mode=one),
            pl.BlockSpec((quarter, heads * 64), lambda c, i: (c * 4 + i, 0)),
            pl.BlockSpec(weight.shape, lambda c, i: (0, 0), pipeline_mode=one),
            pl.BlockSpec((quarter, LANES), lambda c, i: (i, 0)),
            pl.BlockSpec((quarter, LANES), lambda c, i: (i, 0)),
        ],
        out_specs=[
            pl.BlockSpec((quarter, 4 * heads * 64), lambda c, i: (c * 4 + i, 0)),
            pl.BlockSpec((quarter, width), lambda c, i: (c * 4 + i, 0)),
        ],
        out_shape=[
            jax.ShapeDtypeStruct((tokens, 4 * heads * 64), BF),
            jax.ShapeDtypeStruct((tokens, width), BF),
        ],
        compiler_params=pltpu.CompilerParams(
            dimension_semantics=("arbitrary", "arbitrary"), vmem_limit_bytes=20 * MIB
        ),
        name="qkv_back",
    )(pack, dgate, weight, cos, sin)


def unpack_pair(even, odd):
    low = low_lanes(even.shape)
    return jnp.concatenate(
        [
            jnp.where(low, even, pltpu.roll(odd, 64, 1)),
            jnp.where(low, pltpu.roll(even, 64, 1), odd),
        ],
        axis=0,
    )


def gate_landed(clips, heads):
    def finish(dests, in_refs, out_refs):
        pack_ref, gate_ref, (gated_ref, attended_ref) = dests[0], in_refs[1], out_refs
        quarter = gate_ref.shape[0] // clips // 4
        for clip in range(clips):
            for index in range(4):
                query_set, slot = (0, 1, 1, 0)[index], index // 2
                rows = pl.ds((clip * 4 + index) * quarter, quarter)
                for pair in range(heads // 2):
                    cut = slice(pair * LANES, (pair + 1) * LANES)
                    even, odd = [
                        pack_ref[(clip * heads + head) * 2 + query_set, slot]
                        .reshape(quarter // 2, LANES)
                        .astype(F32)
                        for head in (2 * pair, 2 * pair + 1)
                    ]
                    attended = unpack_pair(even, odd)
                    attended_ref[rows, cut] = attended.astype(BF)
                    gate = jax.nn.sigmoid(gate_ref[rows, cut])
                    gated_ref[rows, cut] = (attended * gate).astype(BF)

    return finish


def gate_back_kernel(heads, grad_ref, gate_ref, attended_ref, pack_ref, dgate_ref):
    clip, quarter = pl.program_id(0), pl.program_id(1)
    query_set = jnp.where((quarter == 0) | (quarter == 3), 0, 1)
    slot = quarter // 2
    rows = grad_ref.shape[0]
    half = rows // 2
    low = low_lanes((half, LANES))
    for pair in range(heads // 2):
        cut = slice(pair * LANES, (pair + 1) * LANES)
        sig = jax.nn.sigmoid(gate_ref[:, cut])
        grad = grad_ref[:, cut].astype(F32)
        dgate = grad * attended_ref[:, cut].astype(F32) * sig * (1.0 - sig)
        dgate_ref[:, cut] = dgate.astype(BF)
        down = grad * sig
        turn = pltpu.roll(down, 64, 1)
        pack_ref[clip, 2 * pair, query_set, slot] = jnp.where(low, down[:half], turn[half:]).astype(
            BF
        )
        pack_ref[clip, 2 * pair + 1, query_set, slot] = jnp.where(
            low, turn[:half], down[half:]
        ).astype(BF)


def gate_back(grad, gate, attended, clips, heads):
    tokens = gate.shape[0]
    quarter = tokens // clips // 4
    block = pl.BlockSpec((quarter, heads * 64), lambda c, i: (c * 4 + i, 0))
    pack_shape = (clips, heads, 2, 2, quarter // 2, LANES)
    return pl.pallas_call(
        partial(gate_back_kernel, heads),
        grid=(clips, 4),
        in_specs=[block, block, block],
        out_specs=[pl.BlockSpec(pack_shape, lambda c, i: (0, 0, 0, 0, 0, 0)), block],
        out_shape=[
            jax.ShapeDtypeStruct(pack_shape, BF),
            jax.ShapeDtypeStruct((tokens, heads * 64), BF),
        ],
        compiler_params=pltpu.CompilerParams(
            dimension_semantics=("arbitrary", "arbitrary"), vmem_limit_bytes=12 * MIB
        ),
        name="gate_back",
    )(grad, gate, attended)


def tile_index(step):
    core = lax.axis_index("row") % 2
    slot = step // 2
    quarter = jnp.where(core == 0, 3 * slot, 1 + slot)
    return 2 * quarter + step % 2


def attend_kernel(tile, width, per_frame, scale, q_ref, kv_ref, out_ref, out_t_ref, lse_ref, vt_ref, sa_ref, sb_ref):
    step = pl.program_id(0)
    steps_of = scale * LOG2E
    @pl.when(step == 0)
    def _():
        vt_ref[64:72, :] = jnp.ones((8, vt_ref.shape[1]), BF)
        @pl.loop(0, kv_ref.shape[0] // tile)
        def _(j):
            rows = pl.ds(pl.multiple_of(j * tile, tile), tile)
            vt_ref[0:64, rows] = kv_ref[rows, :].T[64:, :]
    low = low_lanes((tile, LANES))
    packed = q_ref[...].astype(F32)
    packed = jnp.where(step % 2 == 0, packed, pltpu.roll(packed, 64, 1))
    query = jnp.where(low, packed, 0.0).astype(BF)
    def rows_of(part):
        return pl.ds(pl.multiple_of(part * width, width), width)
    def score(part, ref):
        ref[...] = dot(kv_ref[rows_of(part), :], query, 1, 1)
    def absorb(part, ref, carry, start):
        top, total = carry
        scores = ref[...] * steps_of
        if start is not None:
            key = (lax.broadcasted_iota(jnp.int32, (width, 1), 0) + start) // per_frame
            ask = lax.broadcasted_iota(jnp.int32, (1, tile), 1) // per_frame
            scores = jnp.where(key <= ask, scores, -1e30)
        new_top = jnp.maximum(top, jnp.max(scores, axis=0, keepdims=True))
        probs = jnp.exp2(scores - new_top).astype(BF)
        total = total * jnp.exp2(top - new_top) + dot(vt_ref[:, rows_of(part)], probs, 1, 0)
        return new_top, total
    last = tile_index(step)
    score(0, sa_ref)
    def body(j, carry):
        score(2 * j + 1, sb_ref)
        carry = absorb(2 * j, sa_ref, carry, None)
        score(2 * j + 2, sa_ref)
        return absorb(2 * j + 1, sb_ref, carry, None)
    carry = (jnp.full((1, tile), -1e30, F32), jnp.zeros((72, tile), F32))
    carry = lax.fori_loop(0, last, body, carry)
    score(2 * last + 1, sb_ref)
    carry = absorb(2 * last, sa_ref, carry, 0)
    top, total = absorb(2 * last + 1, sb_ref, carry, width)
    norm = total[64:65, :]
    lse_ref[0] = top + jnp.log2(norm)
    result = (total[:64, :] / norm).astype(BF)
    @pl.when(step % 2 == 0)
    def _():
        out_t_ref[0, 0:64, :] = result
    @pl.when(step % 2 == 1)
    def _():
        out_t_ref[0, 64:128, :] = result
        out_ref[...] = out_t_ref[0].T


def attend(queries, keys_values, tile, per_frame, scale):
    one = pl.Buffered(1)
    return pl.pallas_call(
        partial(attend_kernel, tile, tile // 2, per_frame, scale),
        grid=(4,),
        in_specs=[
            pl.BlockSpec((tile, LANES), lambda i: (i // 2, 0)),
            pl.BlockSpec(keys_values.shape, lambda i: (0, 0), pipeline_mode=one),
        ],
        out_specs=[
            pl.BlockSpec((tile, LANES), lambda i: (i // 2, 0)),
            pl.BlockSpec((1, LANES, tile), lambda i: (i // 2, 0, 0)),
            pl.BlockSpec((1, 1, tile), lambda i: (i, 0, 0)),
        ],
        out_shape=[
            jax.ShapeDtypeStruct((2 * tile, LANES), BF),
            jax.ShapeDtypeStruct((2, LANES, tile), BF),
            jax.ShapeDtypeStruct((4, 1, tile), F32),
        ],
        scratch_shapes=[
            pltpu.VMEM((72, keys_values.shape[0]), BF),
            pltpu.VMEM((tile // 2, tile), F32),
            pltpu.VMEM((tile // 2, tile), F32),
        ],
        compiler_params=pltpu.CompilerParams(
            dimension_semantics=("arbitrary",), vmem_limit_bytes=24 * MIB
        ),
        cost_estimate=pl.CostEstimate(
            flops=4_000_000_000, bytes_accessed=8_000_000, transcendentals=0
        ),
        name="attend",
    )(queries, keys_values)


def attend_back_kernel(tile, width, per_frame, scale, q_ref, do_ref, lse_ref, out_t_ref, kv_ref, dq_ref, dkv_ref, kt_ref, acc_ref, dq_t_ref, delta_ref, sa, pa, sb, pb):
    step = pl.program_id(0)
    steps_of = scale * LOG2E
    @pl.when(step == 0)
    def _():
        @pl.loop(0, kv_ref.shape[0] // tile)
        def _(j):
            rows = pl.ds(pl.multiple_of(j * tile, tile), tile)
            kt_ref[:, rows] = kv_ref[rows, :].T[:64, :]
            acc_ref[rows, :] = jnp.zeros((tile, LANES), F32)
    @pl.when(step % 2 == 0)
    def _():
        prod = do_ref[...].astype(F32).T * out_t_ref[0].astype(F32)
        delta_ref[0] = jnp.sum(prod[:64], axis=0, keepdims=True)
        delta_ref[1] = jnp.sum(prod[64:], axis=0, keepdims=True)
    low = low_lanes((tile, LANES))
    first = step % 2 == 0
    packed = q_ref[...].astype(F32)
    packed = jnp.where(first, packed, pltpu.roll(packed, 64, 1))
    query = jnp.where(low, packed, 0.0).astype(BF)
    packed = do_ref[...].astype(F32)
    packed = jnp.where(first, pltpu.roll(packed, 64, 1), packed)
    down = jnp.where(low, 0.0, packed).astype(BF)
    lse = lse_ref[0]
    delta = delta_ref[step % 2]
    def rows_of(part):
        return pl.ds(pl.multiple_of(part * width, width), width)
    def score(part, s, p):
        pieces = kv_ref[rows_of(part), :]
        s[...] = dot(pieces, query, 1, 1)
        p[...] = dot(pieces, down, 1, 1)
    def absorb(part, s, p, dq, start):
        rows = rows_of(part)
        probs = jnp.exp2(s[...] * steps_of - lse)
        if start is not None:
            key = lax.broadcasted_iota(jnp.int32, (width, 1), 0) + start
            ask = lax.broadcasted_iota(jnp.int32, (1, tile), 1)
            probs = jnp.where(key // per_frame <= ask // per_frame, probs, 0.0)
        dscore = (probs * (p[...] - delta)).astype(BF)
        acc_ref[rows, :] += dot(dscore, query, 1, 0) + dot(probs.astype(BF), down, 1, 0)
        return dq + dot(kt_ref[:, rows], dscore, 1, 0)
    last = tile_index(step)
    parts = tile // width
    dq = jnp.zeros((64, tile), F32)
    slots = ((sa, pa), (sb, pb))
    score(0, *slots[0])
    def body(j, dq):
        for i in range(parts):
            score(j * parts + i + 1, *slots[(i + 1) % 2])
            dq = absorb(j * parts + i, *slots[i % 2], dq, None)
        return dq
    dq = lax.fori_loop(0, last, body, dq)
    for i in range(parts):
        if i + 1 < parts:
            score(last * parts + i + 1, *slots[(i + 1) % 2])
        dq = absorb(last * parts + i, *slots[i % 2], dq, i * width)
    dq = dq * scale
    @pl.when(step % 2 == 0)
    def _():
        dq_t_ref[0:64, :] = dq
    @pl.when(step % 2 == 1)
    def _():
        dq_t_ref[64:128, :] = dq
        dq_ref[...] = dq_t_ref[...].T.astype(BF)
    @pl.when(step == 3)
    def _():
        @pl.loop(0, kv_ref.shape[0] // tile)
        def _(j):
            rows = pl.ds(pl.multiple_of(j * tile, tile), tile)
            total = acc_ref[rows, :]
            dkv_ref[rows, :] = jnp.where(low_lanes((tile, LANES)), total * scale, total).astype(BF)


def attend_back(queries, downs, lse, out_t, keys_values, tile, per_frame, scale):
    one = pl.Buffered(1)
    keys = keys_values.shape[0]
    packed = pl.BlockSpec((tile, LANES), lambda i: (i // 2, 0))
    whole = pl.BlockSpec(keys_values.shape, lambda i: (0, 0), pipeline_mode=one)
    return pl.pallas_call(
        partial(attend_back_kernel, tile, tile // 2, per_frame, scale),
        grid=(4,),
        in_specs=[
            packed,
            packed,
            pl.BlockSpec((1, 1, tile), lambda i: (i, 0, 0)),
            pl.BlockSpec((1, LANES, tile), lambda i: (i // 2, 0, 0)),
            whole,
        ],
        out_specs=[packed, pl.BlockSpec(keys_values.shape, lambda i: (0, 0))],
        out_shape=[
            jax.ShapeDtypeStruct((2 * tile, LANES), BF),
            jax.ShapeDtypeStruct(keys_values.shape, BF),
        ],
        scratch_shapes=[
            pltpu.VMEM((64, keys), BF),
            pltpu.VMEM((keys, LANES), F32),
            pltpu.VMEM((LANES, tile), F32),
            pltpu.VMEM((2, 1, tile), F32),
        ]
        + [pltpu.VMEM((tile // 2, tile), F32)] * 4,
        compiler_params=pltpu.CompilerParams(
            dimension_semantics=("arbitrary",), vmem_limit_bytes=36 * MIB
        ),
        cost_estimate=pl.CostEstimate(
            flops=8_000_000_000, bytes_accessed=12_000_000, transcendentals=0
        ),
        name="attend_back",
    )(queries, downs, lse, out_t, keys_values)


def exchange_kernel(axis, moves, sources, results, pair_of, work, finish, *refs):
    in_refs, refs = refs[:sources], refs[sources:]
    out_refs, refs = refs[:results], refs[results:]
    send_sem, recv_sem, own_sem = refs[-3:]
    scratch = refs[:-3]
    dests = scratch if finish is not None else out_refs
    me, count = lax.axis_index(axis), lax.axis_size(axis)
    barrier = pltpu.get_barrier_semaphore()
    for step in range(1, count):
        pl.semaphore_signal(
            barrier,
            inc=1,
            device_id={axis: lax.rem(me + step, count)},
            device_id_type=pl.DeviceIdType.MESH,
        )
    pl.semaphore_wait(barrier, count - 1)
    copies = []
    for step in range(1, count):
        peer = lax.rem(me + step, count)
        for index, (source, dest, take, place) in enumerate(moves):
            copies.append(
                pltpu.make_async_remote_copy(
                    src_ref=take(in_refs[source], peer),
                    dst_ref=place(dests[dest], me, peer),
                    send_sem=send_sem.at[index, step - 1],
                    recv_sem=recv_sem.at[index, step - 1],
                    device_id={axis: peer},
                    device_id_type=pl.DeviceIdType.MESH,
                )
            )
            copies[-1].start()
    for index, (source, dest, take, place) in enumerate(moves):
        copies.append(
            pltpu.make_async_copy(
                take(in_refs[source], me), place(dests[dest], me, me), own_sem.at[index]
            )
        )
        copies[-1].start()
    if work is not None:
        work(in_refs, out_refs, 0, 1)
    for copy in copies:
        copy.wait()
    if pair_of is not None:
        core = lax.rem(me, 2)
        ref = dests[pair_of].at[core]
        copy = pltpu.make_async_remote_copy(
            src_ref=ref,
            dst_ref=ref,
            send_sem=own_sem.at[len(moves)],
            recv_sem=own_sem.at[len(moves) + 1],
            device_id={axis: me + 1 - 2 * core},
            device_id_type=pl.DeviceIdType.MESH,
        )
        copy.start()
        copy.wait()
    if finish is not None:
        finish(dests, in_refs, out_refs)


def exchange(
    name,
    axis,
    number,
    moves,
    arrays,
    shapes,
    pair_of=None,
    work=None,
    finish=None,
    landing=(),
    away=False,
    limit=16,
):
    count = lax.axis_size(axis)
    vmem = pl.BlockSpec(memory_space=pltpu.VMEM)
    out_spec = pl.BlockSpec(memory_space=pltpu.HBM) if away else vmem
    sent = sum(a.size * a.dtype.itemsize for a in arrays)
    return pl.pallas_call(
        partial(
            exchange_kernel, axis, moves, len(arrays), len(shapes), pair_of, work, finish
        ),
        in_specs=[vmem] * len(arrays),
        out_specs=[out_spec] * len(shapes),
        out_shape=[jax.ShapeDtypeStruct(*shape) for shape in shapes],
        scratch_shapes=[pltpu.VMEM(*shape) for shape in landing]
        + [
            pltpu.SemaphoreType.DMA((len(moves), count - 1)),
            pltpu.SemaphoreType.DMA((len(moves), count - 1)),
            pltpu.SemaphoreType.DMA((len(moves) + 2,)),
        ],
        compiler_params=pltpu.CompilerParams(
            collective_id=number, has_side_effects=True, vmem_limit_bytes=limit * MIB
        ),
        cost_estimate=pl.CostEstimate(
            flops=0, bytes_accessed=20_000_000 + 30 * sent, transcendentals=0
        ),
        name=name,
    )(*arrays)


def all_of(ref, peer):
    return ref


def block_of(ref, peer):
    return ref.at[peer]


def at_sender(ref, me, peer):
    return ref.at[me]


def lanes_of(size):
    def view(ref, peer):
        return ref.at[:, pl.ds(pl.multiple_of(peer * size, LANES), size)]

    return view


def lanes_at(size):
    def view(ref, me, peer):
        return ref.at[:, pl.ds(pl.multiple_of(me * size, LANES), size)]

    return view


def add_landed(dests, in_refs, out_refs):
    landed, out = dests[0], out_refs[0]
    rows = out.shape[0]
    step = 32 if rows % 32 == 0 else rows

    @pl.loop(0, rows // step)
    def _(j):
        cut = pl.ds(pl.multiple_of(j * step, step), step)
        total = landed[0, cut, :].astype(F32)
        for other in range(1, landed.shape[0]):
            total += landed[other, cut, :].astype(F32)
        out[cut, :] = total.astype(out.dtype)


def gather(name, axis, number, arrays):
    count = lax.axis_size(axis)
    moves = [(i, i, all_of, at_sender) for i in range(len(arrays))]
    return exchange(
        name, axis, number, moves, arrays, [((count,) + a.shape, a.dtype) for a in arrays]
    )


def back_kernel(
    q_ref, kv_ref, out_ref, landed, summed, send_sem, recv_sem, own_sem, pair_sem
):
    me, count = lax.axis_index("row"), lax.axis_size("row")
    core = lax.rem(me, 2)
    barrier = pltpu.get_barrier_semaphore()
    for step in range(1, count):
        pl.semaphore_signal(
            barrier,
            inc=1,
            device_id={"row": lax.rem(me + step, count)},
            device_id_type=pl.DeviceIdType.MESH,
        )
    pl.semaphore_wait(barrier, count - 1)
    half = pltpu.make_async_remote_copy(
        src_ref=kv_ref.at[1 - core],
        dst_ref=landed,
        send_sem=pair_sem.at[0],
        recv_sem=pair_sem.at[1],
        device_id={"row": me + 1 - 2 * core},
        device_id_type=pl.DeviceIdType.MESH,
    )
    half.start()

    def send(index, source, dest, step):
        peer = lax.rem(me + step, count)
        copy = pltpu.make_async_remote_copy(
            src_ref=source.at[:, :, peer],
            dst_ref=dest,
            send_sem=send_sem.at[index, step - 1],
            recv_sem=recv_sem.at[index, step - 1],
            device_id={"row": peer},
            device_id_type=pl.DeviceIdType.MESH,
        )
        copy.start()
        return copy

    copies = [send(0, q_ref, out_ref.at[me, 0:2], step) for step in range(1, count)]
    copies.append(
        pltpu.make_async_copy(q_ref.at[:, :, me], out_ref.at[me, 0:2], own_sem.at[0])
    )
    copies[-1].start()
    half.wait()
    for part in range(summed.shape[0]):

        @pl.loop(0, summed.shape[1])
        def _(j):
            total = kv_ref[core, part, j].astype(F32) + landed[part, j].astype(F32)
            summed[part, j] = total.astype(BF)

    copies += [send(1, summed, out_ref.at[me, 2:6], step) for step in range(1, count)]
    copies.append(
        pltpu.make_async_copy(summed.at[:, :, me], out_ref.at[me, 2:6], own_sem.at[1])
    )
    copies[-1].start()
    for copy in copies:
        copy.wait()


def exchange_back(number, queries, keys_values, shape):
    count = lax.axis_size("row")
    vmem = pl.BlockSpec(memory_space=pltpu.VMEM)
    return pl.pallas_call(
        back_kernel,
        in_specs=[vmem] * 2,
        out_specs=vmem,
        out_shape=jax.ShapeDtypeStruct(*shape),
        scratch_shapes=[
            pltpu.VMEM(keys_values.shape[1:], BF),
            pltpu.VMEM(keys_values.shape[1:], BF),
            pltpu.SemaphoreType.DMA((2, count - 1)),
            pltpu.SemaphoreType.DMA((2, count - 1)),
            pltpu.SemaphoreType.DMA((2,)),
            pltpu.SemaphoreType.DMA((2,)),
        ],
        compiler_params=pltpu.CompilerParams(
            collective_id=number, has_side_effects=True, vmem_limit_bytes=16 * MIB
        ),
        cost_estimate=pl.CostEstimate(flops=0, bytes_accessed=80_000_000, transcendentals=0),
        name="grad_to_tokens",
    )(queries, keys_values)


def square_gather_kernel(in_ref, out_ref, send_sem, recv_sem, own_sem):
    me = lax.axis_index("frame")
    near = (me + 1 - 2 * lax.rem(me, 2), me + 2 - 4 * (me // 2))
    barrier = pltpu.get_barrier_semaphore()
    for peer in near:
        pl.semaphore_signal(
            barrier, inc=1, device_id={"frame": peer}, device_id_type=pl.DeviceIdType.MESH
        )
    pl.semaphore_wait(barrier, 2)
    half = in_ref.shape[0] // 2
    cuts = (pl.ds(0, half), pl.ds(half, half))

    def copy_of(source, dest, way, index):
        return pltpu.make_async_remote_copy(
            src_ref=source,
            dst_ref=dest,
            send_sem=send_sem.at[way, index],
            recv_sem=recv_sem.at[way, index],
            device_id={"frame": near[way]},
            device_id_type=pl.DeviceIdType.MESH,
        )

    first, second, third = [], [], []
    for way in range(2):
        first.append(copy_of(in_ref.at[cuts[way]], out_ref.at[me, cuts[way]], way, 0))
        first[-1].start()
    for way in range(2):
        rest = cuts[1 - way]
        second.append(copy_of(in_ref.at[rest], out_ref.at[me, rest], way, 1))
        second[-1].start()
    own = pltpu.make_async_copy(in_ref, out_ref.at[me], own_sem)
    own.start()
    for way in range(2):
        first[way].wait_recv()
        block = out_ref.at[near[way], cuts[way]]
        third.append(copy_of(block, block, 1 - way, 2))
        third[-1].start()
    for way in range(2):
        first[way].wait_send()
        second[way].wait()
        third[way].wait()
    own.wait()


def gather_frame(name, number, array):
    if lax.axis_size("frame") != 4:
        return gather(name, "frame", number, [array])[0]
    vmem = pl.BlockSpec(memory_space=pltpu.VMEM)
    return pl.pallas_call(
        square_gather_kernel,
        in_specs=[vmem],
        out_specs=vmem,
        out_shape=jax.ShapeDtypeStruct((4,) + array.shape, array.dtype),
        scratch_shapes=[
            pltpu.SemaphoreType.DMA((2, 3)),
            pltpu.SemaphoreType.DMA((2, 3)),
            pltpu.SemaphoreType.DMA,
        ],
        compiler_params=pltpu.CompilerParams(
            collective_id=number, has_side_effects=True, vmem_limit_bytes=16 * MIB
        ),
        cost_estimate=pl.CostEstimate(flops=0, bytes_accessed=30_000_000, transcendentals=0),
        name=name,
    )(array)


def scatter_sum(name, axis, number, parts, dtype=F32):
    return exchange(
        name,
        axis,
        number,
        [(0, 0, block_of, at_sender)],
        [parts],
        [(parts.shape[1:], dtype)],
        finish=add_landed,
        landing=[(parts.shape, parts.dtype)],
    )[0]


def square_scatter_kernel(sources, results, work, *refs):
    in_refs, refs = refs[:sources], refs[sources:]
    out_refs, refs = refs[:results], refs[results:]
    landed, passing, stage, send_sem, recv_sem = refs
    parts_ref = in_refs[0]
    me = lax.axis_index("frame")
    near = (me + 1 - 2 * lax.rem(me, 2), me + 2 - 4 * (me // 2))
    barrier = pltpu.get_barrier_semaphore()
    for peer in near:
        pl.semaphore_signal(
            barrier, inc=1, device_id={"frame": peer}, device_id_type=pl.DeviceIdType.MESH
        )
    pl.semaphore_wait(barrier, 2)
    rows = parts_ref.shape[1]
    half = rows // 2
    step = 32 if half % 32 == 0 else half

    def copy_of(source, dest, way, index):
        copy = pltpu.make_async_remote_copy(
            src_ref=source,
            dst_ref=dest,
            send_sem=send_sem.at[way, index],
            recv_sem=recv_sem.at[way, index],
            device_id={"frame": near[way]},
            device_id_type=pl.DeviceIdType.MESH,
        )
        copy.start()
        return copy

    cuts = (pl.ds(0, half), pl.ds(half, half))
    first = [
        copy_of(parts_ref.at[3 - me, cuts[way]], passing.at[way], way, 0) for way in range(2)
    ]
    second = [
        copy_of(parts_ref.at[near[way], cuts[way]], landed.at[way, cuts[way]], way, 1)
        for way in range(2)
    ]
    if work is not None:
        work(in_refs, out_refs, 0, 2)
    for way in range(2):
        first[way].wait_recv()

        @pl.loop(0, half // step)
        def _(j):
            cut = pl.ds(pl.multiple_of(j * step, step), step)
            own = pl.ds(pl.multiple_of(way * half + j * step, step), step)
            total = passing[way, cut, :].astype(F32) + parts_ref[near[1 - way], own, :].astype(F32)
            stage[way, cut, :] = total.astype(BF)

    third = [
        copy_of(stage.at[1 - way], landed.at[way, cuts[1 - way]], way, 2) for way in range(2)
    ]
    if work is not None:
        work(in_refs, out_refs, 1, 2)
    for way in range(2):
        first[way].wait_send()
        second[way].wait()
        third[way].wait()
    out = out_refs[0]

    @pl.loop(0, rows // step)
    def _(j):
        cut = pl.ds(pl.multiple_of(j * step, step), step)
        total = parts_ref[me, cut, :].astype(F32)
        total += landed[0, cut, :].astype(F32) + landed[1, cut, :].astype(F32)
        out[cut, :] = total


def scatter_frame(name, number, parts, extras=(), shapes=(), work=None, limit=24):
    arrays = [parts, *extras]
    shapes = [(parts.shape[1:], F32), *shapes]
    if lax.axis_size("frame") != 4:
        return exchange(
            name,
            "frame",
            number,
            [(0, 0, block_of, at_sender)],
            arrays,
            shapes,
            work=work,
            finish=add_landed,
            landing=[(parts.shape, BF)],
            limit=limit + 12,
        )
    vmem = pl.BlockSpec(memory_space=pltpu.VMEM)
    _, rows, width = parts.shape
    return pl.pallas_call(
        partial(square_scatter_kernel, len(arrays), len(shapes), work),
        in_specs=[vmem] * len(arrays),
        out_specs=[vmem] * len(shapes),
        out_shape=[jax.ShapeDtypeStruct(*shape) for shape in shapes],
        scratch_shapes=[
            pltpu.VMEM((2, rows, width), BF),
            pltpu.VMEM((2, rows // 2, width), BF),
            pltpu.VMEM((2, rows // 2, width), BF),
            pltpu.SemaphoreType.DMA((2, 3)),
            pltpu.SemaphoreType.DMA((2, 3)),
        ],
        compiler_params=pltpu.CompilerParams(
            collective_id=number, has_side_effects=True, vmem_limit_bytes=limit * MIB
        ),
        cost_estimate=pl.CostEstimate(flops=0, bytes_accessed=80_000_000, transcendentals=0),
        name=name,
    )(*arrays)


def cut_kernel(slice_width, hidden_slice, in_ref, out_ref, up_ref, down_ref, *refs):
    own_in, own_rest, own_down, sems = refs
    frame = lax.axis_index("frame")
    width = out_ref.shape[1]
    hidden = pl.ds(pl.multiple_of(frame * hidden_slice, LANES), hidden_slice)
    pieces = [
        (out_ref, own_rest.at[:, 0:width]),
        (up_ref.at[:, hidden], own_rest.at[:, width : width + hidden_slice]),
        (down_ref.at[:, hidden], own_down),
    ]
    for part in range(4):
        start = pl.multiple_of(part * width + frame * slice_width, LANES)
        pieces.append(
            (
                in_ref.at[:, pl.ds(start, slice_width)],
                own_in.at[:, part * slice_width : (part + 1) * slice_width],
            )
        )
    copies = [
        pltpu.make_async_copy(source, dest, sems.at[index])
        for index, (source, dest) in enumerate(pieces)
    ]
    for copy in copies:
        copy.start()
    for copy in copies:
        copy.wait()


def cut_weights(attn_in, out_weight, up_weight, down_weight, slice_width, hidden_slice):
    rows, width = out_weight.shape
    vmem = pl.BlockSpec(memory_space=pltpu.VMEM)
    return pl.pallas_call(
        partial(cut_kernel, slice_width, hidden_slice),
        in_specs=[pl.BlockSpec(memory_space=pl.ANY)] * 4,
        out_specs=[vmem] * 3,
        out_shape=[
            jax.ShapeDtypeStruct((rows, 4 * slice_width), BF),
            jax.ShapeDtypeStruct((rows, width + hidden_slice), BF),
            jax.ShapeDtypeStruct((rows, hidden_slice), BF),
        ],
        scratch_shapes=[pltpu.SemaphoreType.DMA((7,))],
        compiler_params=pltpu.CompilerParams(vmem_limit_bytes=8 * MIB),
        name="cut_weights",
    )(attn_in, out_weight, up_weight, down_weight)


def join_kernel(hidden_slice, parts_ref, up_ref, down_ref, out_ref):
    total = None
    for part in range(parts_ref.shape[0]):
        cut = slice(part * hidden_slice, (part + 1) * hidden_slice)
        up_ref[:, cut] = parts_ref[part, :, :hidden_slice].astype(F32)
        down_ref[:, cut] = parts_ref[part, :, hidden_slice : 2 * hidden_slice].astype(F32)
        last = parts_ref[part, :, 2 * hidden_slice :].astype(F32)
        total = last if total is None else total + last
    out_ref[...] = total


def join_in_kernel(width, slice_width, parts_ref, in_ref):
    for part in range(parts_ref.shape[0]):
        for group in range(4):
            start = group * width + part * slice_width
            in_ref[:, start : start + slice_width] = parts_ref[
                part, :, group * slice_width : (group + 1) * slice_width
            ].astype(F32)


def join(name, body, parts, widths):
    count, rows, columns = parts.shape
    step = rows // 4
    return pl.pallas_call(
        body,
        grid=(4,),
        in_specs=[pl.BlockSpec((count, step, columns), lambda i: (0, i, 0))],
        out_specs=[pl.BlockSpec((step, w), lambda i: (i, 0)) for w in widths],
        out_shape=[jax.ShapeDtypeStruct((rows, w), F32) for w in widths],
        compiler_params=pltpu.CompilerParams(
            dimension_semantics=("arbitrary",), vmem_limit_bytes=16 * MIB
        ),
        cost_estimate=pl.CostEstimate(flops=0, bytes_accessed=8_000_000, transcendentals=0),
        name=name,
    )(parts)


def grads_beside(cut):
    def work(in_refs, out_refs, share, shares):
        hid_ref, pre_ref, cot_ref, act_ref, down_ref = in_refs[1:]
        grads_ref, branch_ref = out_refs[1:]
        columns = pre_ref.shape[1]
        block = max(cut, LANES)
        count = hid_ref.shape[1] // block
        rows = branch_ref.shape[0] // count

        @pl.loop(count * share // shares, count * (share + 1) // shares)
        def _(i):
            lanes = pl.ds(pl.multiple_of(i * block, LANES), block)
            for part, (left, right) in enumerate(((hid_ref, pre_ref), (cot_ref, act_ref))):
                result = dot(left[:, lanes], right[...], 0, 0).astype(BF)
                for piece in range(block // cut):
                    grads_ref[
                        i * (block // cut) + piece, :, part * columns : (part + 1) * columns
                    ] = result[piece * cut : (piece + 1) * cut]
            own = pl.ds(pl.multiple_of(i * rows, rows), rows)
            branch_ref[own, :] = dot(act_ref[own, :], down_ref[...], 1, 1).astype(BF)

    return work


def out_grad_kernel(cut, gated_ref, grad_ref, before_ref, out_ref):
    result = dot(gated_ref[...], grad_ref[...], 0, 0).astype(BF)
    for piece in range(out_ref.shape[0]):
        out_ref[piece] = result[piece * cut : (piece + 1) * cut]


def add_out_grad(gated, grad, grads):
    row_devs, cut, columns = grads.shape
    tokens, width = gated.shape
    block = width // 2
    last = (columns - width) // width
    assert columns % width == 0
    return pl.pallas_call(
        partial(out_grad_kernel, cut),
        grid=(width // block,),
        in_specs=[
            pl.BlockSpec((tokens, block), lambda i: (0, i)),
            pl.BlockSpec(grad.shape, lambda i: (0, 0), pipeline_mode=pl.Buffered(1)),
            pl.BlockSpec(memory_space=pl.ANY),
        ],
        out_specs=pl.BlockSpec((block // cut, cut, width), lambda i: (i, 0, last)),
        out_shape=jax.ShapeDtypeStruct(grads.shape, BF),
        input_output_aliases={2: 0},
        compiler_params=pltpu.CompilerParams(
            dimension_semantics=("arbitrary",), vmem_limit_bytes=16 * MIB
        ),
        cost_estimate=pl.CostEstimate(
            flops=600_000_000, bytes_accessed=5_000_000, transcendentals=0
        ),
        name="out_grad",
    )(gated, grad, grads)


def on_device(
    tokens,
    timesteps,
    noise_table,
    mod_weight,
    mod_bias,
    attn_in,
    out_weight,
    up_weight,
    down_weight,
    cotangent,
):
    clips, frames, rows_dev, grid_side, width = tokens.shape
    frame_index = lax.axis_index("frame")
    row_index = lax.axis_index("row")
    frame_devs, row_devs = lax.axis_size("frame"), lax.axis_size("row")
    core = row_index % 2
    clip_len = frames * frame_devs
    head_dim = width // HEADS
    heads = HEADS // frame_devs
    slice_width = width // frame_devs
    per_frame_dev = rows_dev * grid_side
    per_frame = grid_side * grid_side
    token_count = clips * frames * per_frame_dev
    group_count = token_count * frame_devs
    tile = clip_len // 8 * per_frame
    scale = head_dim ** (-0.5)
    step_count = noise_table.shape[0]
    assert head_dim == 64 and row_devs == 2 * clips * heads

    def by_frames(values):
        parts = values.reshape(frame_devs, clips, frames * per_frame_dev, -1)
        return jnp.transpose(parts, (1, 0, 2, 3)).reshape(group_count, values.shape[-1])

    def to_frames(values):
        parts = values.reshape(clips, frame_devs, frames * per_frame_dev, -1)
        return jnp.transpose(parts, (1, 0, 2, 3)).reshape(frame_devs, token_count, -1)

    def gather_frames(values):
        full = lax.all_gather(values, "frame", axis=1, tiled=True)
        return full.reshape(group_count, values.shape[-1])

    def scatter_frames(values):
        parts = to_frames(values).reshape(group_count, width)
        return lax.psum_scatter(parts, "frame", scatter_dimension=0, tiled=True).reshape(
            tokens.shape
        )

    hidden_slice = up_weight.shape[1] // frame_devs
    own_in, own_rest, own_down = cut_weights(
        attn_in, out_weight, up_weight, down_weight, slice_width, hidden_slice
    )
    weight_in = lax.all_gather(own_in, "row", axis=0, tiled=True)

    steps_iota = lax.broadcasted_iota(jnp.int32, (1, 1, step_count), 2)
    one_hot = (timesteps[:, :, None] == steps_iota).astype(BF)
    embedding = jnp.einsum("cls,sd->cld", one_hot, noise_table, preferred_element_type=F32)
    silu_low = jax.nn.silu(embedding).astype(BF)
    mod_local = jnp.einsum(
        "cld,de->cle", silu_low, mod_weight, preferred_element_type=F32
    ) + mod_bias.astype(F32)
    mod_width = mod_local.shape[2]
    modulation = exchange(
        "gather_mod",
        "row",
        0,
        [(0, 0, all_of, lanes_at(mod_width))],
        [mod_local.astype(BF).reshape(clips * frames, mod_width)],
        [((clips * frames, mod_width * row_devs), BF)],
    )[0].astype(F32)
    modulation = modulation.reshape(clips, frames, 6, 1, 1, width)
    shift_one, scale_one, gate_one, shift_two, scale_two, gate_two = [
        modulation[:, :, part] for part in range(6)
    ]

    frame_freq, row_freq, col_freq = [np.tile(t, 4) for t in rotary_freqs(head_dim // 2)]
    shape_three = (clip_len, rows_dev, grid_side, LANES)
    frame_pos = lax.broadcasted_iota(F32, shape_three, 0)
    row_pos = (row_index * rows_dev + lax.broadcasted_iota(jnp.int32, shape_three, 1)).astype(F32)
    col_pos = lax.broadcasted_iota(F32, shape_three, 2)
    angles = (frame_pos * frame_freq + row_pos * row_freq + col_pos * col_freq).reshape(-1, LANES)
    sign = np.where(np.arange(LANES) % 64 < 32, -1.0, 1.0).astype(np.float32)
    cosines = jnp.cos(angles)
    sines = jnp.sin(angles) * sign

    token_f = tokens.astype(F32)
    hidden_one, norm_one_pull = jax.vjp(modulate, token_f, shift_one, scale_one)
    hidden_group = by_frames(
        gather_frame("gather_one", 1, hidden_one.astype(BF).reshape(token_count, width))
    )

    grad_out = cotangent.astype(F32)
    grad_branch_two = (grad_out * gate_two).astype(BF)
    hidden_group, grad_branch_two = lax.optimization_barrier((hidden_group, grad_branch_two))
    grad_two_group = gather_frames(grad_branch_two)

    pack, gate_raw = qkv_project(hidden_group, weight_in, cosines, sines, clips, heads)

    half = tile // row_devs

    spans = half // per_frame_dev
    by_token = (spans, per_frame_dev, LANES)
    by_head = (spans, row_devs, per_frame_dev, LANES)

    def peer_rows(ref, peer):
        return ref.at[:, :, peer]

    queries, keys_values = exchange(
        "to_heads",
        "row",
        2,
        [
            (0, 0, lambda r, p: r.at[p, 0:2], lambda r, me, p: r.at[:, :, me]),
            (0, 1, lambda r, p: r.at[p, 2:6], lambda r, me, p: r.at[p % 2, :, :, me]),
        ],
        [pack.reshape((row_devs, 6) + by_token)],
        [((2,) + by_head, BF), ((2, 4) + by_head, BF)],
        pair_of=1,
        away=True,
    )
    queries = queries.reshape(-1, LANES)
    keys_values = keys_values.reshape(-1, LANES)

    queries, keys_values, grad_two_group, own_rest, own_down = lax.optimization_barrier(
        (queries, keys_values, grad_two_group, own_rest, own_down)
    )
    rest = lax.all_gather(own_rest, "row", axis=0, tiled=True)
    attended_heads, attended_t, lse = attend(queries, keys_values, tile, per_frame, scale)
    gated_group, attended = exchange(
        "to_tokens",
        "row",
        3,
        [(0, 0, peer_rows, at_sender)],
        [attended_heads.reshape((2,) + by_head), gate_raw],
        [(gate_raw.shape, BF)] * 2,
        finish=gate_landed(clips, heads),
        landing=[((row_devs, 2) + by_token, BF)],
    )

    gated_group, rest, own_down = lax.optimization_barrier((gated_group, rest, own_down))
    full_out, weight_up = rest[:, :width], rest[:, width:]
    weight_down = lax.all_gather(own_down, "row", axis=0, tiled=True)
    steps_wide = jnp.broadcast_to(timesteps.reshape(-1, 1), (clips * frames, LANES))
    gated, steps_parts = exchange(
        "gated_back",
        "frame",
        4,
        [(0, 0, block_of, lanes_at(slice_width)), (1, 1, all_of, at_sender)],
        [to_frames(gated_group), steps_wide],
        [((token_count, width), BF), ((frame_devs,) + steps_wide.shape, jnp.int32)],
    )
    branch_one = jnp.dot(gated, full_out, preferred_element_type=F32).reshape(tokens.shape)
    after_one = token_f + gate_one * branch_one
    hidden_two, norm_two_pull = jax.vjp(modulate, after_one, shift_two, scale_two)
    hidden_two_group = by_frames(
        gather_frame("gather_two", 5, hidden_two.astype(BF).reshape(token_count, width))
    )

    pre_act = jnp.dot(hidden_two_group, weight_up, preferred_element_type=F32)
    act_values, gelu_pull = jax.vjp(partial(jax.nn.gelu, approximate=True), pre_act)
    act_low = act_values.astype(BF)
    grad_act = jnp.dot(grad_two_group, weight_down, preferred_element_type=F32)
    (grad_pre,) = gelu_pull(grad_act)
    grad_pre = grad_pre.astype(BF)
    parts = to_frames(dot(grad_pre, weight_up, 1, 1).astype(BF))
    cut = width // row_devs
    grad_hidden_two, weight_grads, branch_two = scatter_frame(
        "scatter_two",
        6,
        parts,
        [hidden_two_group, grad_pre, grad_two_group, act_low, weight_down],
        [
            ((row_devs, cut, 2 * hidden_slice + width), BF),
            ((group_count, width), BF),
        ],
        grads_beside(cut),
        limit=30,
    )
    grad_hidden_two = grad_hidden_two.reshape(tokens.shape)
    branch_two = scatter_frames(branch_two)
    grad_after_part, grad_shift_two, grad_scale_two = norm_two_pull(grad_hidden_two)
    grad_after = grad_out + grad_after_part
    grad_gate_one = jnp.sum(grad_after * branch_one, axis=(2, 3), keepdims=True)
    grad_branch_one = (grad_after * gate_one).astype(BF).reshape(token_count, width)
    grad_gated = dot(grad_branch_one, full_out, 1, 1).astype(BF)
    weight_grads = add_out_grad(gated, grad_branch_one, weight_grads)
    grad_gated, weight_grads = lax.optimization_barrier((grad_gated, weight_grads))
    weight_grads = lax.psum_scatter(weight_grads, "row", scatter_dimension=0, tiled=True)
    (grad_gated,) = exchange(
        "grad_gated",
        "frame",
        7,
        [(0, 0, lanes_of(slice_width), at_sender)],
        [grad_gated],
        [((frame_devs, token_count, slice_width), BF)],
    )
    grad_gated = by_frames(grad_gated)
    down_pack, grad_gate = gate_back(grad_gated, gate_raw, attended, clips, heads)
    (downs,) = exchange(
        "grad_to_heads",
        "row",
        8,
        [(0, 0, block_of, lambda r, me, p: r.at[:, :, me])],
        [down_pack.reshape((row_devs, 2) + by_token)],
        [((2,) + by_head, BF)],
        away=True,
    )
    downs = downs.reshape(-1, LANES)
    downs, branch_two = lax.optimization_barrier((downs, branch_two))
    branch_two = branch_two.astype(F32)
    mixed = (after_one + gate_two * branch_two).astype(BF)
    grad_gate_two = jnp.sum(grad_out * branch_two, axis=(2, 3), keepdims=True)

    grad_queries, grad_kv = attend_back(
        queries, downs, lse, attended_t, keys_values, tile, per_frame, scale
    )
    grad_kv, weight_grads = lax.optimization_barrier((grad_kv, weight_grads))
    grads_all = lax.all_gather(weight_grads[0], "frame", axis=0, tiled=False)
    back_pack = exchange_back(
        9,
        grad_queries.reshape((2,) + by_head),
        grad_kv.reshape((2, 4) + by_head),
        ((row_devs, 6) + by_token, BF),
    )
    back_pack = back_pack.reshape(clips, heads, 2, 6, half, LANES)
    grad_mixed, grad_hidden = qkv_back(
        back_pack, grad_gate, weight_in, cosines, sines, clips, heads
    )
    grad_mixed, grads_all = lax.optimization_barrier((grad_mixed, grads_all))
    (grad_hidden_one,) = scatter_frame("scatter_one", 10, to_frames(grad_hidden), limit=16)
    grad_hidden_one = grad_hidden_one.reshape(tokens.shape)
    in_grad = lax.psum_scatter(
        dot(hidden_group, grad_mixed, 0, 0).astype(BF), "row", scatter_dimension=0, tiled=True
    )

    grad_token_part, grad_shift_one, grad_scale_one = norm_one_pull(grad_hidden_one)
    tokens_grad = (grad_after + grad_token_part).astype(BF)

    grad_mod = jnp.stack(
        [
            grad_shift_one,
            grad_scale_one,
            grad_gate_one,
            grad_shift_two,
            grad_scale_two,
            grad_gate_two,
        ],
        axis=2,
    ).reshape(clips * frames, 6 * width)
    grad_mod = jnp.transpose(
        grad_mod.reshape(clips * frames, row_devs, mod_width), (1, 0, 2)
    )
    grad_mod = scatter_sum("scatter_mod", "row", 11, grad_mod, BF)
    grad_mod, in_grad = lax.optimization_barrier((grad_mod, in_grad))
    (grad_mod_all,) = gather("gather_grad_mod", "frame", 12, [grad_mod])
    grad_mod_all = grad_mod_all.reshape(-1, mod_width)
    steps_all = steps_parts.reshape(-1, LANES)[:, 0]
    hot_all = steps_all[:, None] == lax.broadcasted_iota(jnp.int32, (1, step_count), 1)
    embed_all = jnp.dot(hot_all.astype(BF), noise_table, preferred_element_type=F32)
    silu_all, silu_pull = jax.vjp(jax.nn.silu, embed_all)
    mod_weight_grad = dot(silu_all.astype(BF), grad_mod_all, 0, 0)
    mod_bias_grad = jnp.sum(grad_mod_all.astype(F32), axis=0)
    grad_silu = dot(grad_mod_all, mod_weight, 1, 1)
    frame_count, cut = grad_silu.shape[0], width // row_devs
    grad_silu = jnp.transpose(grad_silu.reshape(frame_count, row_devs, cut), (1, 0, 2))
    grad_silu = scatter_sum("scatter_silu", "row", 13, grad_silu)
    (grad_silu,) = gather("gather_silu", "row", 14, [grad_silu])
    grad_silu = jnp.transpose(grad_silu, (1, 0, 2)).reshape(frame_count, width)
    (grad_embedding,) = silu_pull(grad_silu)
    noise_table_grad = lax.dot_general(
        hot_all.astype(F32),
        grad_embedding,
        (((0,), (0,)), ((), ())),
        precision=lax.Precision.HIGHEST,
    )

    up_weight_grad, down_weight_grad, out_weight_grad = join(
        "join_grads",
        partial(join_kernel, hidden_slice),
        grads_all,
        (up_weight.shape[1], down_weight.shape[1], width),
    )
    in_all = lax.all_gather(in_grad, "frame", axis=0, tiled=False)
    (attn_in_grad,) = join(
        "join_in", partial(join_in_kernel, width, slice_width), in_all, (attn_in.shape[1],)
    )
    return (
        mixed,
        tokens_grad,
        noise_table_grad,
        mod_weight_grad,
        mod_bias_grad,
        attn_in_grad,
        out_weight_grad,
        up_weight_grad,
        down_weight_grad,
    )


def solution(mesh):
    in_specs = (
        P(None, "frame", "row", None, None),
        P(None, "frame"),
        P(),
        P(None, "row"),
        P("row"),
        P("row", None),
        P("row", None),
        P("row", None),
        P("row", None),
        P(None, "frame", "row", None, None),
    )
    out_specs = (
        P(None, "frame", "row", None, None),
        P(None, "frame", "row", None, None),
        P(),
        P(None, "row"),
        P("row"),
        P("row", None),
        P("row", None),
        P("row", None),
        P("row", None),
    )
    return jax.shard_map(
        on_device, mesh=mesh, in_specs=in_specs, out_specs=out_specs, check_vma=False
    )
```

```python
from functools import partial

import jax
import jax.numpy as jnp
import numpy as np
from jax import lax
from jax.experimental import pallas as pl
from jax.experimental.pallas import tpu as pltpu
from jax.sharding import PartitionSpec as P

HEADS = 16
EPS = 1e-06
LOG2E = 1.4426950408889634
F32 = jnp.float32
BF = jnp.bfloat16
LANES = 128
MIB = 1 << 20


def rotary_freqs(pair_count):
    third_count = pair_count // 3
    group_sizes = [pair_count - 2 * third_count, third_count, third_count]
    tables = []
    offset = 0
    for group_index in range(3):
        freq_table = np.zeros((pair_count,), np.float32)
        for inner_index in range(group_sizes[group_index]):
            freq_table[offset + inner_index] = 10000.0 ** (-inner_index / group_sizes[group_index])
        offset += group_sizes[group_index]
        tables.append(freq_table)
    return tables


def layer_norm(values):
    row_mean = jnp.mean(values, axis=-1, keepdims=True)
    centered = values - row_mean
    row_var = jnp.mean(centered * centered, axis=-1, keepdims=True)
    return centered * lax.rsqrt(row_var + EPS)


def modulate(values, shift, scale_part):
    return layer_norm(values) * (1.0 + scale_part) + shift


def dot(left, right, left_dim, right_dim):
    return lax.dot_general(
        left, right, (((left_dim,), (right_dim,)), ((), ())), preferred_element_type=F32
    )


def swap_halves(values):
    lane = lax.broadcasted_iota(jnp.int32, values.shape, 1)
    width = values.shape[1]
    return jnp.where(
        (lane % 64) < 32, pltpu.roll(values, width - 32, 1), pltpu.roll(values, 32, 1)
    )


def low_lanes(shape):
    return lax.broadcasted_iota(jnp.int32, shape, len(shape) - 1) < 64


def qkv_kernel(heads, hid_ref, w_ref, cos_ref, sin_ref, pack_ref, gate_ref):
    clip, quarter = pl.program_id(0), pl.program_id(1)
    width = heads * 64
    mixed = jnp.dot(hid_ref[...], w_ref[...], preferred_element_type=F32)
    cos, sin = cos_ref[...], sin_ref[...]
    rows = mixed.shape[0]
    half = rows // 2
    gate_ref[...] = mixed[:, 3 * width :]
    low = low_lanes((rows, LANES))
    low_half = low_lanes((half, LANES))
    query_set = jnp.where((quarter == 0) | (quarter == 3), 0, 1)
    slot = quarter // 2
    for pair in range(heads // 2):
        cut = slice(pair * LANES, (pair + 1) * LANES)
        query = mixed[:, cut]
        key = mixed[:, width + pair * LANES : width + (pair + 1) * LANES]
        value = mixed[:, 2 * width + pair * LANES : 2 * width + (pair + 1) * LANES]
        query = query * cos + swap_halves(query) * sin
        key = key * cos + swap_halves(key) * sin
        key_turn = pltpu.roll(key, 64, 1)
        value_turn = pltpu.roll(value, 64, 1)
        query_turn = pltpu.roll(query, 64, 1)
        packs = (
            (
                jnp.where(low, key, value_turn),
                jnp.where(low_half, query[:half], query_turn[half:]),
            ),
            (
                jnp.where(low, key_turn, value),
                jnp.where(low_half, query_turn[:half], query[half:]),
            ),
        )
        for inner, (key_value, queries) in enumerate(packs):
            head = 2 * pair + inner
            pack_ref[clip, head, query_set, slot] = queries.astype(BF)
            key_value = key_value.astype(BF)
            first = 2 + 2 * (quarter % 2)
            pack_ref[clip, head, quarter // 2, first] = key_value[:half]
            pack_ref[clip, head, quarter // 2, first + 1] = key_value[half:]


def qkv_project(hidden, weight, cos, sin, clips, heads):
    tokens, width = hidden.shape
    quarter = tokens // clips // 4
    one = pl.Buffered(1)
    return pl.pallas_call(
        partial(qkv_kernel, heads),
        grid=(clips, 4),
        in_specs=[
            pl.BlockSpec((quarter, width), lambda c, i: (c * 4 + i, 0)),
            pl.BlockSpec(weight.shape, lambda c, i: (0, 0), pipeline_mode=one),
            pl.BlockSpec((quarter, LANES), lambda c, i: (i, 0)),
            pl.BlockSpec((quarter, LANES), lambda c, i: (i, 0)),
        ],
        out_specs=[
            pl.BlockSpec(
                (clips, heads, 2, 6, quarter // 2, LANES), lambda c, i: (0, 0, 0, 0, 0, 0)
            ),
            pl.BlockSpec((quarter, heads * 64), lambda c, i: (c * 4 + i, 0)),
        ],
        out_shape=[
            jax.ShapeDtypeStruct((clips, heads, 2, 6, quarter // 2, LANES), BF),
            jax.ShapeDtypeStruct((tokens, heads * 64), F32),
        ],
        compiler_params=pltpu.CompilerParams(
            dimension_semantics=("arbitrary", "arbitrary"), vmem_limit_bytes=20 * MIB
        ),
        name="qkv_project",
    )(hidden, weight, cos, sin)


def qkv_back_kernel(heads, pack_ref, dgate_ref, w_ref, cos_ref, sin_ref, mixed_ref, hid_ref):
    clip, quarter = pl.program_id(0), pl.program_id(1)
    width = heads * 64
    cos, sin = cos_ref[...], sin_ref[...]
    rows = cos.shape[0]
    half = rows // 2
    low_half = low_lanes((half, LANES))
    query_set = jnp.where((quarter == 0) | (quarter == 3), 0, 1)
    slot = quarter // 2
    first = 2 + 2 * (quarter % 2)
    low = low_lanes((rows, LANES))
    for pair in range(heads // 2):
        even, odd = 2 * pair, 2 * pair + 1
        query_even = pack_ref[clip, even, query_set, slot].astype(F32)
        query_odd = pack_ref[clip, odd, query_set, slot].astype(F32)
        query = jnp.concatenate(
            [
                jnp.where(low_half, query_even, pltpu.roll(query_odd, 64, 1)),
                jnp.where(low_half, pltpu.roll(query_even, 64, 1), query_odd),
            ],
            axis=0,
        )
        both = []
        for head in (even, odd):
            both.append(
                jnp.concatenate(
                    [
                        pack_ref[clip, head, quarter // 2, first].astype(F32),
                        pack_ref[clip, head, quarter // 2, first + 1].astype(F32),
                    ],
                    axis=0,
                )
            )
        key = jnp.where(low, both[0], pltpu.roll(both[1], 64, 1))
        value = jnp.where(low, pltpu.roll(both[0], 64, 1), both[1])
        query = query * cos - swap_halves(query) * sin
        key = key * cos - swap_halves(key) * sin
        for part, values in enumerate((query, key, value)):
            start = part * width + pair * LANES
            mixed_ref[:, start : start + LANES] = values.astype(BF)
    mixed_ref[:, 3 * width :] = dgate_ref[...]
    hid_ref[...] = dot(mixed_ref[...], w_ref[...], 1, 1).astype(BF)


def qkv_back(pack, dgate, weight, cos, sin, clips, heads):
    tokens = dgate.shape[0]
    width = weight.shape[0]
    quarter = tokens // clips // 4
    one = pl.Buffered(1)
    return pl.pallas_call(
        partial(qkv_back_kernel, heads),
        grid=(clips, 4),
        in_specs=[
            pl.BlockSpec(pack.shape, lambda c, i: (0, 0, 0, 0, 0, 0), pipeline_mode=one),
            pl.BlockSpec((quarter, heads * 64), lambda c, i: (c * 4 + i, 0)),
            pl.BlockSpec(weight.shape, lambda c, i: (0, 0), pipeline_mode=one),
            pl.BlockSpec((quarter, LANES), lambda c, i: (i, 0)),
            pl.BlockSpec((quarter, LANES), lambda c, i: (i, 0)),
        ],
        out_specs=[
            pl.BlockSpec((quarter, 4 * heads * 64), lambda c, i: (c * 4 + i, 0)),
            pl.BlockSpec((quarter, width), lambda c, i: (c * 4 + i, 0)),
        ],
        out_shape=[
            jax.ShapeDtypeStruct((tokens, 4 * heads * 64), BF),
            jax.ShapeDtypeStruct((tokens, width), BF),
        ],
        compiler_params=pltpu.CompilerParams(
            dimension_semantics=("arbitrary", "arbitrary"), vmem_limit_bytes=20 * MIB
        ),
        name="qkv_back",
    )(pack, dgate, weight, cos, sin)


def unpack_pair(even, odd):
    low = low_lanes(even.shape)
    return jnp.concatenate(
        [
            jnp.where(low, even, pltpu.roll(odd, 64, 1)),
            jnp.where(low, pltpu.roll(even, 64, 1), odd),
        ],
        axis=0,
    )


def gate_landed(clips, heads):
    def finish(dests, in_refs, out_refs):
        pack_ref, gate_ref, (gated_ref, attended_ref) = dests[0], in_refs[1], out_refs
        quarter = gate_ref.shape[0] // clips // 4
        for clip in range(clips):
            for index in range(4):
                query_set, slot = (0, 1, 1, 0)[index], index // 2
                rows = pl.ds((clip * 4 + index) * quarter, quarter)
                for pair in range(heads // 2):
                    cut = slice(pair * LANES, (pair + 1) * LANES)
                    even, odd = [
                        pack_ref[(clip * heads + head) * 2 + query_set, slot]
                        .reshape(quarter // 2, LANES)
                        .astype(F32)
                        for head in (2 * pair, 2 * pair + 1)
                    ]
                    attended = unpack_pair(even, odd)
                    attended_ref[rows, cut] = attended.astype(BF)
                    gate = jax.nn.sigmoid(gate_ref[rows, cut])
                    gated_ref[rows, cut] = (attended * gate).astype(BF)

    return finish


def gate_back_kernel(heads, grad_ref, gate_ref, attended_ref, pack_ref, dgate_ref):
    clip, quarter = pl.program_id(0), pl.program_id(1)
    query_set = jnp.where((quarter == 0) | (quarter == 3), 0, 1)
    slot = quarter // 2
    rows = grad_ref.shape[0]
    half = rows // 2
    low = low_lanes((half, LANES))
    for pair in range(heads // 2):
        cut = slice(pair * LANES, (pair + 1) * LANES)
        sig = jax.nn.sigmoid(gate_ref[:, cut])
        grad = grad_ref[:, cut].astype(F32)
        dgate = grad * attended_ref[:, cut].astype(F32) * sig * (1.0 - sig)
        dgate_ref[:, cut] = dgate.astype(BF)
        down = grad * sig
        turn = pltpu.roll(down, 64, 1)
        pack_ref[clip, 2 * pair, query_set, slot] = jnp.where(low, down[:half], turn[half:]).astype(
            BF
        )
        pack_ref[clip, 2 * pair + 1, query_set, slot] = jnp.where(
            low, turn[:half], down[half:]
        ).astype(BF)


def gate_back(grad, gate, attended, clips, heads):
    tokens = gate.shape[0]
    quarter = tokens // clips // 4
    block = pl.BlockSpec((quarter, heads * 64), lambda c, i: (c * 4 + i, 0))
    pack_shape = (clips, heads, 2, 2, quarter // 2, LANES)
    return pl.pallas_call(
        partial(gate_back_kernel, heads),
        grid=(clips, 4),
        in_specs=[block, block, block],
        out_specs=[pl.BlockSpec(pack_shape, lambda c, i: (0, 0, 0, 0, 0, 0)), block],
        out_shape=[
            jax.ShapeDtypeStruct(pack_shape, BF),
            jax.ShapeDtypeStruct((tokens, heads * 64), BF),
        ],
        compiler_params=pltpu.CompilerParams(
            dimension_semantics=("arbitrary", "arbitrary"), vmem_limit_bytes=12 * MIB
        ),
        name="gate_back",
    )(grad, gate, attended)


def tile_index(step):
    core = lax.axis_index("row") % 2
    slot = step // 2
    quarter = jnp.where(core == 0, 3 * slot, 1 + slot)
    return 2 * quarter + step % 2


def attend_kernel(tile, width, per_frame, scale, q_ref, kv_ref, out_ref, out_t_ref, lse_ref, vt_ref, sa_ref, sb_ref):
    step = pl.program_id(0)
    steps_of = scale * LOG2E
    @pl.when(step == 0)
    def _():
        vt_ref[64:72, :] = jnp.ones((8, vt_ref.shape[1]), BF)
        @pl.loop(0, kv_ref.shape[0] // tile)
        def _(j):
            rows = pl.ds(pl.multiple_of(j * tile, tile), tile)
            vt_ref[0:64, rows] = kv_ref[rows, :].T[64:, :]
    low = low_lanes((tile, LANES))
    packed = q_ref[...].astype(F32)
    packed = jnp.where(step % 2 == 0, packed, pltpu.roll(packed, 64, 1))
    query = jnp.where(low, packed, 0.0).astype(BF)
    def rows_of(part):
        return pl.ds(pl.multiple_of(part * width, width), width)
    def score(part, ref):
        ref[...] = dot(kv_ref[rows_of(part), :], query, 1, 1)
    def absorb(part, ref, carry, start):
        top, total = carry
        scores = ref[...] * steps_of
        if start is not None:
            key = (lax.broadcasted_iota(jnp.int32, (width, 1), 0) + start) // per_frame
            ask = lax.broadcasted_iota(jnp.int32, (1, tile), 1) // per_frame
            scores = jnp.where(key <= ask, scores, -1e30)
        new_top = jnp.maximum(top, jnp.max(scores, axis=0, keepdims=True))
        probs = jnp.exp2(scores - new_top).astype(BF)
        total = total * jnp.exp2(top - new_top) + dot(vt_ref[:, rows_of(part)], probs, 1, 0)
        return new_top, total
    last = tile_index(step)
    score(0, sa_ref)
    def body(j, carry):
        score(2 * j + 1, sb_ref)
        carry = absorb(2 * j, sa_ref, carry, None)
        score(2 * j + 2, sa_ref)
        return absorb(2 * j + 1, sb_ref, carry, None)
    carry = (jnp.full((1, tile), -1e30, F32), jnp.zeros((72, tile), F32))
    carry = lax.fori_loop(0, last, body, carry)
    score(2 * last + 1, sb_ref)
    carry = absorb(2 * last, sa_ref, carry, 0)
    top, total = absorb(2 * last + 1, sb_ref, carry, width)
    norm = total[64:65, :]
    lse_ref[0] = top + jnp.log2(norm)
    result = (total[:64, :] / norm).astype(BF)
    @pl.when(step % 2 == 0)
    def _():
        out_t_ref[0, 0:64, :] = result
    @pl.when(step % 2 == 1)
    def _():
        out_t_ref[0, 64:128, :] = result
        out_ref[...] = out_t_ref[0].T


def attend(queries, keys_values, tile, per_frame, scale):
    one = pl.Buffered(1)
    return pl.pallas_call(
        partial(attend_kernel, tile, tile // 2, per_frame, scale),
        grid=(4,),
        in_specs=[
            pl.BlockSpec((tile, LANES), lambda i: (i // 2, 0)),
            pl.BlockSpec(keys_values.shape, lambda i: (0, 0), pipeline_mode=one),
        ],
        out_specs=[
            pl.BlockSpec((tile, LANES), lambda i: (i // 2, 0)),
            pl.BlockSpec((1, LANES, tile), lambda i: (i // 2, 0, 0)),
            pl.BlockSpec((1, 1, tile), lambda i: (i, 0, 0)),
        ],
        out_shape=[
            jax.ShapeDtypeStruct((2 * tile, LANES), BF),
            jax.ShapeDtypeStruct((2, LANES, tile), BF),
            jax.ShapeDtypeStruct((4, 1, tile), F32),
        ],
        scratch_shapes=[
            pltpu.VMEM((72, keys_values.shape[0]), BF),
            pltpu.VMEM((tile // 2, tile), F32),
            pltpu.VMEM((tile // 2, tile), F32),
        ],
        compiler_params=pltpu.CompilerParams(
            dimension_semantics=("arbitrary",), vmem_limit_bytes=24 * MIB
        ),
        cost_estimate=pl.CostEstimate(
            flops=4_000_000_000, bytes_accessed=8_000_000, transcendentals=0
        ),
        name="attend",
    )(queries, keys_values)


def attend_back_kernel(tile, width, per_frame, scale, q_ref, do_ref, lse_ref, out_t_ref, kv_ref, dq_ref, dkv_ref, kt_ref, acc_ref, dq_t_ref, delta_ref, sa, pa, sb, pb):
    step = pl.program_id(0)
    steps_of = scale * LOG2E
    @pl.when(step == 0)
    def _():
        @pl.loop(0, kv_ref.shape[0] // tile)
        def _(j):
            rows = pl.ds(pl.multiple_of(j * tile, tile), tile)
            kt_ref[:, rows] = kv_ref[rows, :].T[:64, :]
            acc_ref[rows, :] = jnp.zeros((tile, LANES), F32)
    @pl.when(step % 2 == 0)
    def _():
        prod = do_ref[...].astype(F32).T * out_t_ref[0].astype(F32)
        delta_ref[0] = jnp.sum(prod[:64], axis=0, keepdims=True)
        delta_ref[1] = jnp.sum(prod[64:], axis=0, keepdims=True)
    low = low_lanes((tile, LANES))
    first = step % 2 == 0
    packed = q_ref[...].astype(F32)
    packed = jnp.where(first, packed, pltpu.roll(packed, 64, 1))
    query = jnp.where(low, packed, 0.0).astype(BF)
    packed = do_ref[...].astype(F32)
    packed = jnp.where(first, pltpu.roll(packed, 64, 1), packed)
    down = jnp.where(low, 0.0, packed).astype(BF)
    lse = lse_ref[0]
    delta = delta_ref[step % 2]
    def rows_of(part):
        return pl.ds(pl.multiple_of(part * width, width), width)
    def score(part, s, p):
        pieces = kv_ref[rows_of(part), :]
        s[...] = dot(pieces, query, 1, 1)
        p[...] = dot(pieces, down, 1, 1)
    def absorb(part, s, p, dq, start):
        rows = rows_of(part)
        probs = jnp.exp2(s[...] * steps_of - lse)
        if start is not None:
            key = lax.broadcasted_iota(jnp.int32, (width, 1), 0) + start
            ask = lax.broadcasted_iota(jnp.int32, (1, tile), 1)
            probs = jnp.where(key // per_frame <= ask // per_frame, probs, 0.0)
        dscore = (probs * (p[...] - delta)).astype(BF)
        acc_ref[rows, :] += dot(dscore, query, 1, 0) + dot(probs.astype(BF), down, 1, 0)
        return dq + dot(kt_ref[:, rows], dscore, 1, 0)
    last = tile_index(step)
    parts = tile // width
    dq = jnp.zeros((64, tile), F32)
    slots = ((sa, pa), (sb, pb))
    score(0, *slots[0])
    def body(j, dq):
        for i in range(parts):
            score(j * parts + i + 1, *slots[(i + 1) % 2])
            dq = absorb(j * parts + i, *slots[i % 2], dq, None)
        return dq
    dq = lax.fori_loop(0, last, body, dq)
    for i in range(parts):
        if i + 1 < parts:
            score(last * parts + i + 1, *slots[(i + 1) % 2])
        dq = absorb(last * parts + i, *slots[i % 2], dq, i * width)
    dq = dq * scale
    @pl.when(step % 2 == 0)
    def _():
        dq_t_ref[0:64, :] = dq
    @pl.when(step % 2 == 1)
    def _():
        dq_t_ref[64:128, :] = dq
        dq_ref[...] = dq_t_ref[...].T.astype(BF)
    @pl.when(step == 3)
    def _():
        @pl.loop(0, kv_ref.shape[0] // tile)
        def _(j):
            rows = pl.ds(pl.multiple_of(j * tile, tile), tile)
            total = acc_ref[rows, :]
            dkv_ref[rows, :] = jnp.where(low_lanes((tile, LANES)), total * scale, total).astype(BF)


def attend_back(queries, downs, lse, out_t, keys_values, tile, per_frame, scale):
    one = pl.Buffered(1)
    keys = keys_values.shape[0]
    packed = pl.BlockSpec((tile, LANES), lambda i: (i // 2, 0))
    whole = pl.BlockSpec(keys_values.shape, lambda i: (0, 0), pipeline_mode=one)
    return pl.pallas_call(
        partial(attend_back_kernel, tile, tile // 2, per_frame, scale),
        grid=(4,),
        in_specs=[
            packed,
            packed,
            pl.BlockSpec((1, 1, tile), lambda i: (i, 0, 0)),
            pl.BlockSpec((1, LANES, tile), lambda i: (i // 2, 0, 0)),
            whole,
        ],
        out_specs=[packed, pl.BlockSpec(keys_values.shape, lambda i: (0, 0))],
        out_shape=[
            jax.ShapeDtypeStruct((2 * tile, LANES), BF),
            jax.ShapeDtypeStruct(keys_values.shape, BF),
        ],
        scratch_shapes=[
            pltpu.VMEM((64, keys), BF),
            pltpu.VMEM((keys, LANES), F32),
            pltpu.VMEM((LANES, tile), F32),
            pltpu.VMEM((2, 1, tile), F32),
        ]
        + [pltpu.VMEM((tile // 2, tile), F32)] * 4,
        compiler_params=pltpu.CompilerParams(
            dimension_semantics=("arbitrary",), vmem_limit_bytes=36 * MIB
        ),
        cost_estimate=pl.CostEstimate(
            flops=8_000_000_000, bytes_accessed=12_000_000, transcendentals=0
        ),
        name="attend_back",
    )(queries, downs, lse, out_t, keys_values)


def exchange_kernel(axis, moves, sources, results, pair_of, work, finish, *refs):
    in_refs, refs = refs[:sources], refs[sources:]
    out_refs, refs = refs[:results], refs[results:]
    send_sem, recv_sem, own_sem = refs[-3:]
    scratch = refs[:-3]
    dests = scratch if finish is not None else out_refs
    me, count = lax.axis_index(axis), lax.axis_size(axis)
    barrier = pltpu.get_barrier_semaphore()
    for step in range(1, count):
        pl.semaphore_signal(
            barrier,
            inc=1,
            device_id={axis: lax.rem(me + step, count)},
            device_id_type=pl.DeviceIdType.MESH,
        )
    pl.semaphore_wait(barrier, count - 1)
    copies = []
    for step in range(1, count):
        peer = lax.rem(me + step, count)
        for index, (source, dest, take, place) in enumerate(moves):
            copies.append(
                pltpu.make_async_remote_copy(
                    src_ref=take(in_refs[source], peer),
                    dst_ref=place(dests[dest], me, peer),
                    send_sem=send_sem.at[index, step - 1],
                    recv_sem=recv_sem.at[index, step - 1],
                    device_id={axis: peer},
                    device_id_type=pl.DeviceIdType.MESH,
                )
            )
            copies[-1].start()
    for index, (source, dest, take, place) in enumerate(moves):
        copies.append(
            pltpu.make_async_copy(
                take(in_refs[source], me), place(dests[dest], me, me), own_sem.at[index]
            )
        )
        copies[-1].start()
    if work is not None:
        work(in_refs, out_refs, 0, 1)
    for copy in copies:
        copy.wait()
    if pair_of is not None:
        core = lax.rem(me, 2)
        ref = dests[pair_of].at[core]
        copy = pltpu.make_async_remote_copy(
            src_ref=ref,
            dst_ref=ref,
            send_sem=own_sem.at[len(moves)],
            recv_sem=own_sem.at[len(moves) + 1],
            device_id={axis: me + 1 - 2 * core},
            device_id_type=pl.DeviceIdType.MESH,
        )
        copy.start()
        copy.wait()
    if finish is not None:
        finish(dests, in_refs, out_refs)


def exchange(
    name,
    axis,
    number,
    moves,
    arrays,
    shapes,
    pair_of=None,
    work=None,
    finish=None,
    landing=(),
    away=False,
    limit=16,
):
    count = lax.axis_size(axis)
    vmem = pl.BlockSpec(memory_space=pltpu.VMEM)
    out_spec = pl.BlockSpec(memory_space=pltpu.HBM) if away else vmem
    sent = sum(a.size * a.dtype.itemsize for a in arrays)
    return pl.pallas_call(
        partial(
            exchange_kernel, axis, moves, len(arrays), len(shapes), pair_of, work, finish
        ),
        in_specs=[vmem] * len(arrays),
        out_specs=[out_spec] * len(shapes),
        out_shape=[jax.ShapeDtypeStruct(*shape) for shape in shapes],
        scratch_shapes=[pltpu.VMEM(*shape) for shape in landing]
        + [
            pltpu.SemaphoreType.DMA((len(moves), count - 1)),
            pltpu.SemaphoreType.DMA((len(moves), count - 1)),
            pltpu.SemaphoreType.DMA((len(moves) + 2,)),
        ],
        compiler_params=pltpu.CompilerParams(
            collective_id=number, has_side_effects=True, vmem_limit_bytes=limit * MIB
        ),
        cost_estimate=pl.CostEstimate(
            flops=0, bytes_accessed=20_000_000 + 30 * sent, transcendentals=0
        ),
        name=name,
    )(*arrays)


def all_of(ref, peer):
    return ref


def block_of(ref, peer):
    return ref.at[peer]


def at_sender(ref, me, peer):
    return ref.at[me]


def lanes_of(size):
    def view(ref, peer):
        return ref.at[:, pl.ds(pl.multiple_of(peer * size, LANES), size)]

    return view


def lanes_at(size):
    def view(ref, me, peer):
        return ref.at[:, pl.ds(pl.multiple_of(me * size, LANES), size)]

    return view


def add_landed(dests, in_refs, out_refs):
    landed, out = dests[0], out_refs[0]
    rows = out.shape[0]
    step = 32 if rows % 32 == 0 else rows

    @pl.loop(0, rows // step)
    def _(j):
        cut = pl.ds(pl.multiple_of(j * step, step), step)
        total = landed[0, cut, :].astype(F32)
        for other in range(1, landed.shape[0]):
            total += landed[other, cut, :].astype(F32)
        out[cut, :] = total.astype(out.dtype)


def gather(name, axis, number, arrays):
    count = lax.axis_size(axis)
    moves = [(i, i, all_of, at_sender) for i in range(len(arrays))]
    return exchange(
        name, axis, number, moves, arrays, [((count,) + a.shape, a.dtype) for a in arrays]
    )


def back_kernel(
    q_ref, kv_ref, out_ref, landed, summed, send_sem, recv_sem, own_sem, pair_sem
):
    me, count = lax.axis_index("row"), lax.axis_size("row")
    core = lax.rem(me, 2)
    barrier = pltpu.get_barrier_semaphore()
    for step in range(1, count):
        pl.semaphore_signal(
            barrier,
            inc=1,
            device_id={"row": lax.rem(me + step, count)},
            device_id_type=pl.DeviceIdType.MESH,
        )
    pl.semaphore_wait(barrier, count - 1)
    half = pltpu.make_async_remote_copy(
        src_ref=kv_ref.at[1 - core],
        dst_ref=landed,
        send_sem=pair_sem.at[0],
        recv_sem=pair_sem.at[1],
        device_id={"row": me + 1 - 2 * core},
        device_id_type=pl.DeviceIdType.MESH,
    )
    half.start()

    def send(index, source, dest, step):
        peer = lax.rem(me + step, count)
        copy = pltpu.make_async_remote_copy(
            src_ref=source.at[:, :, peer],
            dst_ref=dest,
            send_sem=send_sem.at[index, step - 1],
            recv_sem=recv_sem.at[index, step - 1],
            device_id={"row": peer},
            device_id_type=pl.DeviceIdType.MESH,
        )
        copy.start()
        return copy

    copies = [send(0, q_ref, out_ref.at[me, 0:2], step) for step in range(1, count)]
    copies.append(
        pltpu.make_async_copy(q_ref.at[:, :, me], out_ref.at[me, 0:2], own_sem.at[0])
    )
    copies[-1].start()
    half.wait()
    for part in range(summed.shape[0]):

        @pl.loop(0, summed.shape[1])
        def _(j):
            total = kv_ref[core, part, j].astype(F32) + landed[part, j].astype(F32)
            summed[part, j] = total.astype(BF)

    copies += [send(1, summed, out_ref.at[me, 2:6], step) for step in range(1, count)]
    copies.append(
        pltpu.make_async_copy(summed.at[:, :, me], out_ref.at[me, 2:6], own_sem.at[1])
    )
    copies[-1].start()
    for copy in copies:
        copy.wait()


def exchange_back(number, queries, keys_values, shape):
    count = lax.axis_size("row")
    vmem = pl.BlockSpec(memory_space=pltpu.VMEM)
    return pl.pallas_call(
        back_kernel,
        in_specs=[vmem] * 2,
        out_specs=vmem,
        out_shape=jax.ShapeDtypeStruct(*shape),
        scratch_shapes=[
            pltpu.VMEM(keys_values.shape[1:], BF),
            pltpu.VMEM(keys_values.shape[1:], BF),
            pltpu.SemaphoreType.DMA((2, count - 1)),
            pltpu.SemaphoreType.DMA((2, count - 1)),
            pltpu.SemaphoreType.DMA((2,)),
            pltpu.SemaphoreType.DMA((2,)),
        ],
        compiler_params=pltpu.CompilerParams(
            collective_id=number, has_side_effects=True, vmem_limit_bytes=16 * MIB
        ),
        cost_estimate=pl.CostEstimate(flops=0, bytes_accessed=80_000_000, transcendentals=0),
        name="grad_to_tokens",
    )(queries, keys_values)


def square_gather_kernel(beside, *refs):
    in_ref, refs = refs[0], refs[1:]
    if beside:
        weight_ref, out_ref, full_ref, *refs = refs
    else:
        out_ref, *refs = refs
    send_sem, recv_sem, own_sem = refs[:3]
    me = lax.axis_index("frame")
    near = (me + 1 - 2 * lax.rem(me, 2), me + 2 - 4 * (me // 2))
    row, count = lax.axis_index("row"), lax.axis_size("row")
    partner = row + 1 - 2 * lax.rem(row, 2)
    greet = [{"frame": peer} for peer in near]
    if beside:
        greet += [{"row": lax.rem(row + 2 * k, count)} for k in range(1, count // 2)]
        greet.append({"row": partner})
    barrier = pltpu.get_barrier_semaphore()
    for device in greet:
        pl.semaphore_signal(
            barrier, inc=1, device_id=device, device_id_type=pl.DeviceIdType.MESH
        )
    pl.semaphore_wait(barrier, len(greet))
    half = in_ref.shape[0] // 2
    cuts = (pl.ds(0, half), pl.ds(half, half))

    def start(source, dest, sent, landed, device):
        copy = pltpu.make_async_remote_copy(
            src_ref=source,
            dst_ref=dest,
            send_sem=sent,
            recv_sem=landed,
            device_id=device,
            device_id_type=pl.DeviceIdType.MESH,
        )
        copy.start()
        return copy

    def copy_of(source, dest, way, index):
        device = {"frame": near[way]}
        return start(source, dest, send_sem.at[way, index], recv_sem.at[way, index], device)

    first, second, third = [], [], []
    for way in range(2):
        first.append(copy_of(in_ref.at[cuts[way]], out_ref.at[me, cuts[way]], way, 0))
    for way in range(2):
        rest = cuts[1 - way]
        second.append(copy_of(in_ref.at[rest], out_ref.at[me, rest], way, 1))
    local = [pltpu.make_async_copy(in_ref, out_ref.at[me], own_sem.at[0])]
    along, across = [], []
    if beside:
        row_send, row_recv, pair_send, pair_recv = refs[3:]
        for k in range(1, count // 2):
            device = {"row": lax.rem(row + 2 * k, count)}
            along.append(
                start(weight_ref, full_ref.at[row], row_send.at[k], row_recv.at[k], device)
            )
        across.append(
            start(
                weight_ref, full_ref.at[row], pair_send.at[0], pair_recv.at[0], {"row": partner}
            )
        )
        local.append(pltpu.make_async_copy(weight_ref, full_ref.at[row], own_sem.at[1]))
    for copy in local:
        copy.start()
    for way in range(2):
        first[way].wait_recv()
        block = out_ref.at[near[way], cuts[way]]
        third.append(copy_of(block, block, 1 - way, 2))
    for k, copy in enumerate(along, 1):
        copy.wait_recv()
        block = full_ref.at[lax.rem(row - 2 * k + count, count)]
        across.append(start(block, block, pair_send.at[k], pair_recv.at[k], {"row": partner}))
    for way in range(2):
        first[way].wait_send()
        second[way].wait()
        third[way].wait()
    for copy in along:
        copy.wait_send()
    for copy in across + local:
        copy.wait()


def gather_frame(name, number, array, weight=None):
    if lax.axis_size("frame") != 4:
        full = gather(name, "frame", number, [array])[0]
        if weight is None:
            return full
        return full, lax.all_gather(weight, "row", axis=0, tiled=False)
    vmem = pl.BlockSpec(memory_space=pltpu.VMEM)
    count = lax.axis_size("row")
    arrays = [array] if weight is None else [array, weight]
    shapes = [jax.ShapeDtypeStruct((4,) + array.shape, array.dtype)]
    sems = [(2, 3), (2, 3), (2,)]
    if weight is not None:
        shapes.append(jax.ShapeDtypeStruct((count,) + weight.shape, weight.dtype))
        sems += [(count // 2,)] * 4
    results = pl.pallas_call(
        partial(square_gather_kernel, weight is not None),
        in_specs=[vmem] * len(arrays),
        out_specs=[vmem] * len(shapes),
        out_shape=shapes,
        scratch_shapes=[pltpu.SemaphoreType.DMA(shape) for shape in sems],
        compiler_params=pltpu.CompilerParams(
            collective_id=number, has_side_effects=True, vmem_limit_bytes=16 * MIB
        ),
        cost_estimate=pl.CostEstimate(flops=0, bytes_accessed=30_000_000, transcendentals=0),
        name=name,
    )(*arrays)
    return results[0] if weight is None else results


def greet_all():
    barrier = pltpu.get_barrier_semaphore()
    total = 0
    for axis in ("frame", "row"):
        me, count = lax.axis_index(axis), lax.axis_size(axis)
        for step in range(1, count):
            pl.semaphore_signal(
                barrier,
                inc=1,
                device_id={axis: lax.rem(me + step, count)},
                device_id_type=pl.DeviceIdType.MESH,
            )
        total += count - 1
    pl.semaphore_wait(barrier, total)


def send_all(axis, take, dest, sems, own_sem):
    me, count = lax.axis_index(axis), lax.axis_size(axis)
    send_sem, recv_sem = sems
    copies = []
    for step in range(1, count):
        peer = lax.rem(me + step, count)
        copies.append(
            pltpu.make_async_remote_copy(
                src_ref=take(peer),
                dst_ref=dest.at[me],
                send_sem=send_sem.at[step - 1],
                recv_sem=recv_sem.at[step - 1],
                device_id={axis: peer},
                device_id_type=pl.DeviceIdType.MESH,
            )
        )
    copies.append(pltpu.make_async_copy(take(me), dest.at[me], own_sem))
    for copy in copies:
        copy.start()
    return copies


def two_ways_kernel(mod_ref, parts_ref, mod_out, sum_ref, landed, *sems):
    greet_all()
    copies = send_all("frame", lambda peer: mod_ref, mod_out, sems[0:2], sems[4].at[0])
    copies += send_all("row", lambda peer: parts_ref.at[peer], landed, sems[2:4], sems[4].at[1])
    for copy in copies:
        copy.wait()
    total = landed[0]
    for other in range(1, landed.shape[0]):
        total += landed[other]
    sum_ref[...] = total


def both_axes_kernel(in_ref, out_ref, held, *sems):
    greet_all()
    for copy in send_all("frame", lambda peer: in_ref, held, sems[0:2], sems[4].at[0]):
        copy.wait()
    for copy in send_all("row", lambda peer: held, out_ref, sems[2:4], sems[4].at[1]):
        copy.wait()


def both_axes(body, name, number, arrays, shapes, landing):
    frame_devs, row_devs = lax.axis_size("frame"), lax.axis_size("row")
    vmem = pl.BlockSpec(memory_space=pltpu.VMEM)
    sems = [frame_devs - 1] * 2 + [row_devs - 1] * 2 + [2]
    return pl.pallas_call(
        body,
        in_specs=[vmem] * len(arrays),
        out_specs=[vmem] * len(shapes),
        out_shape=[jax.ShapeDtypeStruct(*shape) for shape in shapes],
        scratch_shapes=[pltpu.VMEM(*landing)]
        + [pltpu.SemaphoreType.DMA((count,)) for count in sems],
        compiler_params=pltpu.CompilerParams(
            collective_id=number, has_side_effects=True, vmem_limit_bytes=8 * MIB
        ),
        cost_estimate=pl.CostEstimate(flops=0, bytes_accessed=20_000_000, transcendentals=0),
        name=name,
    )(*arrays)


def scatter_sum(name, axis, number, parts, dtype=F32):
    return exchange(
        name,
        axis,
        number,
        [(0, 0, block_of, at_sender)],
        [parts],
        [(parts.shape[1:], dtype)],
        finish=add_landed,
        landing=[(parts.shape, parts.dtype)],
    )[0]


def square_scatter_kernel(sources, results, work, *refs):
    in_refs, refs = refs[:sources], refs[sources:]
    out_refs, refs = refs[:results], refs[results:]
    landed, passing, stage, send_sem, recv_sem = refs
    parts_ref = in_refs[0]
    me = lax.axis_index("frame")
    near = (me + 1 - 2 * lax.rem(me, 2), me + 2 - 4 * (me // 2))
    barrier = pltpu.get_barrier_semaphore()
    for peer in near:
        pl.semaphore_signal(
            barrier, inc=1, device_id={"frame": peer}, device_id_type=pl.DeviceIdType.MESH
        )
    pl.semaphore_wait(barrier, 2)
    rows = parts_ref.shape[1]
    half = rows // 2
    step = 32 if half % 32 == 0 else half

    def copy_of(source, dest, way, index):
        copy = pltpu.make_async_remote_copy(
            src_ref=source,
            dst_ref=dest,
            send_sem=send_sem.at[way, index],
            recv_sem=recv_sem.at[way, index],
            device_id={"frame": near[way]},
            device_id_type=pl.DeviceIdType.MESH,
        )
        copy.start()
        return copy

    cuts = (pl.ds(0, half), pl.ds(half, half))
    first = [
        copy_of(parts_ref.at[3 - me, cuts[way]], passing.at[way], way, 0) for way in range(2)
    ]
    second = [
        copy_of(parts_ref.at[near[way], cuts[way]], landed.at[way, cuts[way]], way, 1)
        for way in range(2)
    ]
    if work is not None:
        work(in_refs, out_refs, 0, 2)
    for way in range(2):
        first[way].wait_recv()

        @pl.loop(0, half // step)
        def _(j):
            cut = pl.ds(pl.multiple_of(j * step, step), step)
            own = pl.ds(pl.multiple_of(way * half + j * step, step), step)
            total = passing[way, cut, :].astype(F32) + parts_ref[near[1 - way], own, :].astype(F32)
            stage[way, cut, :] = total.astype(BF)

    third = [
        copy_of(stage.at[1 - way], landed.at[way, cuts[1 - way]], way, 2) for way in range(2)
    ]
    if work is not None:
        work(in_refs, out_refs, 1, 2)
    for way in range(2):
        first[way].wait_send()
        second[way].wait()
        third[way].wait()
    out = out_refs[0]

    @pl.loop(0, rows // step)
    def _(j):
        cut = pl.ds(pl.multiple_of(j * step, step), step)
        total = parts_ref[me, cut, :].astype(F32)
        total += landed[0, cut, :].astype(F32) + landed[1, cut, :].astype(F32)
        out[cut, :] = total


def scatter_frame(name, number, parts, extras=(), shapes=(), work=None, limit=24):
    arrays = [parts, *extras]
    shapes = [(parts.shape[1:], F32), *shapes]
    if lax.axis_size("frame") != 4:
        return exchange(
            name,
            "frame",
            number,
            [(0, 0, block_of, at_sender)],
            arrays,
            shapes,
            work=work,
            finish=add_landed,
            landing=[(parts.shape, BF)],
            limit=limit + 12,
        )
    vmem = pl.BlockSpec(memory_space=pltpu.VMEM)
    _, rows, width = parts.shape
    return pl.pallas_call(
        partial(square_scatter_kernel, len(arrays), len(shapes), work),
        in_specs=[vmem] * len(arrays),
        out_specs=[vmem] * len(shapes),
        out_shape=[jax.ShapeDtypeStruct(*shape) for shape in shapes],
        scratch_shapes=[
            pltpu.VMEM((2, rows, width), BF),
            pltpu.VMEM((2, rows // 2, width), BF),
            pltpu.VMEM((2, rows // 2, width), BF),
            pltpu.SemaphoreType.DMA((2, 3)),
            pltpu.SemaphoreType.DMA((2, 3)),
        ],
        compiler_params=pltpu.CompilerParams(
            collective_id=number, has_side_effects=True, vmem_limit_bytes=limit * MIB
        ),
        cost_estimate=pl.CostEstimate(flops=0, bytes_accessed=80_000_000, transcendentals=0),
        name=name,
    )(*arrays)


def cut_kernel(slice_width, hidden_slice, in_ref, up_ref, down_ref, *refs):
    own_in, own_up, own_down, sems = refs
    frame = lax.axis_index("frame")
    width = in_ref.shape[1] // 4
    hidden = pl.ds(pl.multiple_of(frame * hidden_slice, LANES), hidden_slice)
    pieces = [
        (up_ref.at[:, hidden], own_up),
        (down_ref.at[:, hidden], own_down),
    ]
    for part in range(4):
        start = pl.multiple_of(part * width + frame * slice_width, LANES)
        pieces.append(
            (
                in_ref.at[:, pl.ds(start, slice_width)],
                own_in.at[:, part * slice_width : (part + 1) * slice_width],
            )
        )
    copies = [
        pltpu.make_async_copy(source, dest, sems.at[index])
        for index, (source, dest) in enumerate(pieces)
    ]
    for copy in copies:
        copy.start()
    for copy in copies:
        copy.wait()


def cut_weights(attn_in, up_weight, down_weight, slice_width, hidden_slice):
    rows = attn_in.shape[0]
    vmem = pl.BlockSpec(memory_space=pltpu.VMEM)
    return pl.pallas_call(
        partial(cut_kernel, slice_width, hidden_slice),
        in_specs=[pl.BlockSpec(memory_space=pl.ANY)] * 3,
        out_specs=[vmem] * 3,
        out_shape=[
            jax.ShapeDtypeStruct((rows, 4 * slice_width), BF),
            jax.ShapeDtypeStruct((rows, hidden_slice), BF),
            jax.ShapeDtypeStruct((rows, hidden_slice), BF),
        ],
        scratch_shapes=[pltpu.SemaphoreType.DMA((6,))],
        compiler_params=pltpu.CompilerParams(vmem_limit_bytes=58 * MIB),
        name="cut_weights",
    )(attn_in, up_weight, down_weight)


def join_kernel(hidden_slice, parts_ref, up_ref, down_ref, out_ref):
    total = None
    for part in range(parts_ref.shape[0]):
        cut = slice(part * hidden_slice, (part + 1) * hidden_slice)
        up_ref[:, cut] = parts_ref[part, :, :hidden_slice].astype(F32)
        down_ref[:, cut] = parts_ref[part, :, hidden_slice : 2 * hidden_slice].astype(F32)
        last = parts_ref[part, :, 2 * hidden_slice :].astype(F32)
        total = last if total is None else total + last
    out_ref[...] = total


def join_in_kernel(width, slice_width, parts_ref, in_ref):
    for part in range(parts_ref.shape[0]):
        for group in range(4):
            start = group * width + part * slice_width
            in_ref[:, start : start + slice_width] = parts_ref[
                part, :, group * slice_width : (group + 1) * slice_width
            ].astype(F32)


def join(name, body, parts, widths):
    count, rows, columns = parts.shape
    step = rows // 4
    return pl.pallas_call(
        body,
        grid=(4,),
        in_specs=[pl.BlockSpec((count, step, columns), lambda i: (0, i, 0))],
        out_specs=[pl.BlockSpec((step, w), lambda i: (i, 0)) for w in widths],
        out_shape=[jax.ShapeDtypeStruct((rows, w), F32) for w in widths],
        compiler_params=pltpu.CompilerParams(
            dimension_semantics=("arbitrary",), vmem_limit_bytes=16 * MIB
        ),
        cost_estimate=pl.CostEstimate(flops=0, bytes_accessed=8_000_000, transcendentals=0),
        name=name,
    )(parts)


def grads_beside(cut):
    def work(in_refs, out_refs, share, shares):
        hid_ref, pre_ref, cot_ref, act_ref, down_ref = in_refs[1:]
        grads_ref, branch_ref = out_refs[1:]
        columns = pre_ref.shape[1]
        block = max(cut, LANES)
        count = hid_ref.shape[1] // block
        rows = branch_ref.shape[0] // count

        @pl.loop(count * share // shares, count * (share + 1) // shares)
        def _(i):
            lanes = pl.ds(pl.multiple_of(i * block, LANES), block)
            for part, (left, right) in enumerate(((hid_ref, pre_ref), (cot_ref, act_ref))):
                result = dot(left[:, lanes], right[...], 0, 0).astype(BF)
                for piece in range(block // cut):
                    grads_ref[
                        i * (block // cut) + piece, :, part * columns : (part + 1) * columns
                    ] = result[piece * cut : (piece + 1) * cut]
            own = pl.ds(pl.multiple_of(i * rows, rows), rows)
            branch_ref[own, :] = dot(act_ref[own, :], down_ref[...], 1, 1).astype(BF)

    return work


def out_grad_kernel(cut, gated_ref, grad_ref, before_ref, out_ref):
    result = dot(gated_ref[...], grad_ref[...], 0, 0).astype(BF)
    for piece in range(out_ref.shape[0]):
        out_ref[piece] = result[piece * cut : (piece + 1) * cut]


def add_out_grad(gated, grad, grads):
    row_devs, cut, columns = grads.shape
    tokens, width = gated.shape
    block = width // 2
    last = (columns - width) // width
    assert columns % width == 0
    return pl.pallas_call(
        partial(out_grad_kernel, cut),
        grid=(width // block,),
        in_specs=[
            pl.BlockSpec((tokens, block), lambda i: (0, i)),
            pl.BlockSpec(grad.shape, lambda i: (0, 0), pipeline_mode=pl.Buffered(1)),
            pl.BlockSpec(memory_space=pl.ANY),
        ],
        out_specs=pl.BlockSpec((block // cut, cut, width), lambda i: (i, 0, last)),
        out_shape=jax.ShapeDtypeStruct(grads.shape, BF),
        input_output_aliases={2: 0},
        compiler_params=pltpu.CompilerParams(
            dimension_semantics=("arbitrary",), vmem_limit_bytes=58 * MIB
        ),
        cost_estimate=pl.CostEstimate(
            flops=600_000_000, bytes_accessed=5_000_000, transcendentals=0
        ),
        name="out_grad",
    )(gated, grad, grads)


def on_device(
    tokens,
    timesteps,
    noise_table,
    mod_weight,
    mod_bias,
    attn_in,
    out_weight,
    up_weight,
    down_weight,
    cotangent,
):
    clips, frames, rows_dev, grid_side, width = tokens.shape
    frame_index = lax.axis_index("frame")
    row_index = lax.axis_index("row")
    frame_devs, row_devs = lax.axis_size("frame"), lax.axis_size("row")
    core = row_index % 2
    clip_len = frames * frame_devs
    head_dim = width // HEADS
    heads = HEADS // frame_devs
    slice_width = width // frame_devs
    per_frame_dev = rows_dev * grid_side
    per_frame = grid_side * grid_side
    token_count = clips * frames * per_frame_dev
    group_count = token_count * frame_devs
    tile = clip_len // 8 * per_frame
    scale = head_dim ** (-0.5)
    step_count = noise_table.shape[0]
    assert head_dim == 64 and row_devs == 2 * clips * heads

    def by_frames(values):
        parts = values.reshape(frame_devs, clips, frames * per_frame_dev, -1)
        return jnp.transpose(parts, (1, 0, 2, 3)).reshape(group_count, values.shape[-1])

    def to_frames(values):
        parts = values.reshape(clips, frame_devs, frames * per_frame_dev, -1)
        return jnp.transpose(parts, (1, 0, 2, 3)).reshape(frame_devs, token_count, -1)

    def gather_frames(values):
        full = lax.all_gather(values, "frame", axis=1, tiled=True)
        return full.reshape(group_count, values.shape[-1])

    def scatter_frames(values):
        parts = to_frames(values).reshape(group_count, width)
        return lax.psum_scatter(parts, "frame", scatter_dimension=0, tiled=True).reshape(
            tokens.shape
        )

    hidden_slice = up_weight.shape[1] // frame_devs
    own_in, own_up, own_down = cut_weights(
        attn_in, up_weight, down_weight, slice_width, hidden_slice
    )
    weight_in = lax.all_gather(own_in, "row", axis=0, tiled=True)

    steps_iota = lax.broadcasted_iota(jnp.int32, (1, 1, step_count), 2)
    one_hot = (timesteps[:, :, None] == steps_iota).astype(BF)
    embedding = jnp.einsum("cls,sd->cld", one_hot, noise_table, preferred_element_type=F32)
    silu_low = jax.nn.silu(embedding).astype(BF)
    mod_local = jnp.einsum(
        "cld,de->cle", silu_low, mod_weight, preferred_element_type=F32
    ) + mod_bias.astype(F32)
    mod_width = mod_local.shape[2]
    modulation = exchange(
        "gather_mod",
        "row",
        0,
        [(0, 0, all_of, lanes_at(mod_width))],
        [mod_local.astype(BF).reshape(clips * frames, mod_width)],
        [((clips * frames, mod_width * row_devs), BF)],
    )[0].astype(F32)
    modulation = modulation.reshape(clips, frames, 6, 1, 1, width)
    shift_one, scale_one, gate_one, shift_two, scale_two, gate_two = [
        modulation[:, :, part] for part in range(6)
    ]

    frame_freq, row_freq, col_freq = [np.tile(t, 4) for t in rotary_freqs(head_dim // 2)]
    shape_three = (clip_len, rows_dev, grid_side, LANES)
    frame_pos = lax.broadcasted_iota(F32, shape_three, 0)
    row_pos = (row_index * rows_dev + lax.broadcasted_iota(jnp.int32, shape_three, 1)).astype(F32)
    col_pos = lax.broadcasted_iota(F32, shape_three, 2)
    angles = (frame_pos * frame_freq + row_pos * row_freq + col_pos * col_freq).reshape(-1, LANES)
    sign = np.where(np.arange(LANES) % 64 < 32, -1.0, 1.0).astype(np.float32)
    cosines = jnp.cos(angles)
    sines = jnp.sin(angles) * sign

    token_f = tokens.astype(F32)
    hidden_one, norm_one_pull = jax.vjp(modulate, token_f, shift_one, scale_one)
    hidden_group = by_frames(
        gather_frame("gather_one", 1, hidden_one.astype(BF).reshape(token_count, width))
    )

    grad_out = cotangent.astype(F32)
    grad_branch_two = (grad_out * gate_two).astype(BF)
    hidden_group, grad_branch_two = lax.optimization_barrier((hidden_group, grad_branch_two))
    grad_two_group = gather_frames(grad_branch_two)

    pack, gate_raw = qkv_project(hidden_group, weight_in, cosines, sines, clips, heads)

    half = tile // row_devs

    spans = half // per_frame_dev
    by_token = (spans, per_frame_dev, LANES)
    by_head = (spans, row_devs, per_frame_dev, LANES)

    def peer_rows(ref, peer):
        return ref.at[:, :, peer]

    queries, keys_values = exchange(
        "to_heads",
        "row",
        2,
        [
            (0, 0, lambda r, p: r.at[p, 0:2], lambda r, me, p: r.at[:, :, me]),
            (0, 1, lambda r, p: r.at[p, 2:6], lambda r, me, p: r.at[p % 2, :, :, me]),
        ],
        [pack.reshape((row_devs, 6) + by_token)],
        [((2,) + by_head, BF), ((2, 4) + by_head, BF)],
        pair_of=1,
        away=True,
    )
    queries = queries.reshape(-1, LANES)
    keys_values = keys_values.reshape(-1, LANES)

    queries, keys_values, grad_two_group, own_out = lax.optimization_barrier(
        (queries, keys_values, grad_two_group, out_weight)
    )
    full_out = lax.all_gather(own_out, "row", axis=0, tiled=True)

    attended_heads, attended_t, lse = attend(queries, keys_values, tile, per_frame, scale)
    gated_group, attended = exchange(
        "to_tokens",
        "row",
        3,
        [(0, 0, peer_rows, at_sender)],
        [attended_heads.reshape((2,) + by_head), gate_raw],
        [(gate_raw.shape, BF)] * 2,
        finish=gate_landed(clips, heads),
        landing=[((row_devs, 2) + by_token, BF)],
    )

    gated_group, full_out, own_up = lax.optimization_barrier((gated_group, full_out, own_up))
    weight_up = lax.all_gather(own_up, "row", axis=0, tiled=True)
    steps_wide = jnp.broadcast_to(timesteps.reshape(-1, 1), (clips * frames, LANES))
    gated, steps_parts = exchange(
        "gated_back",
        "frame",
        4,
        [(0, 0, block_of, lanes_at(slice_width)), (1, 1, all_of, at_sender)],
        [to_frames(gated_group), steps_wide],
        [((token_count, width), BF), ((frame_devs,) + steps_wide.shape, jnp.int32)],
    )
    branch_one = jnp.dot(gated, full_out, preferred_element_type=F32).reshape(tokens.shape)
    after_one = token_f + gate_one * branch_one
    hidden_two, norm_two_pull = jax.vjp(modulate, after_one, shift_two, scale_two)
    hidden_two_parts, weight_down = gather_frame(
        "gather_two", 5, hidden_two.astype(BF).reshape(token_count, width), own_down
    )
    hidden_two_group = by_frames(hidden_two_parts)
    weight_down = weight_down.reshape(width, hidden_slice)

    pre_act = jnp.dot(hidden_two_group, weight_up, preferred_element_type=F32)
    act_values, gelu_pull = jax.vjp(partial(jax.nn.gelu, approximate=True), pre_act)
    act_low = act_values.astype(BF)
    grad_act = jnp.dot(grad_two_group, weight_down, preferred_element_type=F32)
    (grad_pre,) = gelu_pull(grad_act)
    grad_pre = grad_pre.astype(BF)
    parts = to_frames(dot(grad_pre, weight_up, 1, 1).astype(BF))
    cut = width // row_devs
    grad_hidden_two, weight_grads, branch_two = scatter_frame(
        "scatter_two",
        6,
        parts,
        [hidden_two_group, grad_pre, grad_two_group, act_low, weight_down],
        [
            ((row_devs, cut, 2 * hidden_slice + width), BF),
            ((group_count, width), BF),
        ],
        grads_beside(cut),
        limit=30,
    )
    grad_hidden_two = grad_hidden_two.reshape(tokens.shape)
    branch_two = scatter_frames(branch_two)
    grad_after_part, grad_shift_two, grad_scale_two = norm_two_pull(grad_hidden_two)
    grad_after = grad_out + grad_after_part
    grad_gate_one = jnp.sum(grad_after * branch_one, axis=(2, 3), keepdims=True)
    grad_branch_one = (grad_after * gate_one).astype(BF).reshape(token_count, width)
    grad_gated = dot(grad_branch_one, full_out, 1, 1).astype(BF)
    weight_grads = add_out_grad(gated, grad_branch_one, weight_grads)
    grad_gated, weight_grads = lax.optimization_barrier((grad_gated, weight_grads))
    weight_grads = lax.psum_scatter(weight_grads, "row", scatter_dimension=0, tiled=True)
    (grad_gated,) = exchange(
        "grad_gated",
        "frame",
        7,
        [(0, 0, lanes_of(slice_width), at_sender)],
        [grad_gated],
        [((frame_devs, token_count, slice_width), BF)],
    )
    grad_gated = by_frames(grad_gated)
    down_pack, grad_gate = gate_back(grad_gated, gate_raw, attended, clips, heads)
    (downs,) = exchange(
        "grad_to_heads",
        "row",
        8,
        [(0, 0, block_of, lambda r, me, p: r.at[:, :, me])],
        [down_pack.reshape((row_devs, 2) + by_token)],
        [((2,) + by_head, BF)],
        away=True,
    )
    downs = downs.reshape(-1, LANES)
    downs, branch_two = lax.optimization_barrier((downs, branch_two))
    branch_two = branch_two.astype(F32)
    mixed = (after_one + gate_two * branch_two).astype(BF)
    grad_gate_two = jnp.sum(grad_out * branch_two, axis=(2, 3), keepdims=True)

    grad_queries, grad_kv = attend_back(
        queries, downs, lse, attended_t, keys_values, tile, per_frame, scale
    )
    grad_kv, weight_grads = lax.optimization_barrier((grad_kv, weight_grads))
    grads_all = lax.all_gather(weight_grads[0], "frame", axis=0, tiled=False)
    back_pack = exchange_back(
        9,
        grad_queries.reshape((2,) + by_head),
        grad_kv.reshape((2, 4) + by_head),
        ((row_devs, 6) + by_token, BF),
    )
    back_pack = back_pack.reshape(clips, heads, 2, 6, half, LANES)
    grad_mixed, grad_hidden = qkv_back(
        back_pack, grad_gate, weight_in, cosines, sines, clips, heads
    )
    grad_mixed, grads_all = lax.optimization_barrier((grad_mixed, grads_all))
    (grad_hidden_one,) = scatter_frame("scatter_one", 10, to_frames(grad_hidden), limit=16)
    grad_hidden_one = grad_hidden_one.reshape(tokens.shape)
    in_grad = lax.psum_scatter(
        dot(hidden_group, grad_mixed, 0, 0).astype(BF), "row", scatter_dimension=0, tiled=True
    )

    grad_token_part, grad_shift_one, grad_scale_one = norm_one_pull(grad_hidden_one)
    tokens_grad = (grad_after + grad_token_part).astype(BF)

    grad_mod = jnp.stack(
        [
            grad_shift_one,
            grad_scale_one,
            grad_gate_one,
            grad_shift_two,
            grad_scale_two,
            grad_gate_two,
        ],
        axis=2,
    ).reshape(clips * frames, 6 * width)
    grad_mod = jnp.transpose(
        grad_mod.reshape(clips * frames, row_devs, mod_width), (1, 0, 2)
    )
    grad_mod = scatter_sum("scatter_mod", "row", 11, grad_mod, BF)
    grad_mod, in_grad = lax.optimization_barrier((grad_mod, in_grad))
    frame_count = frame_devs * clips * frames
    grad_silu = dot(grad_mod, mod_weight, 1, 1).reshape(clips * frames, row_devs, cut)
    grad_silu = jnp.transpose(grad_silu, (1, 0, 2))
    grad_mod_all, grad_silu = both_axes(
        two_ways_kernel,
        "gather_grad_mod",
        12,
        [grad_mod, grad_silu],
        [((frame_devs,) + grad_mod.shape, BF), (grad_silu.shape[1:], F32)],
        (grad_silu.shape, F32),
    )
    (grad_silu,) = both_axes(
        both_axes_kernel,
        "gather_silu",
        13,
        [grad_silu],
        [((row_devs, frame_devs) + grad_silu.shape, F32)],
        ((frame_devs,) + grad_silu.shape, F32),
    )
    grad_silu = jnp.transpose(grad_silu, (1, 2, 0, 3)).reshape(frame_count, width)
    grad_mod_all = grad_mod_all.reshape(-1, mod_width)
    steps_all = steps_parts.reshape(-1, LANES)[:, 0]
    hot_all = steps_all[:, None] == lax.broadcasted_iota(jnp.int32, (1, step_count), 1)
    embed_all = jnp.dot(hot_all.astype(BF), noise_table, preferred_element_type=F32)
    silu_all, silu_pull = jax.vjp(jax.nn.silu, embed_all)
    mod_weight_grad = dot(silu_all.astype(BF), grad_mod_all, 0, 0)
    mod_bias_grad = jnp.sum(grad_mod_all.astype(F32), axis=0)
    (grad_embedding,) = silu_pull(grad_silu)
    noise_table_grad = lax.dot_general(
        hot_all.astype(F32),
        grad_embedding,
        (((0,), (0,)), ((), ())),
        precision=lax.Precision.HIGHEST,
    )

    up_weight_grad, down_weight_grad, out_weight_grad = join(
        "join_grads",
        partial(join_kernel, hidden_slice),
        grads_all,
        (up_weight.shape[1], down_weight.shape[1], width),
    )
    in_all = lax.all_gather(in_grad, "frame", axis=0, tiled=False)
    (attn_in_grad,) = join(
        "join_in", partial(join_in_kernel, width, slice_width), in_all, (attn_in.shape[1],)
    )
    return (
        mixed,
        tokens_grad,
        noise_table_grad,
        mod_weight_grad,
        mod_bias_grad,
        attn_in_grad,
        out_weight_grad,
        up_weight_grad,
        down_weight_grad,
    )


def solution(mesh):
    in_specs = (
        P(None, "frame", "row", None, None),
        P(None, "frame"),
        P(),
        P(None, "row"),
        P("row"),
        P("row", None),
        P("row", None),
        P("row", None),
        P("row", None),
        P(None, "frame", "row", None, None),
    )
    out_specs = (
        P(None, "frame", "row", None, None),
        P(None, "frame", "row", None, None),
        P(),
        P(None, "row"),
        P("row"),
        P("row", None),
        P("row", None),
        P("row", None),
        P("row", None),
    )
    return jax.shard_map(
        on_device, mesh=mesh, in_specs=in_specs, out_specs=out_specs, check_vma=False
    )
```
